8 devices in a mesh: dp: 2 (over z, y), cp: 4 (over x, core).
Axes of the slice: x: 2, y: 2, z: 1, core: 2. Of those that a mesh axis runs over, the one named last changes fastest.
Arguments:
- hidden: bfloat16 [4096, 2048], P(('dp', 'cp')), parts along dimension 0
- grad_out: bfloat16 [4096, 2048], P(('dp', 'cp')), parts along dimension 0
- w_query: bfloat16 [2048, 16, 128], replicated
- w_key: bfloat16 [2048, 2, 128], replicated
- w_value: bfloat16 [2048, 2, 128], replicated
- w_out: bfloat16 [16, 128, 2048], replicated
Outputs:
- output 1: bfloat16 [4096, 2048], P(('dp', 'cp')), parts along dimension 0
- output 2: bfloat16 [4096, 2048], P(('dp', 'cp')), parts along dimension 0
- output 3: float32 [4096, 16, 128], P('dp'), parts along dimension 0
- output 4: float32 [4096, 2, 128], P('dp'), parts along dimension 0
- output 5: float32 [4096, 2, 128], P('dp'), parts along dimension 0
- output 6: float32 [32, 128, 2048], P('dp'), parts along dimension 0
There are 2 independent parts. The reference program is written for one: setup_inputs(seed, part) draws one part's arguments, and reference() takes and returns one part's arrays. A program takes and returns all parts, laid end to end along the dimension named above; an argument that names none is the same for every part.
All inputs are finite; a program needn't handle non-finite values.
Results may differ from the reference program's by a relative error of at most 0.0107973.
Values are sent between devices in bfloat16 or wider.
A program may use at most 1 GiB of HBM per device.

```python
import jax
import jax.numpy as jnp
from jax import lax

TOKENS_DEV = 512
CP = 4
D = 2048
HEADS = 16
KV_HEADS = 2
HEAD = 128


def setup_inputs(seed: int = 0, part: int = 0) -> dict:
    seq_len = TOKENS_DEV * CP
    part_key = jax.random.fold_in(jax.random.key(seed), part)
    key_hidden, key_grad = jax.random.split(part_key)
    key_wq, key_wk, key_wv, key_wo = jax.random.split(jax.random.key(seed + 1), 4)
    hidden = jax.random.normal(key_hidden, (seq_len, D), jnp.float32)
    grad_out = jax.random.normal(key_grad, (seq_len, D), jnp.float32)
    w_query = jax.random.normal(key_wq, (D, HEADS, HEAD), jnp.float32) * D ** -0.5
    w_key = jax.random.normal(key_wk, (D, KV_HEADS, HEAD), jnp.float32) * D ** -0.5
    w_value = jax.random.normal(key_wv, (D, KV_HEADS, HEAD), jnp.float32) * D ** -0.5
    w_out = jax.random.normal(key_wo, (HEADS, HEAD, D), jnp.float32) * (HEADS * HEAD) ** -0.5
    return {
        "hidden": hidden.astype(jnp.bfloat16),
        "grad_out": grad_out.astype(jnp.bfloat16),
        "w_query": w_query.astype(jnp.bfloat16),
        "w_key": w_key.astype(jnp.bfloat16),
        "w_value": w_value.astype(jnp.bfloat16),
        "w_out": w_out.astype(jnp.bfloat16),
    }


def token_positions():
    half_len = TOKENS_DEV // 2
    row_ids = jnp.arange(TOKENS_DEV * CP)
    owner_dev = row_ids // TOKENS_DEV
    within = row_ids % TOKENS_DEV
    block_idx = jnp.where(within < half_len, owner_dev, 2 * CP - 1 - owner_dev)
    return block_idx * half_len + within % half_len


def reference(hidden, grad_out, w_query, w_key, w_value, w_out):
    seq_len = TOKENS_DEV * CP
    half_len = TOKENS_DEV // 2
    num_blocks = 2 * CP
    group_size = HEADS // KV_HEADS
    score_scale = HEAD ** -0.5
    positions = token_positions()
    wq_flat = w_query.reshape(D, HEADS * HEAD)
    wk_flat = w_key.reshape(D, KV_HEADS * HEAD)
    wv_flat = w_value.reshape(D, KV_HEADS * HEAD)
    wo_flat = w_out.reshape(HEADS * HEAD, D)
    query_all = jnp.dot(hidden, wq_flat, preferred_element_type=jnp.float32).astype(jnp.bfloat16)
    keys_all = jnp.dot(hidden, wk_flat, preferred_element_type=jnp.float32).astype(jnp.bfloat16)
    values_all = jnp.dot(hidden, wv_flat, preferred_element_type=jnp.float32).astype(jnp.bfloat16)
    keys_wide = keys_all.reshape(seq_len, KV_HEADS, HEAD).astype(jnp.float32)
    values_wide = values_all.reshape(seq_len, KV_HEADS, HEAD).astype(jnp.float32)
    query_blocks = query_all.reshape(num_blocks, half_len, KV_HEADS, group_size, HEAD)
    pos_blocks = positions.reshape(num_blocks, half_len)

    def masked_scores(query_block, pos_block):
        scores = jnp.einsum("qkgd,skd->kgqs", query_block.astype(jnp.float32), keys_wide) * score_scale
        visible = pos_block[:, None] >= positions[None, :]
        return jnp.where(visible, scores, -jnp.inf)

    def forward_block(items):
        query_block, pos_block = items
        masked = masked_scores(query_block, pos_block)
        log_norm = jax.nn.logsumexp(masked, axis=-1)
        att_probs = jnp.exp(masked - log_norm[..., None]).astype(jnp.bfloat16)
        attended = jnp.einsum("kgqs,skd->qkgd", att_probs.astype(jnp.float32), values_wide)
        return attended.astype(jnp.bfloat16), log_norm

    att_blocks, norm_blocks = lax.map(forward_block, (query_blocks, pos_blocks))
    attended = att_blocks.reshape(seq_len, HEADS * HEAD)
    output = jnp.dot(attended, wo_flat, preferred_element_type=jnp.float32).astype(jnp.bfloat16)
    d_att = jnp.dot(grad_out, wo_flat.T, preferred_element_type=jnp.float32).astype(jnp.bfloat16)
    delta_rows = jnp.sum(
        d_att.astype(jnp.float32).reshape(seq_len, KV_HEADS, group_size, HEAD)
        * attended.astype(jnp.float32).reshape(seq_len, KV_HEADS, group_size, HEAD),
        axis=-1,
    )
    delta_blocks = jnp.transpose(delta_rows.reshape(num_blocks, half_len, KV_HEADS, group_size), (0, 2, 3, 1))
    dout_blocks = d_att.reshape(num_blocks, half_len, KV_HEADS, group_size, HEAD)

    def backward_block(carry, items):
        key_acc, value_acc = carry
        query_block, pos_block, log_norm, dout_block, delta_block = items
        masked = masked_scores(query_block, pos_block)
        att_probs = jnp.exp(masked - log_norm[..., None]).astype(jnp.bfloat16).astype(jnp.float32)
        dout_wide = dout_block.astype(jnp.float32)
        d_probs = jnp.einsum("qkgd,skd->kgqs", dout_wide, values_wide)
        d_scores = (att_probs * (d_probs - delta_block[..., None])).astype(jnp.bfloat16).astype(jnp.float32)
        query_grad = (jnp.einsum("kgqs,skd->qkgd", d_scores, keys_wide) * score_scale).astype(jnp.bfloat16)
        key_acc = key_acc + jnp.einsum("kgqs,qkgd->skd", d_scores, query_block.astype(jnp.float32)) * score_scale
        value_acc = value_acc + jnp.einsum("kgqs,qkgd->skd", att_probs, dout_wide)
        return (key_acc, value_acc), query_grad

    zero_acc = jnp.zeros((seq_len, KV_HEADS, HEAD), jnp.float32)
    (key_sum, value_sum), query_grads = lax.scan(
        backward_block, (zero_acc, zero_acc), (query_blocks, pos_blocks, norm_blocks, dout_blocks, delta_blocks)
    )
    query_grad = query_grads.reshape(seq_len, HEADS * HEAD)
    key_grad = key_sum.astype(jnp.bfloat16).reshape(seq_len, KV_HEADS * HEAD)
    value_grad = value_sum.astype(jnp.bfloat16).reshape(seq_len, KV_HEADS * HEAD)
    grad_hidden = (
        jnp.dot(query_grad, wq_flat.T, preferred_element_type=jnp.float32)
        + jnp.dot(key_grad, wk_flat.T, preferred_element_type=jnp.float32)
        + jnp.dot(value_grad, wv_flat.T, preferred_element_type=jnp.float32)
    ).astype(jnp.bfloat16)
    grad_w_query = jnp.dot(hidden.T, query_grad, preferred_element_type=jnp.float32).reshape(D, HEADS, HEAD)
    grad_w_key = jnp.dot(hidden.T, key_grad, preferred_element_type=jnp.float32).reshape(D, KV_HEADS, HEAD)
    grad_w_value = jnp.dot(hidden.T, value_grad, preferred_element_type=jnp.float32).reshape(D, KV_HEADS, HEAD)
    grad_w_out = jnp.dot(attended.T, grad_out, preferred_element_type=jnp.float32).reshape(HEADS, HEAD, D)
    return (output, grad_hidden, grad_w_query, grad_w_key, grad_w_value, grad_w_out)
```

```python
import functools
import math

import jax
import jax.numpy as jnp
from jax import lax
from jax.experimental import pallas as pl
from jax.experimental.pallas import tpu as pltpu
from jax.sharding import PartitionSpec as P

BLK = 256
LOW = -3.0e38
F32 = jnp.float32
BF16 = jnp.bfloat16


def dot(a, b):
    return jnp.dot(a, b, preferred_element_type=F32)


def dot_nt(a, b):
    return lax.dot_general(a, b, (((1,), (1,)), ((), ())), preferred_element_type=F32)


def dot_tn(a, b):
    return lax.dot_general(a, b, (((0,), (0,)), ((), ())), preferred_element_type=F32)


def params(n=1, mib=60):
    return pltpu.CompilerParams(
        dimension_semantics=("arbitrary",) * n, vmem_limit_bytes=mib * 1024 * 1024
    )


def cost(flops, nbytes):
    return pl.CostEstimate(flops=int(flops), bytes_accessed=int(nbytes), transcendentals=0)


def proj_kernel(trans, num_w, sc, a_hbm, b_hbm, *refs):
    w_refs, out_ref, xs, sems = refs[:num_w], refs[num_w], refs[num_w + 1], refs[num_w + 2]
    i = pl.program_id(0)
    first = pltpu.make_async_copy(a_hbm, xs.at[0], sems.at[0])
    second = pltpu.make_async_copy(b_hbm, xs.at[1], sems.at[1])

    @pl.when(i == 0)
    def _():
        first.start()
        second.start()
        first.wait()

    @pl.when(i == 1)
    def _():
        second.wait()

    col = 0
    for w in w_refs:
        width = w.shape[0] if trans else w.shape[1]
        res = (dot_nt if trans else dot)(xs[i], w[...])
        out_ref[:, col : col + width] = res.astype(BF16)
        col += width


def project(core, a, b, weights, width, trans):
    rows, depth = a.shape
    if trans:
        specs = [pl.BlockSpec((width, depth), lambda i, s: (s[0], 0)) for _ in weights]
    else:
        specs = [pl.BlockSpec((depth, width), lambda i, s: (0, s[0])) for _ in weights]
    total = width * len(weights)
    return pl.pallas_call(
        functools.partial(proj_kernel, trans, len(weights)),
        out_shape=jax.ShapeDtypeStruct((2 * rows, total), BF16),
        grid_spec=pltpu.PrefetchScalarGridSpec(
            num_scalar_prefetch=1,
            grid=(2,),
            in_specs=[pl.BlockSpec(memory_space=pl.ANY)] * 2 + specs,
            out_specs=pl.BlockSpec((rows, total), lambda i, s: (i, 0)),
            scratch_shapes=[pltpu.VMEM((2, rows, depth), BF16), pltpu.SemaphoreType.DMA((2,))],
        ),
        compiler_params=params(),
        cost_estimate=cost(4 * rows * depth * total, 2 * (2 * rows * depth + depth * total + 2 * rows * total)),
    )(core, a, b, *weights)


def attn_kernel(heads, scale, final, sc, q_ref, do_ref, kv_a, kv_b, *refs):
    if final:
        init_ref, o_ref, dq_ref, dkv_ref = refs[:4]
        scratch = refs[4:]
    else:
        o_ref, dq_ref, dkv_ref = refs[:3]
        scratch = refs[3:]
    ks, vs, kt, vt, dk, dv, qt, dot_t, qst, dost, s_ref, p_ref, ds_ref, ot, dqt = scratch
    step = pl.program_id(0)
    wide = heads * BLK
    hd = 128
    c2 = scale * math.log2(math.e)

    @pl.when(step == 0)
    def _():
        for i in range(8):
            src = kv_a if i < 4 else kv_b
            rows = slice((i % 4) * BLK, (i % 4 + 1) * BLK)
            at = pl.ds(pl.multiple_of(sc[i] * BLK, BLK), BLK)
            kk, vv = src[rows, :hd], src[rows, hd:]
            ks[at, :] = kk
            vs[at, :] = vv
            kt[:, at] = kk.T
            vt[:, at] = vv.T
            if final:
                init_rows = slice(i * BLK, (i + 1) * BLK)
                dk[at, :] = init_ref[init_rows, :hd]
                dv[at, :] = init_ref[init_rows, hd:]
            else:
                dk[at, :] = jnp.zeros((BLK, hd), F32)
                dv[at, :] = jnp.zeros((BLK, hd), F32)

    for h in range(heads):
        cols = slice(h * hd, (h + 1) * hd)
        span = slice(h * BLK, (h + 1) * BLK)
        qh, dh = q_ref[:, cols], do_ref[:, cols]
        qst[span, :] = qh
        dost[span, :] = dh
        qt[:, span] = qh.T
        dot_t[:, span] = dh.T

    b = sc[8 + step]

    def softmax_block(j, stats, masked):
        m8, l8 = stats
        at = pl.ds(pl.multiple_of(j * BLK, BLK), BLK)
        t = dot(ks[at, :], qt[...]) * c2
        if masked:
            key = lax.broadcasted_iota(jnp.int32, (BLK, wide), 0)
            query = lax.broadcasted_iota(jnp.int32, (BLK, wide), 1) % BLK
            t = jnp.where(key <= query, t, LOW)
        s_ref[at, :] = t
        t3 = t.reshape(BLK // 8, 8, wide)
        new = jnp.maximum(m8, jnp.max(t3, axis=0))
        e = jnp.exp2(t3 - new[None])
        return new, l8 * jnp.exp2(m8 - new) + jnp.sum(e, axis=0)

    stats = (jnp.full((8, wide), LOW, F32), jnp.zeros((8, wide), F32))
    stats = lax.fori_loop(0, b, lambda j, st: softmax_block(j, st, False), stats)
    m8, l8 = softmax_block(b, stats, True)
    top = jnp.max(m8, axis=0, keepdims=True)
    lse = top + jnp.log2(jnp.sum(l8 * jnp.exp2(m8 - top), axis=0, keepdims=True))

    ot[...] = jnp.zeros_like(ot)

    def value_block(j, _):
        at = pl.ds(pl.multiple_of(j * BLK, BLK), BLK)
        p = jnp.exp2(s_ref[at, :] - lse).astype(BF16)
        p_ref[at, :] = p
        ot[...] += dot(vt[:, at], p)
        return 0

    lax.fori_loop(0, b + 1, value_block, 0)

    o_round = ot[...].astype(BF16)
    delta = jnp.sum(o_round.astype(F32) * dot_t[...].astype(F32), axis=0, keepdims=True)
    for h in range(heads):
        o_ref[:, h * hd : (h + 1) * hd] = o_round[:, h * BLK : (h + 1) * BLK].T
    dqt[...] = jnp.zeros_like(dqt)

    def grad_block(j, _):
        at = pl.ds(pl.multiple_of(j * BLK, BLK), BLK)
        dp = dot(vs[at, :], dot_t[...])
        dv[at, :] += dot(p_ref[at, :], dost[...])
        ds = (p_ref[at, :].astype(F32) * (dp - delta)).astype(BF16)
        ds_ref[...] = ds
        dqt[...] += dot(kt[:, at], ds_ref[...])
        dk[at, :] += dot(ds_ref[...], qst[...])
        return 0

    lax.fori_loop(0, b + 1, grad_block, 0)

    for h in range(heads):
        dq_ref[:, h * hd : (h + 1) * hd] = (dqt[:, h * BLK : (h + 1) * BLK] * scale).astype(BF16).T

    @pl.when(step == pl.num_programs(0) - 1)
    def _():
        for i in range(8):
            at = pl.ds(pl.multiple_of(sc[i] * BLK, BLK), BLK)
            if final:
                out = pl.ds(pl.multiple_of((i // 4 * 4 + sc[12 + i % 4]) * BLK, BLK), BLK)
                dkv_ref[out, :hd] = (dk[at, :] * scale).astype(BF16)
                dkv_ref[out, hd:] = dv[at, :].astype(BF16)
            else:
                out = slice(i * BLK, (i + 1) * BLK)
                dkv_ref[out, :hd] = dk[at, :]
                dkv_ref[out, hd:] = dv[at, :]


def attention(sc, q, do, kv_a, kv_b, init, scale):
    final = init is not None
    rows, width = q.shape
    heads = width // 128
    wide = heads * BLK
    seq = 2 * rows
    row_spec = pl.BlockSpec((BLK, width), lambda i, s: (i, 0))
    out_spec = pl.BlockSpec((BLK, width), lambda i, s: (s[12 + i], 0))
    full = lambda shape: pl.BlockSpec(shape, lambda i, s: (0, 0))
    ins = [q, do, kv_a, kv_b] + ([init] if final else [])
    in_specs = [row_spec, row_spec, full(kv_a.shape), full(kv_b.shape)]
    if final:
        in_specs.append(full(init.shape))
    return pl.pallas_call(
        functools.partial(attn_kernel, heads, scale, final),
        out_shape=(
            jax.ShapeDtypeStruct((rows, width), BF16),
            jax.ShapeDtypeStruct((rows, width), BF16),
            jax.ShapeDtypeStruct((seq, 256), BF16 if final else F32),
        ),
        grid_spec=pltpu.PrefetchScalarGridSpec(
            num_scalar_prefetch=1,
            grid=(rows // BLK,),
            in_specs=in_specs,
            out_specs=(out_spec, out_spec, full((seq, 256))),
            scratch_shapes=[
                pltpu.VMEM((seq, 128), BF16),
                pltpu.VMEM((seq, 128), BF16),
                pltpu.VMEM((128, seq), BF16),
                pltpu.VMEM((128, seq), BF16),
                pltpu.VMEM((seq, 128), F32),
                pltpu.VMEM((seq, 128), F32),
                pltpu.VMEM((128, wide), BF16),
                pltpu.VMEM((128, wide), BF16),
                pltpu.VMEM((wide, 128), BF16),
                pltpu.VMEM((wide, 128), BF16),
                pltpu.VMEM((seq, wide), F32),
                pltpu.VMEM((seq, wide), BF16),
                pltpu.VMEM((BLK, wide), BF16),
                pltpu.VMEM((128, wide), F32),
                pltpu.VMEM((128, wide), F32),
            ],
        ),
        compiler_params=params(),
        cost_estimate=cost(24e9, 20e6),
    )(sc, *ins)


def y_kernel(sc, o_mine, o_other, w_mine, w_other, out_ref):
    out_ref[...] = (dot(o_mine[...], w_mine[...]) + dot(o_other[...], w_other[...])).astype(BF16)


def out_rows(core, o_mine, o_other, wo):
    rows, half, model, tile = 512, o_mine.shape[1], wo.shape[1], 512
    return pl.pallas_call(
        y_kernel,
        out_shape=jax.ShapeDtypeStruct((rows, model), BF16),
        grid_spec=pltpu.PrefetchScalarGridSpec(
            num_scalar_prefetch=1,
            grid=(model // tile,),
            in_specs=[
                pl.BlockSpec((rows, half), lambda i, s: (s[0], 0)),
                pl.BlockSpec((rows, half), lambda i, s: (s[0], 0)),
                pl.BlockSpec((half, tile), lambda i, s: (s[0], i)),
                pl.BlockSpec((half, tile), lambda i, s: (1 - s[0], i)),
            ],
            out_specs=pl.BlockSpec((rows, tile), lambda i, s: (0, i)),
        ),
        compiler_params=params(),
        cost_estimate=cost(4 * rows * half * model, 12e6),
    )(core, o_mine, o_other, wo, wo)


def dx_kernel(sc, q_mine, q_other, kv_mine, kv_other, wq_mine, wq_other, wk_mine, wk_other, wv_mine, wv_other, out_ref):
    hd = 128
    acc = dot_nt(q_mine[...], wq_mine[...]) + dot_nt(q_other[...], wq_other[...])
    acc += dot_nt(kv_mine[:, :hd], wk_mine[...]) + dot_nt(kv_other[:, :hd], wk_other[...])
    acc += dot_nt(kv_mine[:, hd:], wv_mine[...]) + dot_nt(kv_other[:, hd:], wv_other[...])
    out_ref[...] = acc.astype(BF16)


def grad_rows(core, dq_mine, dq_other, dkv_mine, dkv_other, wq, wk, wv):
    rows, half, model, tile = 512, dq_mine.shape[1], wq.shape[0], 512
    mine = lambda i, s: (s[0], 0)
    return pl.pallas_call(
        dx_kernel,
        out_shape=jax.ShapeDtypeStruct((rows, model), BF16),
        grid_spec=pltpu.PrefetchScalarGridSpec(
            num_scalar_prefetch=1,
            grid=(model // tile,),
            in_specs=[
                pl.BlockSpec((rows, half), mine),
                pl.BlockSpec((rows, half), mine),
                pl.BlockSpec((rows, 256), mine),
                pl.BlockSpec((rows, 256), mine),
                pl.BlockSpec((tile, half), lambda i, s: (i, s[0])),
                pl.BlockSpec((tile, half), lambda i, s: (i, 1 - s[0])),
                pl.BlockSpec((tile, 128), lambda i, s: (i, s[0])),
                pl.BlockSpec((tile, 128), lambda i, s: (i, 1 - s[0])),
                pl.BlockSpec((tile, 128), lambda i, s: (i, s[0])),
                pl.BlockSpec((tile, 128), lambda i, s: (i, 1 - s[0])),
            ],
            out_specs=pl.BlockSpec((rows, tile), lambda i, s: (0, i)),
        ),
        compiler_params=params(),
        cost_estimate=cost(4 * rows * half * model * 1.25, 14e6),
    )(core, dq_mine, dq_other, dkv_mine, dkv_other, wq, wq, wk, wk, wv, wv)


def dwq_kernel(aliased, sc, x0, x1, x2, x3, q0, q1, q2, q3, k0, k1, k2, k3, *refs):
    out_ref, kv_ref = refs[-2:]
    xs = [x[...].T for x in (x0, x1, x2, x3)]
    acc = sum(dot(x, q[...]) for x, q in zip(xs, (q0, q1, q2, q3)))
    for h in range(8):
        out_ref[:, h, :] = acc[:, h * 128 : (h + 1) * 128]
    kv_ref[...] = sum(dot(x, k[...]) for x, k in zip(xs, (k0, k1, k2, k3)))


def grad_wq(sc, xs, dq_chip, dq_rem, dkv, flip, into):
    model, half, rows, tile = xs[0].shape[1], dq_chip.shape[1], 512, 256
    x_spec = pl.BlockSpec((rows, tile), lambda i, s: (0, i))
    at = lambda f, base=0: lambda i, s: (base + (1 - s[0] if f else s[0]), 0)
    specs = [x_spec] * 4
    specs += [pl.BlockSpec((rows, half), at(f)) for f in (0, 1, 0, 1)]
    specs += [pl.BlockSpec((rows, 256), at(f, base)) for f, base in ((0, 0), (1, 0), (0, 2), (1, 2))]
    ins = list(xs) + [dq_chip, dq_chip, dq_rem, dq_rem, dkv, dkv, dkv, dkv]
    alias = {}
    if into is not None:
        specs.append(pl.BlockSpec(memory_space=pl.ANY))
        ins.append(into)
        alias = {len(ins): 0}
    col = (lambda i, s: (i, 1 - s[0], 0)) if flip else (lambda i, s: (i, s[0], 0))
    return pl.pallas_call(
        functools.partial(dwq_kernel, into is not None),
        out_shape=(
            jax.ShapeDtypeStruct((model, 16, 128), F32),
            jax.ShapeDtypeStruct((model, 256), F32),
        ),
        grid_spec=pltpu.PrefetchScalarGridSpec(
            num_scalar_prefetch=1,
            grid=(model // tile,),
            in_specs=specs,
            out_specs=(
                pl.BlockSpec((tile, 8, 128), col),
                pl.BlockSpec((tile, 256), lambda i, s: (i, 0)),
            ),
        ),
        input_output_aliases=alias,
        compiler_params=params(),
        cost_estimate=cost(2 * 2048 * model * (half + 256), 22e6),
    )(sc, *ins)


def dwo_kernel(aliased, sc, o0, o1, o2, o3, y0, y1, y2, y3, *refs):
    out_ref = refs[-1]
    out_ref[...] = sum(dot(o[...].T, y[...]) for o, y in zip((o0, o1, o2, o3), (y0, y1, y2, y3)))


def grad_wo(sc, ys, o_chip, o_rem, flip, into):
    model, half, rows, tile = ys[0].shape[1], o_chip.shape[1], 512, 256
    at = lambda f: lambda i, s: ((1 - s[0] if f else s[0]), i)
    specs = [pl.BlockSpec((rows, tile), at(f)) for f in (0, 1, 0, 1)]
    specs += [pl.BlockSpec((rows, model), lambda i, s: (0, 0))] * 4
    ins = [o_chip, o_chip, o_rem, o_rem] + list(ys)
    alias = {}
    if into is not None:
        specs.append(pl.BlockSpec(memory_space=pl.ANY))
        ins.append(into)
        alias = {len(ins): 0}
    steps = half // tile
    base = (lambda i, s: ((1 - s[0]) * steps + i, 0)) if flip else (lambda i, s: (s[0] * steps + i, 0))
    return pl.pallas_call(
        functools.partial(dwo_kernel, into is not None),
        out_shape=jax.ShapeDtypeStruct((2 * half, model), F32),
        grid_spec=pltpu.PrefetchScalarGridSpec(
            num_scalar_prefetch=1,
            grid=(steps,),
            in_specs=specs,
            out_specs=pl.BlockSpec((tile, model), base),
        ),
        input_output_aliases=alias,
        compiler_params=params(),
        cost_estimate=cost(2 * 2048 * model * half, 22e6),
    )(sc, *ins)


def solution(mesh):
    row_spec = P(("dp", "cp"), None)
    rep_spec = P(None, None, None)
    part_spec = P("dp", None, None)
    core_swap = [(0, 1), (1, 0), (2, 3), (3, 2)]
    chip_swap = [(0, 2), (2, 0), (1, 3), (3, 1)]

    def device_layer(x, dy, w_query, w_key, w_value, w_out):
        rows, model = x.shape
        num_heads, hd = w_query.shape[1:]
        kv_heads = w_key.shape[1]
        scale = hd ** -0.5
        rank = lax.axis_index("cp").astype(jnp.int32)
        core = (rank & 1).reshape(1)
        devs = [rank, rank ^ 1, rank ^ 2, rank ^ 3]
        kv_pos = [p for e in devs for p in (e, 7 - e)]
        slots = [p for e in devs[:2] for p in ((e & 1) * 2, (e & 1) * 2 + 1)]
        sc_chip = jnp.stack(kv_pos + kv_pos[:4] + slots)
        sc_rem = jnp.stack(kv_pos + kv_pos[4:] + slots)

        to_core = lambda v: lax.ppermute(v, "cp", core_swap)
        to_chip = lambda v: lax.ppermute(v, "cp", chip_swap)

        x_p = to_core(x)
        dy_p = to_core(dy)
        wk = w_key.reshape(model, kv_heads * hd)
        wv = w_value.reshape(model, kv_heads * hd)
        wq = w_query.reshape(model, num_heads * hd)
        wo = w_out.reshape(num_heads * hd, model)

        kv = project(core, x, x_p, (wk, wv), hd, False)
        kv_r = to_chip(kv)
        x_send, kv2 = lax.optimization_barrier((x, kv))
        x_r = to_chip(x_send)
        dy_send, _ = lax.optimization_barrier((dy, kv))
        dy_r = to_chip(dy_send)
        x_rp = to_core(x_r)
        dy_rp = to_core(dy_r)

        q = project(core, x, x_p, (wq,), 1024, False)
        do = project(core, dy, dy_p, (wo,), 1024, True)
        o_c, dq_c, dkv_part = attention(sc_chip, q, do, kv2, kv_r, None, scale)
        o_co = to_core(o_c)
        y = out_rows(core, o_c, o_co, wo)

        q_rem = project(core, x_r, x_rp, (wq,), 1024, False)
        do_rem = project(core, dy_r, dy_rp, (wo,), 1024, True)
        o_r, dq_r, dkv = attention(sc_rem, q_rem, do_rem, kv2, kv_r, dkv_part, scale)
        dq_co = to_core(dq_c)
        dkv_o = to_core(dkv)
        dq_ro = to_core(dq_r)
        o_ro = to_core(o_r)

        xs = (x, x_p, x_r, x_rp)
        ys = (dy, dy_p, dy_r, dy_rp)
        gwo = grad_wo(core, ys, o_c, o_r, False, None)
        gwq, gkv = grad_wq(core, xs, dq_c, dq_r, dkv, False, None)
        dx = grad_rows(core, dq_c, dq_co, dkv, dkv_o, wq, wk, wv)
        gwo = grad_wo(core, ys, o_co, o_ro, True, gwo)
        gwq, gkv_o = grad_wq(core, xs, dq_co, dq_ro, dkv_o, True, gwq)
        low = core[0] == 0
        first, second = jnp.where(low, gkv, gkv_o), jnp.where(low, gkv_o, gkv)
        gwk = jnp.stack([first[:, :hd], second[:, :hd]], axis=1)
        gwv = jnp.stack([first[:, hd:], second[:, hd:]], axis=1)
        return y, dx, gwq, gwk, gwv, gwo.reshape(num_heads, hd, model)

    return jax.shard_map(
        device_layer,
        mesh=mesh,
        in_specs=(row_spec, row_spec, rep_spec, rep_spec, rep_spec, rep_spec),
        out_specs=(row_spec, row_spec, part_spec, part_spec, part_spec, part_spec),
        check_vma=False,
    )
```

```python
import functools
import math

import jax
import jax.numpy as jnp
from jax import lax
from jax.experimental import pallas as pl
from jax.experimental.pallas import tpu as pltpu
from jax.sharding import PartitionSpec as P

BLK = 256
LOW = -3.0e38
F32 = jnp.float32
BF16 = jnp.bfloat16


def dot(a, b):
    return jnp.dot(a, b, preferred_element_type=F32)


def dot_nt(a, b):
    return lax.dot_general(a, b, (((1,), (1,)), ((), ())), preferred_element_type=F32)


def dot_tn(a, b):
    return lax.dot_general(a, b, (((0,), (0,)), ((), ())), preferred_element_type=F32)


def params(n=1, mib=60):
    return pltpu.CompilerParams(
        dimension_semantics=("arbitrary",) * n, vmem_limit_bytes=mib * 1024 * 1024
    )


def cost(flops, nbytes):
    return pl.CostEstimate(flops=int(flops), bytes_accessed=int(nbytes), transcendentals=0)


def heads_kernel(w_ref, out_ref, wide):
    rows, num, hd = w_ref.shape
    wide[...] = w_ref[...].astype(F32).reshape(rows * num, hd)
    for h in range(num):
        out_ref[:, h * hd : (h + 1) * hd] = wide[pl.ds(h, rows, stride=num), :].astype(BF16)


def flat_heads(w):
    model, num, hd = w.shape
    tile = 256
    return pl.pallas_call(
        heads_kernel,
        out_shape=jax.ShapeDtypeStruct((model, num * hd), BF16),
        grid=(model // tile,),
        in_specs=[pl.BlockSpec((tile, num, hd), lambda i: (i, 0, 0))],
        out_specs=pl.BlockSpec((tile, num * hd), lambda i: (i, 0)),
        scratch_shapes=[pltpu.VMEM((tile * num, hd), F32)],
        compiler_params=params(),
        cost_estimate=cost(4e9, 4 * model * num * hd),
    )(w)


def proj_kernel(trans, rows, sc, *refs):
    num = len(rows)
    xs_hbm, (w_ref, out_ref, xs, sems) = refs[:num], refs[num:]
    copies, base = [], 0
    for n, (x, r) in enumerate(zip(xs_hbm, rows)):
        copies.append(pltpu.make_async_copy(x, xs.at[base : base + r, :], sems.at[n]))
        base += r

    @pl.when(pl.program_id(0) == 0)
    def _():
        for cp in copies:
            cp.start()
        for cp in copies:
            cp.wait()

    out_ref[...] = (dot_nt if trans else dot)(xs[...], w_ref[...]).astype(BF16)


def project(core, pieces, w, width, trans):
    rows, depth, tile = [p.shape[0] for p in pieces], pieces[0].shape[1], 256
    total, steps = sum(rows), width // tile
    if trans:
        spec = pl.BlockSpec((tile, depth), lambda i, s: (s[0] * steps + i, 0))
    else:
        spec = pl.BlockSpec((depth, tile), lambda i, s: (0, s[0] * steps + i))
    return pl.pallas_call(
        functools.partial(proj_kernel, trans, rows),
        out_shape=jax.ShapeDtypeStruct((total, width), BF16),
        grid_spec=pltpu.PrefetchScalarGridSpec(
            num_scalar_prefetch=1,
            grid=(steps,),
            in_specs=[pl.BlockSpec(memory_space=pl.ANY)] * len(pieces) + [spec],
            out_specs=pl.BlockSpec((total, tile), lambda i, s: (0, i)),
            scratch_shapes=[pltpu.VMEM((total, depth), BF16), pltpu.SemaphoreType.DMA((len(pieces),))],
        ),
        compiler_params=params(),
        cost_estimate=cost(2 * total * depth * width, 2 * (total * depth + depth * width + total * width)),
    )(core, *pieces, w)


def kv_kernel(x_ref, wk_ref, wv_ref, out_ref):
    out_ref[:, :256] = dot(x_ref[...], wk_ref[...]).astype(BF16)
    out_ref[:, 256:] = dot(x_ref[...], wv_ref[...]).astype(BF16)


def project_kv(x, wk, wv):
    rows, depth = x.shape
    tile = 256
    return pl.pallas_call(
        kv_kernel,
        out_shape=jax.ShapeDtypeStruct((rows, 512), BF16),
        grid=(rows // tile,),
        in_specs=[
            pl.BlockSpec((tile, depth), lambda i: (i, 0)),
            pl.BlockSpec((depth, 256), lambda i: (0, 0)),
            pl.BlockSpec((depth, 256), lambda i: (0, 0)),
        ],
        out_specs=pl.BlockSpec((tile, 512), lambda i: (i, 0)),
        compiler_params=params(),
        cost_estimate=cost(2 * rows * depth * 512, 5e6),
    )(x, wk, wv)


def attn_kernel(heads, scale, first, final, sc, q_ref, do_ref, *refs):
    kv_refs, refs = refs[:8], refs[8:]
    if first:
        o_ref, dq_ref, dkv_ref = refs[:3]
        scratch = refs[3:]
    else:
        init_ref, o_ref, dq_ref, dkv_ref = refs[:4]
        scratch = refs[4:]
    ks, vs, kt, vt, dk, dv, qt, dot_t, qst, dost, s_ref, p_ref, ds_ref, ot, dqt, m_ref, l_ref = scratch
    step = pl.program_id(0)
    wide = heads * BLK
    hd = 128
    c2 = scale * math.log2(math.e)

    @pl.when(step == 0)
    def _():
        for i in range(8):
            rows = slice((i % 2) * BLK, (i % 2 + 1) * BLK)
            at = pl.ds(pl.multiple_of(sc[i] * BLK, BLK), BLK)
            kk, vv = kv_refs[i // 2][rows, :], kv_refs[4 + i // 2][rows, :]
            ks[at, :] = kk
            vs[at, :] = vv
            kt[:, at] = kk.T
            vt[:, at] = vv.T
            if not first:
                init_rows = slice(i * BLK, (i + 1) * BLK)
                dk[at, :] = init_ref[init_rows, :hd]
                dv[at, :] = init_ref[init_rows, hd:]
            else:
                dk[at, :] = jnp.zeros((BLK, hd), F32)
                dv[at, :] = jnp.zeros((BLK, hd), F32)

    for h in range(heads):
        cols = slice(h * hd, (h + 1) * hd)
        span = slice(h * BLK, (h + 1) * BLK)
        qh, dh = q_ref[:, cols], do_ref[:, cols]
        qst[span, :] = qh
        dost[span, :] = dh
        qt[:, span] = qh.T
        dot_t[:, span] = dh.T

    b = sc[8 + step]

    def softmax_block(j, masked):
        at = pl.ds(pl.multiple_of(j * BLK, BLK), BLK)
        for h in range(heads):
            span = slice(h * BLK, (h + 1) * BLK)
            t = dot(ks[at, :], qt[:, span]) * c2
            if masked:
                key = lax.broadcasted_iota(jnp.int32, (BLK, BLK), 0)
                query = lax.broadcasted_iota(jnp.int32, (BLK, BLK), 1)
                t = jnp.where(key <= query, t, LOW)
            s_ref[at, span] = t
            m8 = m_ref[:, span]
            new = jnp.maximum(m8, jnp.max(t.reshape(BLK // 8, 8, BLK), axis=0))
            e = jnp.exp2(s_ref[at, span].reshape(BLK // 8, 8, BLK) - new[None])
            l_ref[:, span] = l_ref[:, span] * jnp.exp2(m8 - new) + jnp.sum(e, axis=0)
            m_ref[:, span] = new

    m_ref[...] = jnp.full((8, wide), LOW, F32)
    l_ref[...] = jnp.zeros((8, wide), F32)

    def open_block(j, _):
        softmax_block(j, False)
        return 0

    lax.fori_loop(0, b, open_block, 0)
    softmax_block(b, True)
    m8 = m_ref[...]
    top = jnp.max(m8, axis=0, keepdims=True)
    lse = top + jnp.log2(jnp.sum(l_ref[...] * jnp.exp2(m8 - top), axis=0, keepdims=True))

    ot[...] = jnp.zeros_like(ot)

    def value_block(j, _):
        at = pl.ds(pl.multiple_of(j * BLK, BLK), BLK)
        for h in range(heads):
            span = slice(h * BLK, (h + 1) * BLK)
            p = jnp.exp2(s_ref[at, span] - lse[:, span]).astype(BF16)
            p_ref[at, span] = p
            ot[:, span] += dot(vt[:, at], p)
        return 0

    lax.fori_loop(0, b + 1, value_block, 0)

    o_round = ot[...].astype(BF16)
    delta = jnp.sum(o_round.astype(F32) * dot_t[...].astype(F32), axis=0, keepdims=True)
    for h in range(heads):
        o_ref[:, h * hd : (h + 1) * hd] = o_round[:, h * BLK : (h + 1) * BLK].T
    dqt[...] = jnp.zeros_like(dqt)

    def grad_block(j, _):
        at = pl.ds(pl.multiple_of(j * BLK, BLK), BLK)
        dp = dot(vs[at, :], dot_t[...])
        dv[at, :] += dot(p_ref[at, :], dost[...])
        ds = (p_ref[at, :].astype(F32) * (dp - delta)).astype(BF16)
        ds_ref[...] = ds
        dqt[...] += dot(kt[:, at], ds_ref[...])
        dk[at, :] += dot(ds_ref[...], qst[...])
        return 0

    lax.fori_loop(0, b + 1, grad_block, 0)

    for h in range(heads):
        dq_ref[:, h * hd : (h + 1) * hd] = (dqt[:, h * BLK : (h + 1) * BLK] * scale).astype(BF16).T

    @pl.when(step == pl.num_programs(0) - 1)
    def _():
        for i in range(8):
            at = pl.ds(pl.multiple_of(sc[i] * BLK, BLK), BLK)
            if final:
                out = pl.ds(pl.multiple_of(sc[16 + i] * BLK, BLK), BLK)
                dkv_ref[out, :hd] = (dk[at, :] * scale).astype(BF16)
                dkv_ref[out, hd:] = dv[at, :].astype(BF16)
            else:
                out = slice(i * BLK, (i + 1) * BLK)
                dkv_ref[out, :hd] = dk[at, :]
                dkv_ref[out, hd:] = dv[at, :]


def attention(sc, q, do, kv_pieces, init, final, scale):
    first = init is None
    rows, width = q.shape
    heads = width // 128
    wide = heads * BLK
    seq = 2048
    row_spec = pl.BlockSpec((BLK, width), lambda i, s: (i, 0))
    out_spec = pl.BlockSpec((BLK, width), lambda i, s: (s[12 + i], 0))
    full = lambda shape: pl.BlockSpec(shape, lambda i, s: (0, 0))
    ins = [q, do] + list(kv_pieces) * 2 + ([] if first else [init])
    in_specs = [row_spec, row_spec]
    in_specs += [pl.BlockSpec((512, 128), lambda i, s: (0, s[24]))] * 4
    in_specs += [pl.BlockSpec((512, 128), lambda i, s: (0, 2 + s[24]))] * 4
    if not first:
        in_specs.append(full(init.shape))
    return pl.pallas_call(
        functools.partial(attn_kernel, heads, scale, first, final),
        out_shape=(
            jax.ShapeDtypeStruct((rows, width), BF16),
            jax.ShapeDtypeStruct((rows, width), BF16),
            jax.ShapeDtypeStruct((seq, 256), BF16 if final else F32),
        ),
        grid_spec=pltpu.PrefetchScalarGridSpec(
            num_scalar_prefetch=1,
            grid=(rows // BLK,),
            in_specs=in_specs,
            out_specs=(out_spec, out_spec, full((seq, 256))),
            scratch_shapes=[
                pltpu.VMEM((seq, 128), BF16),
                pltpu.VMEM((seq, 128), BF16),
                pltpu.VMEM((128, seq), BF16),
                pltpu.VMEM((128, seq), BF16),
                pltpu.VMEM((seq, 128), F32),
                pltpu.VMEM((seq, 128), F32),
                pltpu.VMEM((128, wide), BF16),
                pltpu.VMEM((128, wide), BF16),
                pltpu.VMEM((wide, 128), BF16),
                pltpu.VMEM((wide, 128), BF16),
                pltpu.VMEM((seq, wide), F32),
                pltpu.VMEM((seq, wide), BF16),
                pltpu.VMEM((BLK, wide), BF16),
                pltpu.VMEM((128, wide), F32),
                pltpu.VMEM((128, wide), F32),
                pltpu.VMEM((8, wide), F32),
                pltpu.VMEM((8, wide), F32),
            ],
        ),
        compiler_params=params(),
        cost_estimate=cost(6e9 * (rows // BLK), 20e6),
    )(sc, *ins)


def y_kernel(sc, o_mine, o_other, w_mine, w_other, out_ref):
    out_ref[...] = (dot(o_mine[...], w_mine[...]) + dot(o_other[...], w_other[...])).astype(BF16)


def out_rows(core, o_mine, o_other, wo):
    rows, half, model, tile = 512, o_mine.shape[1], wo.shape[1], 256
    return pl.pallas_call(
        y_kernel,
        out_shape=jax.ShapeDtypeStruct((rows, model), BF16),
        grid_spec=pltpu.PrefetchScalarGridSpec(
            num_scalar_prefetch=1,
            grid=(model // tile,),
            in_specs=[
                pl.BlockSpec((rows, half), lambda i, s: (s[0], 0)),
                pl.BlockSpec((rows, half), lambda i, s: (s[0], 0)),
                pl.BlockSpec((half, tile), lambda i, s: (s[0], i)),
                pl.BlockSpec((half, tile), lambda i, s: (1 - s[0], i)),
            ],
            out_specs=pl.BlockSpec((rows, tile), lambda i, s: (0, i)),
        ),
        compiler_params=params(),
        cost_estimate=cost(4 * rows * half * model, 12e6),
    )(core, o_mine, o_other, wo, wo)


def dx_kernel(sc, q_mine, q_other, kv_mine, kv_other, wq_mine, wq_other, wk_mine, wk_other, wv_mine, wv_other, out_ref):
    hd = 128
    acc = dot_nt(q_mine[...], wq_mine[...]) + dot_nt(q_other[...], wq_other[...])
    acc += dot_nt(kv_mine[:, :hd], wk_mine[...]) + dot_nt(kv_other[:, :hd], wk_other[...])
    acc += dot_nt(kv_mine[:, hd:], wv_mine[...]) + dot_nt(kv_other[:, hd:], wv_other[...])
    out_ref[...] = acc.astype(BF16)


def grad_rows(core, dq_mine, dq_other, dkv_mine, dkv_other, wq, wk, wv):
    rows, half, model, tile = 512, dq_mine.shape[1], wq.shape[0], 256
    mine = lambda i, s: (s[0], 0)
    return pl.pallas_call(
        dx_kernel,
        out_shape=jax.ShapeDtypeStruct((rows, model), BF16),
        grid_spec=pltpu.PrefetchScalarGridSpec(
            num_scalar_prefetch=1,
            grid=(model // tile,),
            in_specs=[
                pl.BlockSpec((rows, half), mine),
                pl.BlockSpec((rows, half), mine),
                pl.BlockSpec((rows, 256), mine),
                pl.BlockSpec((rows, 256), mine),
                pl.BlockSpec((tile, half), lambda i, s: (i, s[0])),
                pl.BlockSpec((tile, half), lambda i, s: (i, 1 - s[0])),
                pl.BlockSpec((tile, 128), lambda i, s: (i, s[0])),
                pl.BlockSpec((tile, 128), lambda i, s: (i, 1 - s[0])),
                pl.BlockSpec((tile, 128), lambda i, s: (i, s[0])),
                pl.BlockSpec((tile, 128), lambda i, s: (i, 1 - s[0])),
            ],
            out_specs=pl.BlockSpec((rows, tile), lambda i, s: (0, i)),
        ),
        compiler_params=params(),
        cost_estimate=cost(4 * rows * half * model * 1.25, 14e6),
    )(core, dq_mine, dq_other, dkv_mine, dkv_other, wq, wq, wk, wk, wv, wv)


def piece_specs(width, s_col):
    flips = (0, 1, 0, 1, 0, 1)
    return [
        pl.BlockSpec((512 if n < 2 else 256, width), lambda g, i, s, f=f: (1 - s[0] if f else s[0], s_col(g, i)))
        for n, f in enumerate(flips)
    ]


def dwq_kernel(sc, *refs):
    xs_in, mine, other, kvm, kvo = refs[:6], refs[6:12], refs[12:18], refs[18:24], refs[24:30]
    out_ref, gk_ref, gv_ref = refs[30:33]
    g = pl.program_id(0)
    tile = out_ref.shape[0]

    def store(rhs):
        acc = sum(dot(x[...].T, q[...]) for x, q in zip(xs_in, rhs))
        flat = out_ref.reshape(tile * 8, 128)
        for h in range(8):
            flat[pl.ds(h, tile, stride=8), :] = acc[:, h * 128 : (h + 1) * 128]

    @pl.when(g == 0)
    def _():
        store(mine)

    @pl.when(g == 1)
    def _():
        store(other)
        core = sc[0]
        k_flat, v_flat = gk_ref.reshape(tile * 2, 128), gv_ref.reshape(tile * 2, 128)
        for src, head in ((kvm, core), (kvo, 1 - core)):
            acc = sum(dot(x[...].T, k[...]) for x, k in zip(xs_in, src))
            k_flat[pl.ds(head, tile, stride=2), :] = acc[:, :128]
            v_flat[pl.ds(head, tile, stride=2), :] = acc[:, 128:]


def grad_wq(core, xs, mine, other, kvm, kvo):
    model, half, tile = xs[0].shape[1], mine[0].shape[1], 256
    x_specs = [pl.BlockSpec((x.shape[0], tile), lambda g, i, s: (0, i)) for x in xs]
    q_specs = piece_specs(half, lambda g, i: 0)
    kv_at = ((0, 512, 0), (1, 512, 0), (0, 256, 4), (1, 256, 4), (0, 256, 6), (1, 256, 6))
    kv_specs = [
        pl.BlockSpec((r, 256), lambda g, i, s, f=f, base=base: (base + (1 - s[0] if f else s[0]), 0))
        for f, r, base in kv_at
    ]
    ex = lambda t: [t[0], t[0], t[1], t[1], t[2], t[2]]
    small = pl.BlockSpec((tile, 2, 128), lambda g, i, s: (i * g, 0, 0))
    return pl.pallas_call(
        dwq_kernel,
        out_shape=(
            jax.ShapeDtypeStruct((model, 16, 128), F32),
            jax.ShapeDtypeStruct((model, 2, 128), F32),
            jax.ShapeDtypeStruct((model, 2, 128), F32),
        ),
        grid_spec=pltpu.PrefetchScalarGridSpec(
            num_scalar_prefetch=1,
            grid=(2, model // tile),
            in_specs=x_specs + q_specs + q_specs + kv_specs + kv_specs,
            out_specs=(
                pl.BlockSpec((tile, 8, 128), lambda g, i, s: (i, (s[0] + g) % 2, 0)),
                small,
                small,
            ),
        ),
        compiler_params=params(2),
        cost_estimate=cost(2 * 2048 * model * (2 * half + 512), 40e6),
    )(core, *xs, *ex(mine), *ex(other), *([kvm] * 6), *([kvo] * 6))


def dwo_kernel(sc, *refs):
    mine, other, ys, out_ref = refs[:6], refs[6:12], refs[12:18], refs[18]
    g = pl.program_id(0)

    def store(lhs):
        out_ref[...] = sum(dot(o[...].T, y[...]) for o, y in zip(lhs, ys))

    @pl.when(g == 0)
    def _():
        store(mine)

    @pl.when(g == 1)
    def _():
        store(other)


def grad_wo(core, ys, mine, other):
    model, half, tile = ys[0].shape[1], mine[0].shape[1], 256
    steps = half // tile
    specs = piece_specs(tile, lambda g, i: jnp.where(g == 0, i, steps - 1))
    specs += piece_specs(tile, lambda g, i: jnp.where(g == 0, 0, i))
    specs += [pl.BlockSpec(y.shape, lambda g, i, s: (0, 0)) for y in ys]
    ex = lambda t: [t[0], t[0], t[1], t[1], t[2], t[2]]
    return pl.pallas_call(
        dwo_kernel,
        out_shape=jax.ShapeDtypeStruct((2 * half, model), F32),
        grid_spec=pltpu.PrefetchScalarGridSpec(
            num_scalar_prefetch=1,
            grid=(2, steps),
            in_specs=specs,
            out_specs=pl.BlockSpec((tile, model), lambda g, i, s: ((s[0] + g) % 2 * steps + i, 0)),
        ),
        compiler_params=params(2),
        cost_estimate=cost(4 * 2048 * model * half, 40e6),
    )(core, *ex(mine), *ex(other), *ys)


def solution(mesh):
    row_spec = P(("dp", "cp"), None)
    rep_spec = P(None, None, None)
    part_spec = P("dp", None, None)
    core_swap = [(0, 1), (1, 0), (2, 3), (3, 2)]
    chip_swap = [(0, 2), (2, 0), (1, 3), (3, 1)]

    def device_layer(x, dy, w_query, w_key, w_value, w_out):
        rows, model = x.shape
        num_heads, hd = w_query.shape[1:]
        kv_heads = w_key.shape[1]
        scale = hd ** -0.5
        rank = lax.axis_index("cp").astype(jnp.int32)
        c = rank & 1
        core = c.reshape(1)
        devs = [rank, rank ^ 1, rank ^ 2, rank ^ 3]
        kv_pos = [p for e in devs for p in (e, 7 - e)]
        own_slots = [p for e in devs[:2] for p in ((e & 1) * 2, (e & 1) * 2 + 1)]
        far_slots = []
        for e in devs[2:]:
            far_slots += [jnp.where((e & 1) == 1, 4, 6) + (e & 1), jnp.where((e & 1) == 0, 4, 6) + (e & 1)]
        pos_a = [jnp.where((e & 1) == 0, 7 - e, e) for e in devs[2:]]
        pos_b = [jnp.where((e & 1) == 0, e, 7 - e) for e in devs[2:]]
        far = [c, 1 - c]
        tail = own_slots + far_slots + [c]
        sc_chip = jnp.stack(kv_pos + kv_pos[:4] + own_slots + tail)
        sc_a = jnp.stack(kv_pos + pos_a * 2 + far * 2 + tail)
        sc_b = jnp.stack(kv_pos + pos_b * 2 + far * 2 + tail)

        to_core = lambda v: lax.ppermute(v, "cp", core_swap)
        to_chip = lambda v: lax.ppermute(v, "cp", chip_swap)

        wk = w_key.reshape(model, kv_heads * hd)
        wv = w_value.reshape(model, kv_heads * hd)
        wo = w_out.reshape(num_heads * hd, model)
        x_p = to_core(x)
        dy_p = to_core(dy)

        kv = project_kv(x, wk, wv)
        kv_r = to_chip(kv)
        kv_p = to_core(kv)
        x_s, dy_s, w_s, _ = lax.optimization_barrier((x, dy, w_query, kv))
        cut = lambda v, at: lax.dynamic_slice(v, (at * BLK, 0), (BLK, model))
        x_a = to_chip(cut(x_s, 1 - c))
        dy_a = to_chip(cut(dy_s, 1 - c))
        x_b = to_chip(cut(x_s, c))
        dy_b = to_chip(cut(dy_s, c))
        kv_rp = to_core(kv_r)
        wq = flat_heads(w_s)
        pieces = (kv, kv_p, kv_r, kv_rp)
        q = project(core, (x, x_p), wq, 1024, False)
        do = project(core, (dy, dy_p), wo, 1024, True)
        o_c, dq_c, part = attention(sc_chip, q, do, pieces, None, False, scale)
        x_a, dy_a, o_c, dq_c = lax.optimization_barrier((x_a, dy_a, o_c, dq_c))
        x_pa, dy_pa, o_co, dq_co = to_core(x_a), to_core(dy_a), to_core(o_c), to_core(dq_c)

        q = project(core, (x_a, x_pa), wq, 1024, False)
        do = project(core, (dy_a, dy_pa), wo, 1024, True)
        o_a, dq_a, part = attention(sc_a, q, do, pieces, part, False, scale)
        x_b, dy_b, o_a, dq_a = lax.optimization_barrier((x_b, dy_b, o_a, dq_a))
        x_pb, dy_pb, o_ao, dq_ao = to_core(x_b), to_core(dy_b), to_core(o_a), to_core(dq_a)

        q = project(core, (x_b, x_pb), wq, 1024, False)
        do = project(core, (dy_b, dy_pb), wo, 1024, True)
        o_b, dq_b, dkv = attention(sc_b, q, do, pieces, part, True, scale)
        o_co, dkv = lax.optimization_barrier((o_co, dkv))
        dkv_o, o_bo, dq_bo = to_core(dkv), to_core(o_b), to_core(dq_b)
        y = out_rows(core, o_c, o_co, wo)

        xs = (x, x_p, x_a, x_pa, x_b, x_pb)
        ys = (dy, dy_p, dy_a, dy_pa, dy_b, dy_pb)
        gwo = grad_wo(core, ys, (o_c, o_a, o_b), (o_co, o_ao, o_bo))
        dx = grad_rows(core, dq_c, dq_co, dkv, dkv_o, wq, wk, wv)
        gwq, gwk, gwv = grad_wq(core, xs, (dq_c, dq_a, dq_b), (dq_co, dq_ao, dq_bo), dkv, dkv_o)
        return y, dx, gwq, gwk, gwv, gwo.reshape(num_heads, hd, model)

    return jax.shard_map(
        device_layer,
        mesh=mesh,
        in_specs=(row_spec, row_spec, rep_spec, rep_spec, rep_spec, rep_spec),
        out_specs=(row_spec, row_spec, part_spec, part_spec, part_spec, part_spec),
        check_vma=False,
    )
```

```python
import functools
import math

import jax
import jax.numpy as jnp
from jax import lax
from jax.experimental import pallas as pl
from jax.experimental.pallas import tpu as pltpu
from jax.sharding import PartitionSpec as P

BLK = 256
LOW = -3.0e38
F32 = jnp.float32
BF16 = jnp.bfloat16


def dot(a, b):
    return jnp.dot(a, b, preferred_element_type=F32)


def dot_nt(a, b):
    return lax.dot_general(a, b, (((1,), (1,)), ((), ())), preferred_element_type=F32)


def params(n=1, mib=60):
    return pltpu.CompilerParams(
        dimension_semantics=("arbitrary",) * n, vmem_limit_bytes=mib * 1024 * 1024
    )


def cost(flops, nbytes):
    return pl.CostEstimate(flops=int(flops), bytes_accessed=int(nbytes), transcendentals=0)


def heads_kernel(w_ref, perm_ref, out_ref):
    rows, num, hd = w_ref.shape
    flat = w_ref.reshape(rows * num, hd)
    group = num * 16
    for g in range(0, rows // 16, 2):
        pair = [flat[(g + n) * group : (g + n + 1) * group, :] for n in range(2)]
        res = dot(perm_ref[...], jnp.concatenate(pair, axis=1)).astype(BF16)
        for n in range(2):
            for h in range(num):
                out_ref[(g + n) * 16 : (g + n + 1) * 16, h * hd : (h + 1) * hd] = res[
                    h * 16 : (h + 1) * 16, n * hd : (n + 1) * hd
                ]


def flat_heads(w):
    model, num, hd = w.shape
    tile = 256
    row = jnp.arange(num * 16)
    perm = ((row % 16 * num + row // 16)[:, None] == row[None, :]).astype(BF16)
    return pl.pallas_call(
        heads_kernel,
        out_shape=jax.ShapeDtypeStruct((model, num * hd), BF16),
        grid=(model // tile,),
        in_specs=[
            pl.BlockSpec((tile, num, hd), lambda i: (i, 0, 0)),
            pl.BlockSpec((num * 16, num * 16), lambda i: (0, 0)),
        ],
        out_specs=pl.BlockSpec((tile, num * hd), lambda i: (i, 0)),
        compiler_params=params(),
        cost_estimate=cost(4e9, 4 * model * num * hd),
    )(w, perm)


def kv_kernel(sc, x_ref, dy_ref, wk_ref, wv_ref, out_ref, xa, xb, dya, dyb):
    out_ref[:, :256] = dot(x_ref[...], wk_ref[...]).astype(BF16)
    out_ref[:, 256:] = dot(x_ref[...], wv_ref[...]).astype(BF16)

    @pl.when(pl.program_id(0) == 1 - sc[0])
    def _():
        xa[...] = x_ref[...]
        dya[...] = dy_ref[...]

    @pl.when(pl.program_id(0) == sc[0])
    def _():
        xb[...] = x_ref[...]
        dyb[...] = dy_ref[...]


def project_kv(core, x, dy, wk, wv):
    rows, depth = x.shape
    row = pl.BlockSpec((BLK, depth), lambda i, s: (i, 0))
    fixed = lambda shape: pl.BlockSpec(shape, lambda i, s: (0, 0))
    half = jax.ShapeDtypeStruct((BLK, depth), BF16)
    return pl.pallas_call(
        kv_kernel,
        out_shape=(jax.ShapeDtypeStruct((rows, 512), BF16), half, half, half, half),
        grid_spec=pltpu.PrefetchScalarGridSpec(
            num_scalar_prefetch=1,
            grid=(rows // BLK,),
            in_specs=[row, row, fixed((depth, 256)), fixed((depth, 256))],
            out_specs=(pl.BlockSpec((BLK, 512), lambda i, s: (i, 0)),) + (fixed((BLK, depth)),) * 4,
        ),
        compiler_params=params(),
        cost_estimate=cost(2 * rows * depth * 512, 8e6),
    )(core, x, dy, wk, wv)


def attn_kernel(heads, scale, first, final, sc, wq_hbm, wo_hbm, *refs):
    x_hbm, dy_hbm, kv_refs, refs = refs[:2], refs[2:4], refs[4:12], refs[12:]
    if first:
        o_ref, dq_ref, dkv_ref = refs[:3]
        scratch = refs[3:]
    else:
        init_ref, o_ref, dq_ref, dkv_ref = refs[:4]
        scratch = refs[4:]
    ks, vs, kt, vt, dk, dv, qt, dot_t, qst, dost, s_ref, p_ref, ds_ref, ot, dqt, m_ref, l_ref, wq, wo, xs, dys, w_sem, x_sem, dy_sem = scratch
    step = pl.program_id(0)
    wide = heads * BLK
    hd = 128
    c2 = scale * math.log2(math.e)

    steps = 2 * x_hbm[0].shape[0] // BLK
    core = pl.multiple_of(sc[24] * heads * hd, heads * hd)
    load_wq = pltpu.make_async_copy(wq_hbm.at[:, pl.ds(core, heads * hd)], wq, w_sem.at[0])
    load_wo = pltpu.make_async_copy(wo_hbm.at[pl.ds(core, heads * hd), :], wo, w_sem.at[1])

    def load_rows(n):
        piece, row = divmod(n, steps // 2)
        src = pl.ds(row * BLK, BLK)
        return (
            pltpu.make_async_copy(x_hbm[piece].at[src, :], xs.at[n % 2], x_sem.at[n % 2]),
            pltpu.make_async_copy(dy_hbm[piece].at[src, :], dys.at[n % 2], dy_sem.at[n % 2]),
        )

    @pl.when(step == 0)
    def _():
        load_x, load_dy = load_rows(0)
        load_x.start()
        load_wq.start()
        load_dy.start()
        load_wo.start()

    for n in range(1, steps):

        @pl.when(step == n - 1)
        def _():
            for cp in load_rows(n):
                cp.start()

    @pl.when(step == 0)
    def _():
        for i in range(8):
            rows = slice((i % 2) * BLK, (i % 2 + 1) * BLK)
            at = pl.ds(pl.multiple_of(sc[i] * BLK, BLK), BLK)
            kk, vv = kv_refs[i // 2][rows, :], kv_refs[4 + i // 2][rows, :]
            ks[at, :] = kk
            vs[at, :] = vv
            kt[:, at] = kk.T
            vt[:, at] = vv.T
            if not first:
                init_rows = slice(i * BLK, (i + 1) * BLK)
                dk[at, :] = init_ref[init_rows, :hd]
                dv[at, :] = init_ref[init_rows, hd:]
            else:
                dk[at, :] = jnp.zeros((BLK, hd), F32)
                dv[at, :] = jnp.zeros((BLK, hd), F32)

    @pl.when(step == 0)
    def _():
        load_wq.wait()

    slot = step % 2
    pltpu.make_async_copy(x_hbm[0].at[0:BLK, :], xs.at[slot], x_sem.at[slot]).wait()
    q = dot(xs[slot], wq[...]).astype(BF16)
    for h in range(heads):
        qh = q[:, h * hd : (h + 1) * hd]
        qst[h * BLK : (h + 1) * BLK, :] = qh
        qt[:, h * BLK : (h + 1) * BLK] = qh.T

    @pl.when(step == 0)
    def _():
        load_wo.wait()

    pltpu.make_async_copy(dy_hbm[0].at[0:BLK, :], dys.at[slot], dy_sem.at[slot]).wait()
    do = dot_nt(dys[slot], wo[...]).astype(BF16)
    for h in range(heads):
        dh = do[:, h * hd : (h + 1) * hd]
        dost[h * BLK : (h + 1) * BLK, :] = dh
        dot_t[:, h * BLK : (h + 1) * BLK] = dh.T

    b = sc[8 + step]

    def softmax_block(j, masked):
        at = pl.ds(pl.multiple_of(j * BLK, BLK), BLK)
        for h in range(heads):
            span = slice(h * BLK, (h + 1) * BLK)
            t = dot(ks[at, :], qt[:, span]) * c2
            if masked:
                key = lax.broadcasted_iota(jnp.int32, (BLK, BLK), 0)
                query = lax.broadcasted_iota(jnp.int32, (BLK, BLK), 1)
                t = jnp.where(key <= query, t, LOW)
            s_ref[at, span] = t
            m8 = m_ref[:, span]
            new = jnp.maximum(m8, jnp.max(t.reshape(BLK // 8, 8, BLK), axis=0))
            e = jnp.exp2(s_ref[at, span].reshape(BLK // 8, 8, BLK) - new[None])
            l_ref[:, span] = l_ref[:, span] * jnp.exp2(m8 - new) + jnp.sum(e, axis=0)
            m_ref[:, span] = new

    m_ref[...] = jnp.full((8, wide), LOW, F32)
    l_ref[...] = jnp.zeros((8, wide), F32)

    def open_block(j, _):
        softmax_block(j, False)
        return 0

    lax.fori_loop(0, b, open_block, 0)
    softmax_block(b, True)
    m8 = m_ref[...]
    top = jnp.max(m8, axis=0, keepdims=True)
    lse = top + jnp.log2(jnp.sum(l_ref[...] * jnp.exp2(m8 - top), axis=0, keepdims=True))

    ot[...] = jnp.zeros_like(ot)

    def value_block(j, _):
        at = pl.ds(pl.multiple_of(j * BLK, BLK), BLK)
        for h in range(heads):
            span = slice(h * BLK, (h + 1) * BLK)
            p = jnp.exp2(s_ref[at, span] - lse[:, span]).astype(BF16)
            p_ref[at, span] = p
            ot[:, span] += dot(vt[:, at], p)
        return 0

    lax.fori_loop(0, b + 1, value_block, 0)

    o_round = ot[...].astype(BF16)
    delta = jnp.sum(o_round.astype(F32) * dot_t[...].astype(F32), axis=0, keepdims=True)
    for h in range(heads):
        o_ref[h * hd : (h + 1) * hd, :] = o_round[:, h * BLK : (h + 1) * BLK]
    dqt[...] = jnp.zeros_like(dqt)

    def grad_block(j, _):
        at = pl.ds(pl.multiple_of(j * BLK, BLK), BLK)
        dp = dot(vs[at, :], dot_t[...])
        dv[at, :] += dot(p_ref[at, :], dost[...])
        ds = (p_ref[at, :].astype(F32) * (dp - delta)).astype(BF16)
        ds_ref[...] = ds
        dqt[...] += dot(kt[:, at], ds_ref[...])
        dk[at, :] += dot(ds_ref[...], qst[...])
        return 0

    lax.fori_loop(0, b + 1, grad_block, 0)

    for h in range(heads):
        dq_ref[:, h * hd : (h + 1) * hd] = (dqt[:, h * BLK : (h + 1) * BLK] * scale).astype(BF16).T

    @pl.when(step == pl.num_programs(0) - 1)
    def _():
        for i in range(8):
            at = pl.ds(pl.multiple_of(sc[i] * BLK, BLK), BLK)
            if final:
                out = pl.ds(pl.multiple_of(sc[16 + i] * BLK, BLK), BLK)
                dkv_ref[out, :hd] = (dk[at, :] * scale).astype(BF16)
                dkv_ref[out, hd:] = dv[at, :].astype(BF16)
            else:
                out = slice(i * BLK, (i + 1) * BLK)
                dkv_ref[out, :hd] = dk[at, :]
                dkv_ref[out, hd:] = dv[at, :]


def attention(sc, wq, wo, x_pieces, dy_pieces, kv_pieces, init, final, scale):
    first = init is None
    rows, width, model = 2 * x_pieces[0].shape[0], wq.shape[1] // 2, wq.shape[0]
    hd = 128
    heads = width // hd
    wide = heads * BLK
    seq = 2048
    o_spec = pl.BlockSpec((width, BLK), lambda i, s: (0, s[12 + i]))
    out_spec = pl.BlockSpec((BLK, width), lambda i, s: (s[12 + i], 0))
    full = lambda shape: pl.BlockSpec(shape, lambda i, s: (0, 0), pipeline_mode=pl.Buffered(1))
    ins = [wq, wo, *x_pieces, *dy_pieces] + list(kv_pieces) * 2 + ([] if first else [init])
    in_specs = [pl.BlockSpec(memory_space=pl.ANY)] * 6
    in_specs += [pl.BlockSpec((2 * BLK, hd), lambda i, s: (0, s[24]))] * 4
    in_specs += [pl.BlockSpec((2 * BLK, hd), lambda i, s: (0, 2 + s[24]))] * 4
    if not first:
        in_specs.append(full(init.shape))
    return pl.pallas_call(
        functools.partial(attn_kernel, heads, scale, first, final),
        out_shape=(
            jax.ShapeDtypeStruct((width, rows), BF16),
            jax.ShapeDtypeStruct((rows, width), BF16),
            jax.ShapeDtypeStruct((seq, 256), BF16 if final else F32),
        ),
        grid_spec=pltpu.PrefetchScalarGridSpec(
            num_scalar_prefetch=1,
            grid=(rows // BLK,),
            in_specs=in_specs,
            out_specs=(o_spec, out_spec, full((seq, 256))),
            scratch_shapes=[
                *[pltpu.VMEM((seq, hd), BF16) for _ in "kv"],
                *[pltpu.VMEM((hd, seq), BF16) for _ in "kv"],
                *[pltpu.VMEM((seq, hd), F32) for _ in "kv"],
                *[pltpu.VMEM((hd, wide), BF16) for _ in "qd"],
                *[pltpu.VMEM((wide, hd), BF16) for _ in "qd"],
                pltpu.VMEM((seq, wide), F32),
                pltpu.VMEM((seq, wide), BF16),
                pltpu.VMEM((BLK, wide), BF16),
                *[pltpu.VMEM((hd, wide), F32) for _ in "od"],
                *[pltpu.VMEM((8, wide), F32) for _ in "ml"],
                pltpu.VMEM((model, width), BF16),
                pltpu.VMEM((width, model), BF16),
                *[pltpu.VMEM((2, BLK, model), BF16) for _ in "xd"],
                *[pltpu.SemaphoreType.DMA((2,)) for _ in "wxd"],
            ],
        ),
        compiler_params=params(1, 63),
        cost_estimate=cost(8e9 * (rows // BLK), 20e6),
    )(sc, *ins)


def y_kernel(sc, o_mine, o_other, w_mine, w_other, out_ref, os):
    half = o_mine.shape[0]

    @pl.when(pl.program_id(0) == 0)
    def _():
        os[:, :half] = o_mine[...].T
        os[:, half:] = o_other[...].T

    out_ref[...] = (dot(os[:, :half], w_mine[...]) + dot(os[:, half:], w_other[...])).astype(BF16)


def out_rows(core, o_mine, o_other, wo):
    rows, half, model, tile = 512, o_mine.shape[0], wo.shape[1], 512
    return pl.pallas_call(
        y_kernel,
        out_shape=jax.ShapeDtypeStruct((rows, model), BF16),
        grid_spec=pltpu.PrefetchScalarGridSpec(
            num_scalar_prefetch=1,
            grid=(model // tile,),
            in_specs=[
                pl.BlockSpec((half, rows), lambda i, s: (0, s[0])),
                pl.BlockSpec((half, rows), lambda i, s: (0, s[0])),
                pl.BlockSpec((half, tile), lambda i, s: (s[0], i)),
                pl.BlockSpec((half, tile), lambda i, s: (1 - s[0], i)),
            ],
            out_specs=pl.BlockSpec((rows, tile), lambda i, s: (0, i)),
            scratch_shapes=[pltpu.VMEM((rows, 2 * half), BF16)],
        ),
        compiler_params=params(),
        cost_estimate=cost(4 * rows * half * model, 12e6),
    )(core, o_mine, o_other, wo, wo)


def dx_kernel(sc, q_mine, q_other, kv_mine, kv_other, wq_mine, wq_other, wk_mine, wk_other, wv_mine, wv_other, out_ref):
    kv = jnp.concatenate([kv_mine[...], kv_other[...]], axis=1)
    w = jnp.concatenate([wk_mine[...], wv_mine[...], wk_other[...], wv_other[...]], axis=1)
    acc = dot_nt(q_mine[...], wq_mine[...]) + dot_nt(q_other[...], wq_other[...])
    out_ref[...] = (acc + dot_nt(kv, w)).astype(BF16)


def grad_rows(core, dq_mine, dq_other, dkv_mine, dkv_other, wq, wk, wv):
    rows, half, model, tile = 512, dq_mine.shape[1], wq.shape[0], 512
    hd = 128
    mine = lambda i, s: (s[0], 0)
    near, far = lambda i, s: (i, s[0]), lambda i, s: (i, 1 - s[0])
    return pl.pallas_call(
        dx_kernel,
        out_shape=jax.ShapeDtypeStruct((rows, model), BF16),
        grid_spec=pltpu.PrefetchScalarGridSpec(
            num_scalar_prefetch=1,
            grid=(model // tile,),
            in_specs=[
                *[pl.BlockSpec((rows, n), mine) for n in (half, half, 2 * hd, 2 * hd)],
                *[pl.BlockSpec((tile, n), at) for n in (half, hd, hd) for at in (near, far)],
            ],
            out_specs=pl.BlockSpec((rows, tile), lambda i, s: (0, i)),
        ),
        compiler_params=params(),
        cost_estimate=cost(4 * rows * half * model * 1.25, 14e6),
    )(core, dq_mine, dq_other, dkv_mine, dkv_other, wq, wq, wk, wk, wv, wv)


PIECES = ((0, 512), (1, 512), (0, 256), (1, 256), (0, 256), (1, 256))
STARTS = (0, 512, 1024, 1280, 1536, 1792)


def dwq_kernel(sc, *refs):
    xs_in, mine, other, kvm, kvo = refs[:6], refs[6:12], refs[12:18], refs[18:24], refs[24:30]
    out_ref, gk_ref, gv_ref, xt = refs[30:34]
    g, i = pl.program_id(0), pl.program_id(1)
    tile = out_ref.shape[0]

    def part(rhs):
        return sum(dot(xt[i, :, s : s + n], r[...]) for s, (_, n), r in zip(STARTS, PIECES, rhs))

    def store(rhs):
        acc = part(rhs)
        flat = out_ref.reshape(tile * 8, 128)
        for h in range(8):
            flat[pl.ds(h, tile, stride=8), :] = acc[:, h * 128 : (h + 1) * 128]

    @pl.when(g == 0)
    def _():
        for s, (_, n), x in zip(STARTS, PIECES, xs_in):
            xt[i, :, s : s + n] = x[...].T
        store(mine)

    @pl.when(g == 1)
    def _():
        store(other)
        core = sc[0]
        k_flat, v_flat = gk_ref.reshape(tile * 2, 128), gv_ref.reshape(tile * 2, 128)
        for src, head in ((kvm, core), (kvo, 1 - core)):
            acc = part(src)
            k_flat[pl.ds(head, tile, stride=2), :] = acc[:, :128]
            v_flat[pl.ds(head, tile, stride=2), :] = acc[:, 128:]


def grad_wq(core, xs, mine, other, kvm, kvo):
    model, half, tile = xs[0].shape[1], mine[0].shape[1], 256
    tiles = model // tile
    x_specs = [pl.BlockSpec((n, tile), lambda g, i, s: (0, jnp.where(g == 0, i, tiles - 1))) for _, n in PIECES]
    q_specs = [pl.BlockSpec((n, half), lambda g, i, s, f=f: (1 - s[0] if f else s[0], 0)) for f, n in PIECES]
    kv_specs = [
        pl.BlockSpec((n, 256), lambda g, i, s, f=f, at=at: (at + (1 - s[0] if f else s[0]), 0))
        for (f, n), at in zip(PIECES, (0, 0, 4, 4, 6, 6))
    ]
    ex = lambda t: [t[0], t[0], t[1], t[1], t[2], t[2]]
    small = pl.BlockSpec((tile, 2, 128), lambda g, i, s: (i * g, 0, 0))
    return pl.pallas_call(
        dwq_kernel,
        out_shape=(
            jax.ShapeDtypeStruct((model, 16, 128), F32),
            jax.ShapeDtypeStruct((model, 2, 128), F32),
            jax.ShapeDtypeStruct((model, 2, 128), F32),
        ),
        grid_spec=pltpu.PrefetchScalarGridSpec(
            num_scalar_prefetch=1,
            grid=(2, tiles),
            in_specs=x_specs + q_specs + q_specs + kv_specs + kv_specs,
            out_specs=(
                pl.BlockSpec((tile, 8, 128), lambda g, i, s: (i, (s[0] + g) % 2, 0)),
                small,
                small,
            ),
            scratch_shapes=[pltpu.VMEM((tiles, tile, 2048), BF16)],
        ),
        compiler_params=params(2),
        cost_estimate=cost(2 * 2048 * model * (2 * half + 512), 40e6),
    )(core, *xs, *ex(mine), *ex(other), *([kvm] * 6), *([kvo] * 6))


def dwo_kernel(sc, *refs):
    mine, other, ys, out_ref = refs[:6], refs[6:12], refs[12:18], refs[18]

    def store(lhs):
        out_ref[...] = sum(dot(o[...], y[...]) for o, y in zip(lhs, ys))

    @pl.when(pl.program_id(1) == 0)
    def _():
        store(mine)

    @pl.when(pl.program_id(1) == 1)
    def _():
        store(other)


def grad_wo(core, ys, mine, other):
    model, half, tile, wide = ys[0].shape[1], mine[0].shape[0], 512, 1024
    steps = half // tile
    specs = []
    for rest in (0, 1):
        specs += [
            pl.BlockSpec(
                (tile, n),
                lambda j, g, i, s, f=f, rest=rest: (
                    jnp.where(g == rest, i, 0 if rest else steps - 1),
                    1 - s[0] if f else s[0],
                ),
            )
            for f, n in PIECES
        ]
    specs += [pl.BlockSpec((n, wide), lambda j, g, i, s: (0, j)) for _, n in PIECES]
    ex = lambda t: [t[0], t[0], t[1], t[1], t[2], t[2]]
    return pl.pallas_call(
        dwo_kernel,
        out_shape=jax.ShapeDtypeStruct((2 * half, model), F32),
        grid_spec=pltpu.PrefetchScalarGridSpec(
            num_scalar_prefetch=1,
            grid=(model // wide, 2, steps),
            in_specs=specs,
            out_specs=pl.BlockSpec((tile, wide), lambda j, g, i, s: ((s[0] + g) % 2 * steps + i, j)),
        ),
        compiler_params=params(3),
        cost_estimate=cost(4 * 2048 * model * half, 40e6),
    )(core, *ex(mine), *ex(other), *ys)


def solution(mesh):
    row_spec = P(("dp", "cp"), None)
    rep_spec = P(None, None, None)
    part_spec = P("dp", None, None)
    core_swap = [(0, 1), (1, 0), (2, 3), (3, 2)]
    chip_swap = [(0, 2), (2, 0), (1, 3), (3, 1)]

    def device_layer(x, dy, w_query, w_key, w_value, w_out):
        rows, model = x.shape
        num_heads, hd = w_query.shape[1:]
        kv_heads = w_key.shape[1]
        scale = hd ** -0.5
        rank = lax.axis_index("cp").astype(jnp.int32)
        c = rank & 1
        core = c.reshape(1)
        devs = [rank, rank ^ 1, rank ^ 2, rank ^ 3]
        kv_pos = [p for e in devs for p in (e, 7 - e)]
        own_slots = [p for e in devs[:2] for p in ((e & 1) * 2, (e & 1) * 2 + 1)]
        far_slots = []
        for e in devs[2:]:
            far_slots += [jnp.where((e & 1) == 1, 4, 6) + (e & 1), jnp.where((e & 1) == 0, 4, 6) + (e & 1)]
        pos_a = [jnp.where((e & 1) == 0, 7 - e, e) for e in devs[2:]]
        pos_b = [jnp.where((e & 1) == 0, e, 7 - e) for e in devs[2:]]
        far = [c, 1 - c]
        tail = own_slots + far_slots + [c]
        sc_chip = jnp.stack(kv_pos + kv_pos[:4] + own_slots + tail)
        sc_a = jnp.stack(kv_pos + pos_a * 2 + far * 2 + tail)
        sc_b = jnp.stack(kv_pos + pos_b * 2 + far * 2 + tail)

        to_core = lambda v: lax.ppermute(v, "cp", core_swap)
        to_chip = lambda v: lax.ppermute(v, "cp", chip_swap)

        wk = w_key.reshape(model, kv_heads * hd)
        wv = w_value.reshape(model, kv_heads * hd)
        wo = w_out.reshape(num_heads * hd, model)
        x_p = to_core(x)
        dy_p = to_core(dy)

        kv, x_a, x_b, dy_a, dy_b = project_kv(core, x, dy, wk, wv)
        kv_r, kv_p = to_chip(kv), to_core(kv)
        w_s, _ = lax.optimization_barrier((w_query, kv))
        x_a, dy_a, x_b, dy_b = to_chip(x_a), to_chip(dy_a), to_chip(x_b), to_chip(dy_b)
        wq = flat_heads(w_s)
        kv_rp = to_core(kv_r)
        pieces = (kv, kv_p, kv_r, kv_rp)

        o_c, dq_c, part = attention(sc_chip, wq, wo, (x, x_p), (dy, dy_p), pieces, None, False, scale)
        x_a, dy_a, o_c, dq_c = lax.optimization_barrier((x_a, dy_a, o_c, dq_c))
        x_pa, dy_pa, o_co, dq_co = to_core(x_a), to_core(dy_a), to_core(o_c), to_core(dq_c)

        o_a, dq_a, part = attention(sc_a, wq, wo, (x_a, x_pa), (dy_a, dy_pa), pieces, part, False, scale)
        x_b, dy_b, o_a, dq_a = lax.optimization_barrier((x_b, dy_b, o_a, dq_a))
        x_pb, dy_pb, o_ao, dq_ao = to_core(x_b), to_core(dy_b), to_core(o_a), to_core(dq_a)

        o_b, dq_b, dkv = attention(sc_b, wq, wo, (x_b, x_pb), (dy_b, dy_pb), pieces, part, True, scale)
        o_co, dkv = lax.optimization_barrier((o_co, dkv))
        dkv_o, o_bo, dq_bo = to_core(dkv), to_core(o_b), to_core(dq_b)
        y = out_rows(core, o_c, o_co, wo)

        xs = (x, x_p, x_a, x_pa, x_b, x_pb)
        ys = (dy, dy_p, dy_a, dy_pa, dy_b, dy_pb)
        gwo = grad_wo(core, ys, (o_c, o_a, o_b), (o_co, o_ao, o_bo))
        dx = grad_rows(core, dq_c, dq_co, dkv, dkv_o, wq, wk, wv)
        gwq, gwk, gwv = grad_wq(core, xs, (dq_c, dq_a, dq_b), (dq_co, dq_ao, dq_bo), dkv, dkv_o)
        return y, dx, gwq, gwk, gwv, gwo.reshape(num_heads, hd, model)

    return jax.shard_map(
        device_layer,
        mesh=mesh,
        in_specs=(row_spec, row_spec, rep_spec, rep_spec, rep_spec, rep_spec),
        out_specs=(row_spec, row_spec, part_spec, part_spec, part_spec, part_spec),
        check_vma=False,
    )
```

```python
import functools
import math

import jax
import jax.numpy as jnp
from jax import lax
from jax.experimental import pallas as pl
from jax.experimental.pallas import tpu as pltpu
from jax.sharding import PartitionSpec as P


BLK = 256
HD = 128
DUO = 512
HALF = 1024
SEQ = 2048
LOW = -3.0e38
F32 = jnp.float32
BF16 = jnp.bfloat16


def dot(a, b):
    return jnp.dot(a, b, preferred_element_type=F32)


def dot_nt(a, b):
    return lax.dot_general(a, b, (((1,), (1,)), ((), ())), preferred_element_type=F32)


def params(n=1, mib=60):
    return pltpu.CompilerParams(
        dimension_semantics=("arbitrary",) * n, vmem_limit_bytes=mib * HALF * HALF
    )


def cost(flops, nbytes):
    return pl.CostEstimate(flops=int(flops), bytes_accessed=int(nbytes), transcendentals=0)


def heads_kernel(perm_ref, w_hbm, out_hbm, w_in, w_out, in_sem, out_sem):
    chunks, rows, num, hd = w_in.shape
    group = perm_ref.shape[0]
    loads = [
        pltpu.make_async_copy(w_hbm.at[c * rows : (c + 1) * rows], w_in.at[c], in_sem.at[c]) for c in range(chunks)
    ]
    stores = [
        pltpu.make_async_copy(w_out.at[c], out_hbm.at[c * rows : (c + 1) * rows, :], out_sem.at[c]) for c in range(chunks)
    ]
    for cp in loads:
        cp.start()

    def chunk(c, _):
        pltpu.make_async_copy(w_hbm.at[:rows], w_in.at[c], in_sem.at[c]).wait()
        flat = w_in.at[c].reshape(rows * num, hd)
        for g in range(0, rows // 16, 2):
            pair = [flat[(g + n) * group : (g + n + 1) * group, :] for n in range(2)]
            res = dot(perm_ref[...], jnp.concatenate(pair, axis=1)).astype(BF16)
            for n in range(2):
                for h in range(num):
                    w_out[c, (g + n) * 16 : (g + n + 1) * 16, h * hd : (h + 1) * hd] = res[
                        h * 16 : (h + 1) * 16, n * hd : (n + 1) * hd
                    ]
        at = pl.ds(pl.multiple_of(c * rows, rows), rows)
        pltpu.make_async_copy(w_out.at[c], out_hbm.at[at, :], out_sem.at[c]).start()
        return 0

    lax.fori_loop(0, chunks, chunk, 0)
    for cp in stores:
        cp.wait()


def gather_heads(num, rows):
    row = jnp.arange(num * rows)
    return ((row % rows * num + row // rows)[:, None] == row[None, :]).astype(BF16)


def flat_heads(w):
    model, num, hd = w.shape
    chunks = 8
    rows = model // chunks
    return pl.pallas_call(
        heads_kernel,
        out_shape=jax.ShapeDtypeStruct((model, num * hd), BF16),
        in_specs=[pl.BlockSpec(memory_space=pltpu.VMEM), pl.BlockSpec(memory_space=pl.ANY)],
        out_specs=pl.BlockSpec(memory_space=pl.ANY),
        scratch_shapes=[
            pltpu.VMEM((chunks, rows, num, hd), BF16),
            pltpu.VMEM((chunks, rows, num * hd), BF16),
            pltpu.SemaphoreType.DMA((chunks,)),
            pltpu.SemaphoreType.DMA((chunks,)),
        ],
        compiler_params=pltpu.CompilerParams(vmem_limit_bytes=params(1).vmem_limit_bytes),
        cost_estimate=cost(4e9, 4 * model * num * hd),
    )(gather_heads(num, 16), w)


def kv_kernel(sc, x_ref, dy_ref, wk_ref, wv_ref, perm_ref, out_ref, w_ref, xa, xb, dya, dyb):
    @pl.when(pl.program_id(0) == 0)
    def _():
        for g in range(w_ref.shape[0] // HD):
            rows = slice(g * BLK, (g + 1) * BLK)
            pair = jnp.concatenate([wk_ref[rows, :], wv_ref[rows, :]], axis=1)
            res = dot(perm_ref[...], pair).astype(BF16)
            for h in range(2):
                for v in range(2):
                    col = (v * 2 + h) * HD
                    w_ref[g * HD : (g + 1) * HD, col : col + HD] = res[h * HD : (h + 1) * HD, v * HD : (v + 1) * HD]

    out_ref[...] = dot(x_ref[...], w_ref[...]).astype(BF16)

    @pl.when(pl.program_id(0) == 1 - sc[0])
    def _():
        xa[...] = x_ref[...]
        dya[...] = dy_ref[...]

    @pl.when(pl.program_id(0) == sc[0])
    def _():
        xb[...] = x_ref[...]
        dyb[...] = dy_ref[...]


def project_kv(core, x, dy, wk, wv):
    rows, depth = x.shape
    row = pl.BlockSpec((BLK, depth), lambda i, s: (i, 0))
    fixed = lambda shape: pl.BlockSpec(shape, lambda i, s: (0, 0))
    half = jax.ShapeDtypeStruct((BLK, depth), BF16)
    return pl.pallas_call(
        kv_kernel,
        out_shape=(jax.ShapeDtypeStruct((rows, DUO), BF16), jax.ShapeDtypeStruct((depth, DUO), BF16), half, half, half, half),
        grid_spec=pltpu.PrefetchScalarGridSpec(
            num_scalar_prefetch=1,
            grid=(rows // BLK,),
            in_specs=[row, row, fixed(wk.shape), fixed(wv.shape), fixed((BLK, BLK))],
            out_specs=(pl.BlockSpec((BLK, DUO), lambda i, s: (i, 0)), fixed((depth, DUO))) + (fixed((BLK, depth)),) * 4,
        ),
        compiler_params=params(),
        cost_estimate=cost(2 * rows * depth * DUO, 8e6),
    )(core, x, dy, wk, wv, gather_heads(2, HD))


def attn_kernel(heads, scale, first, final, sc, wq_hbm, wo_hbm, *refs):
    x_hbm, dy_hbm, kv_refs, refs = refs[:2], refs[2:4], refs[4:12], refs[12:]
    if first:
        o_ref, dq_ref, dkv_ref = refs[:3]
        scratch = refs[3:]
    else:
        init_ref, o_ref, dq_ref, dkv_ref = refs[:4]
        scratch = refs[4:]
    ks, vs, kt, vt, dk, dv, qt, dot_t, qst, dost, s_ref, p_ref, ds_ref, ot, dqt, m_ref, l_ref, wq, wo, xs, dys, w_sem, x_sem, dy_sem = scratch
    step = pl.program_id(0)
    wide = heads * BLK
    hd = HD
    c2 = scale * math.log2(math.e)

    steps = 2 * x_hbm[0].shape[0] // BLK
    core = pl.multiple_of(sc[24] * heads * hd, heads * hd)
    load_wq, load_wo = [], []
    for n in range(4):
        span = slice(n * DUO, (n + 1) * DUO)
        load_wq.append(pltpu.make_async_copy(wq_hbm.at[span, pl.ds(core, heads * hd)], wq.at[span, :], w_sem.at[0]))
        rows = heads * hd // 4
        dst = wo.at[n * rows : (n + 1) * rows, :]
        load_wo.append(pltpu.make_async_copy(wo_hbm.at[pl.ds(core + n * rows, rows), :], dst, w_sem.at[1]))

    def load_rows(n):
        piece, row = divmod(n, steps // 2)
        src = pl.ds(row * BLK, BLK)
        return (
            pltpu.make_async_copy(x_hbm[piece].at[src, :], xs.at[n % 2], x_sem.at[n % 2]),
            pltpu.make_async_copy(dy_hbm[piece].at[src, :], dys.at[n % 2], dy_sem.at[n % 2]),
        )

    @pl.when(step == 0)
    def _():
        load_x, load_dy = load_rows(0)
        load_x.start()
        for cp in load_wq:
            cp.start()
        load_dy.start()
        for cp in load_wo:
            cp.start()

    for n in range(1, steps):

        @pl.when(step == n - 1)
        def _():
            for cp in load_rows(n):
                cp.start()

    @pl.when(step == 0)
    def _():
        for i in range(8):
            rows = slice((i % 2) * BLK, (i % 2 + 1) * BLK)
            at = pl.ds(pl.multiple_of(sc[i] * BLK, BLK), BLK)
            kk, vv = kv_refs[i // 2][rows, :], kv_refs[4 + i // 2][rows, :]
            ks[at, :] = kk
            vs[at, :] = vv
            kt[:, at] = kk.T
            vt[:, at] = vv.T
            if not first:
                init_rows = slice(i * BLK, (i + 1) * BLK)
                dk[at, :] = init_ref[init_rows, :hd]
                dv[at, :] = init_ref[init_rows, hd:]
            else:
                dk[at, :] = jnp.zeros((BLK, hd), F32)
                dv[at, :] = jnp.zeros((BLK, hd), F32)

    @pl.when(step == 0)
    def _():
        for cp in load_wq:
            cp.wait()

    slot = step % 2
    pltpu.make_async_copy(x_hbm[0].at[0:BLK, :], xs.at[slot], x_sem.at[slot]).wait()
    q = dot(xs[slot], wq[...]).astype(BF16)
    for h in range(heads):
        qh = q[:, h * hd : (h + 1) * hd]
        qst[h * BLK : (h + 1) * BLK, :] = qh
        qt[:, h * BLK : (h + 1) * BLK] = qh.T

    @pl.when(step == 0)
    def _():
        for cp in load_wo:
            cp.wait()

    pltpu.make_async_copy(dy_hbm[0].at[0:BLK, :], dys.at[slot], dy_sem.at[slot]).wait()
    do = dot_nt(dys[slot], wo[...]).astype(BF16)
    for h in range(heads):
        dh = do[:, h * hd : (h + 1) * hd]
        dost[h * BLK : (h + 1) * BLK, :] = dh
        dot_t[:, h * BLK : (h + 1) * BLK] = dh.T

    b = sc[8 + step]

    def softmax_block(j, masked):
        at = pl.ds(pl.multiple_of(j * BLK, BLK), BLK)
        for h in range(heads):
            span = slice(h * BLK, (h + 1) * BLK)
            t = dot(ks[at, :], qt[:, span]) * c2
            if masked:
                key = lax.broadcasted_iota(jnp.int32, (BLK, BLK), 0)
                query = lax.broadcasted_iota(jnp.int32, (BLK, BLK), 1)
                t = jnp.where(key <= query, t, LOW)
            s_ref[at, span] = t
            m8 = m_ref[:, span]
            new = jnp.maximum(m8, jnp.max(t.reshape(BLK // 8, 8, BLK), axis=0))
            e = jnp.exp2(s_ref[at, span].reshape(BLK // 8, 8, BLK) - new[None])
            l_ref[:, span] = l_ref[:, span] * jnp.exp2(m8 - new) + jnp.sum(e, axis=0)
            m_ref[:, span] = new

    m_ref[...] = jnp.full((8, wide), LOW, F32)
    l_ref[...] = jnp.zeros((8, wide), F32)

    def open_block(j, _):
        softmax_block(j, False)
        return 0

    lax.fori_loop(0, b, open_block, 0)
    softmax_block(b, True)
    m8 = m_ref[...]
    top = jnp.max(m8, axis=0, keepdims=True)
    lse = top + jnp.log2(jnp.sum(l_ref[...] * jnp.exp2(m8 - top), axis=0, keepdims=True))

    ot[...] = jnp.zeros_like(ot)

    def value_block(j, _):
        at = pl.ds(pl.multiple_of(j * BLK, BLK), BLK)
        for h in range(heads):
            span = slice(h * BLK, (h + 1) * BLK)
            p = jnp.exp2(s_ref[at, span] - lse[:, span]).astype(BF16)
            p_ref[at, span] = p
            ot[:, span] += dot(vt[:, at], p)
        return 0

    lax.fori_loop(0, b + 1, value_block, 0)

    o_round = ot[...].astype(BF16)
    delta = jnp.sum(o_round.astype(F32) * dot_t[...].astype(F32), axis=0, keepdims=True)
    for h in range(heads):
        o_ref[h * hd : (h + 1) * hd, :] = o_round[:, h * BLK : (h + 1) * BLK]
    dqt[...] = jnp.zeros_like(dqt)

    def grad_block(j, _):
        at = pl.ds(pl.multiple_of(j * BLK, BLK), BLK)
        dp = dot(vs[at, :], dot_t[...])
        dv[at, :] += dot(p_ref[at, :], dost[...])
        ds = (p_ref[at, :].astype(F32) * (dp - delta)).astype(BF16)
        ds_ref[...] = ds
        dqt[...] += dot(kt[:, at], ds_ref[...])
        dk[at, :] += dot(ds_ref[...], qst[...])
        return 0

    lax.fori_loop(0, b + 1, grad_block, 0)

    for h in range(heads):
        dq_ref[:, h * hd : (h + 1) * hd] = (dqt[:, h * BLK : (h + 1) * BLK] * scale).astype(BF16).T

    @pl.when(step == pl.num_programs(0) - 1)
    def _():
        for i in range(8):
            at = pl.ds(pl.multiple_of(sc[i] * BLK, BLK), BLK)
            if final:
                out = pl.ds(pl.multiple_of(sc[16 + i] * BLK, BLK), BLK)
                dkv_ref[out, :hd] = (dk[at, :] * scale).astype(BF16)
                dkv_ref[out, hd:] = dv[at, :].astype(BF16)
            else:
                out = slice(i * BLK, (i + 1) * BLK)
                dkv_ref[out, :hd] = dk[at, :]
                dkv_ref[out, hd:] = dv[at, :]


def attention(sc, wq, wo, x_pieces, dy_pieces, kv_pieces, init, final, scale):
    first = init is None
    rows, width, model = 2 * x_pieces[0].shape[0], wq.shape[1] // 2, wq.shape[0]
    hd = HD
    heads = width // hd
    wide = heads * BLK
    seq = SEQ
    o_spec = pl.BlockSpec((width, BLK), lambda i, s: (0, s[12 + i]))
    out_spec = pl.BlockSpec((BLK, width), lambda i, s: (s[12 + i], 0))
    full = lambda shape: pl.BlockSpec(shape, lambda i, s: (0, 0), pipeline_mode=pl.Buffered(1))
    ins = [wq, wo, *x_pieces, *dy_pieces] + list(kv_pieces) * 2 + ([] if first else [init])
    in_specs = [pl.BlockSpec(memory_space=pl.ANY)] * 6
    in_specs += [pl.BlockSpec((2 * BLK, hd), lambda i, s: (0, s[24]))] * 4
    in_specs += [pl.BlockSpec((2 * BLK, hd), lambda i, s: (0, 2 + s[24]))] * 4
    if not first:
        in_specs.append(full(init.shape))
    return pl.pallas_call(
        functools.partial(attn_kernel, heads, scale, first, final),
        out_shape=(
            jax.ShapeDtypeStruct((width, rows), BF16),
            jax.ShapeDtypeStruct((rows, width), BF16),
            jax.ShapeDtypeStruct((seq, BLK), BF16 if final else F32),
        ),
        grid_spec=pltpu.PrefetchScalarGridSpec(
            num_scalar_prefetch=1,
            grid=(rows // BLK,),
            in_specs=in_specs,
            out_specs=(o_spec, out_spec, full((seq, BLK))),
            scratch_shapes=[
                *[pltpu.VMEM((seq, hd), BF16) for _ in "kv"],
                *[pltpu.VMEM((hd, seq), BF16) for _ in "kv"],
                *[pltpu.VMEM((seq, hd), F32) for _ in "kv"],
                *[pltpu.VMEM((hd, wide), BF16) for _ in "qd"],
                *[pltpu.VMEM((wide, hd), BF16) for _ in "qd"],
                pltpu.VMEM((seq, wide), F32),
                pltpu.VMEM((seq, wide), BF16),
                pltpu.VMEM((BLK, wide), BF16),
                *[pltpu.VMEM((hd, wide), F32) for _ in "od"],
                *[pltpu.VMEM((8, wide), F32) for _ in "ml"],
                pltpu.VMEM((model, width), BF16),
                pltpu.VMEM((width, model), BF16),
                *[pltpu.VMEM((2, BLK, model), BF16) for _ in "xd"],
                *[pltpu.SemaphoreType.DMA((2,)) for _ in "wxd"],
            ],
        ),
        compiler_params=params(1, 63),
        cost_estimate=cost(8e9 * (rows // BLK), 20e6),
    )(sc, *ins)


def y_kernel(sc, o_mine, o_other, w_mine, w_other, out_ref, os):
    half = o_mine.shape[0]

    @pl.when(pl.program_id(0) == 0)
    def _():
        os[:, :half] = o_mine[...].T
        os[:, half:] = o_other[...].T

    out_ref[...] = (dot(os[:, :half], w_mine[...]) + dot(os[:, half:], w_other[...])).astype(BF16)


def out_rows(core, o_mine, o_other, wo):
    rows, half, model, tile = DUO, o_mine.shape[0], wo.shape[1], DUO
    return pl.pallas_call(
        y_kernel,
        out_shape=jax.ShapeDtypeStruct((rows, model), BF16),
        grid_spec=pltpu.PrefetchScalarGridSpec(
            num_scalar_prefetch=1,
            grid=(model // tile,),
            in_specs=[
                pl.BlockSpec((half, rows), lambda i, s: (0, s[0])),
                pl.BlockSpec((half, rows), lambda i, s: (0, s[0])),
                pl.BlockSpec((half, tile), lambda i, s: (s[0], i)),
                pl.BlockSpec((half, tile), lambda i, s: (1 - s[0], i)),
            ],
            out_specs=pl.BlockSpec((rows, tile), lambda i, s: (0, i)),
            scratch_shapes=[pltpu.VMEM((rows, 2 * half), BF16)],
        ),
        compiler_params=params(),
        cost_estimate=cost(4 * rows * half * model, 12e6),
    )(core, o_mine, o_other, wo, wo)


def dx_kernel(sc, q_mine, q_other, kv_mine, kv_other, wq_mine, wq_other, wkv, out_ref, kv):
    hd = HD

    @pl.when(pl.program_id(0) == 0)
    def _():
        for n, src in ((sc[0], kv_mine), (1 - sc[0], kv_other)):
            kv[:, pl.ds(pl.multiple_of(n * hd, hd), hd)] = src[:, :hd]
            kv[:, pl.ds(pl.multiple_of((2 + n) * hd, hd), hd)] = src[:, hd:]

    acc = dot_nt(q_mine[...], wq_mine[...]) + dot_nt(q_other[...], wq_other[...])
    out_ref[...] = (acc + dot_nt(kv[...], wkv[...])).astype(BF16)


def grad_rows(core, dq_mine, dq_other, dkv_mine, dkv_other, wq, wkv):
    rows, half, model, tile = DUO, dq_mine.shape[1], wq.shape[0], DUO
    mine = lambda i, s: (s[0], 0)
    near, far = lambda i, s: (i, s[0]), lambda i, s: (i, 1 - s[0])
    return pl.pallas_call(
        dx_kernel,
        out_shape=jax.ShapeDtypeStruct((rows, model), BF16),
        grid_spec=pltpu.PrefetchScalarGridSpec(
            num_scalar_prefetch=1,
            grid=(model // tile,),
            in_specs=[
                *[pl.BlockSpec((rows, n), mine) for n in (half, half, BLK, BLK)],
                *[pl.BlockSpec((tile, half), at) for at in (near, far)],
                pl.BlockSpec((tile, DUO), lambda i, s: (i, 0)),
            ],
            out_specs=pl.BlockSpec((rows, tile), lambda i, s: (0, i)),
            scratch_shapes=[pltpu.VMEM((rows, DUO), BF16)],
        ),
        compiler_params=params(),
        cost_estimate=cost(4 * rows * half * model * 1.25, 14e6),
    )(core, dq_mine, dq_other, dkv_mine, dkv_other, wq, wq, wkv)


PIECES = ((0, DUO), (1, DUO), (0, BLK), (1, BLK), (0, BLK), (1, BLK))
STARTS = (0, DUO, HALF, 1280, 1536, 1792)


def piece_copies(core, arrays, dst, sem, along):
    copies = []
    for n, ((flip, size), start) in enumerate(zip(PIECES, STARTS)):
        at = pl.ds(pl.multiple_of((1 - core if flip else core) * size, size), size)
        src = arrays[n // 2]
        if along:
            copies.append(pltpu.make_async_copy(src.at[:, at], dst.at[:, start : start + size], sem))
        else:
            copies.append(pltpu.make_async_copy(src.at[at, :], dst.at[start : start + size, :], sem))
    return copies


def dwq_kernel(sc, *refs):
    xs_in, mine, other, kv_in = refs[:6], refs[6:9], refs[9:12], refs[12:14]
    out_ref, gk_ref, gv_ref, xt, dq, kv, sems = refs[14:]
    g, i = pl.program_id(0), pl.program_id(1)
    tile, core, hd = out_ref.shape[0], sc[0], HD
    first = piece_copies(core, mine, dq.at[0], sems.at[0], False)
    later = piece_copies(core, other, dq.at[1], sems.at[1], False)
    for n, src in enumerate(kv_in):
        parts = [src.at[at : at + size, :] for at, size in ((0, HALF), (HALF, DUO), (1536, DUO))]
        later += piece_copies(core, parts, kv.at[:, n * BLK : (n + 1) * BLK], sems.at[1], False)

    @pl.when((g == 0) & (i == 0))
    def _():
        for cp in first:
            cp.start()

    @pl.when((g == 0) & (i == 1))
    def _():
        for cp in later:
            cp.start()

    @pl.when(g == 0)
    def _():
        for s, (_, n), x in zip(STARTS, PIECES, xs_in):
            xt[i, :, s : s + n] = x[...].T

    @pl.when((g == 0) & (i == 0))
    def _():
        for cp in first:
            cp.wait()

    @pl.when((g == 1) & (i == 0))
    def _():
        for cp in later:
            cp.wait()

    acc = dot(xt[i], dq[g])
    flat = out_ref.reshape(tile * 8, hd)
    for h in range(8):
        flat[pl.ds(h, tile, stride=8), :] = acc[:, h * hd : (h + 1) * hd]

    @pl.when(g == 1)
    def _():
        k_flat, v_flat = gk_ref.reshape(tile * 2, hd), gv_ref.reshape(tile * 2, hd)
        both = dot(xt[i], kv[...])
        for n, head in enumerate((core, 1 - core)):
            k_flat[pl.ds(head, tile, stride=2), :] = both[:, 2 * n * hd : (2 * n + 1) * hd]
            v_flat[pl.ds(head, tile, stride=2), :] = both[:, (2 * n + 1) * hd : (2 * n + 2) * hd]


def grad_wq(core, xs, mine, other, kvm, kvo):
    model, half, tile = xs[0].shape[1], mine[0].shape[1], BLK
    tiles = model // tile
    x_specs = [pl.BlockSpec((n, tile), lambda g, i, s: (0, jnp.where(g == 0, i, tiles - 1))) for _, n in PIECES]
    small = pl.BlockSpec((tile, 2, HD), lambda g, i, s: (i * g, 0, 0))
    return pl.pallas_call(
        dwq_kernel,
        out_shape=(
            jax.ShapeDtypeStruct((model, 16, HD), F32),
            jax.ShapeDtypeStruct((model, 2, HD), F32),
            jax.ShapeDtypeStruct((model, 2, HD), F32),
        ),
        grid_spec=pltpu.PrefetchScalarGridSpec(
            num_scalar_prefetch=1,
            grid=(2, tiles),
            in_specs=x_specs + [pl.BlockSpec(memory_space=pl.ANY)] * 8,
            out_specs=(
                pl.BlockSpec((tile, 8, HD), lambda g, i, s: (i, (s[0] + g) % 2, 0)),
                small,
                small,
            ),
            scratch_shapes=[
                pltpu.VMEM((tiles, tile, SEQ), BF16),
                pltpu.VMEM((2, SEQ, half), BF16),
                pltpu.VMEM((SEQ, DUO), BF16),
                pltpu.SemaphoreType.DMA((2,)),
            ],
        ),
        compiler_params=params(2),
        cost_estimate=cost(2 * SEQ * model * (2 * half + DUO), 40e6),
    )(core, *xs, *mine, *other, kvm, kvo)


def dwo_kernel(sc, *refs):
    mine, other, ys, (out_ref, o_all, y_all, sems) = refs[:3], refs[3:6], refs[6:12], refs[12:]
    j, g, i = pl.program_id(0), pl.program_id(1), pl.program_id(2)
    tile, wide = out_ref.shape
    o_first = piece_copies(sc[0], mine, o_all.at[0], sems.at[0], True)
    o_later = piece_copies(sc[0], other, o_all.at[1], sems.at[1], True)
    y_copies = [
        [
            pltpu.make_async_copy(y.at[:, n * wide : (n + 1) * wide], y_all.at[n, s : s + r, :], sems.at[2 + n])
            for y, s, (_, r) in zip(ys, STARTS, PIECES)
        ]
        for n in range(2)
    ]

    def when(jj, gg, ii, copies, start):
        @pl.when((j == jj) & (g == gg) & (i == ii))
        def _():
            for cp in copies:
                cp.start() if start else cp.wait()

    when(0, 0, 0, y_copies[0] + o_first, True)
    when(0, 0, 1, o_later, True)
    when(0, 1, 0, y_copies[1], True)
    when(0, 0, 0, y_copies[0] + o_first, False)
    when(0, 1, 0, o_later, False)
    when(1, 0, 0, y_copies[1], False)
    out_ref[...] = dot(o_all[g, pl.ds(pl.multiple_of(i * tile, tile), tile), :], y_all[j])


def grad_wo(core, ys, mine, other):
    model, half, tile, wide = ys[0].shape[1], mine[0].shape[0], DUO, HALF
    steps = half // tile
    return pl.pallas_call(
        dwo_kernel,
        out_shape=jax.ShapeDtypeStruct((2 * half, model), F32),
        grid_spec=pltpu.PrefetchScalarGridSpec(
            num_scalar_prefetch=1,
            grid=(2, 2, steps),
            in_specs=[pl.BlockSpec(memory_space=pl.ANY)] * 12,
            out_specs=pl.BlockSpec((tile, wide), lambda j, g, i, s: ((s[0] + g) % 2 * steps + i, j)),
            scratch_shapes=[
                pltpu.VMEM((2, half, SEQ), BF16),
                pltpu.VMEM((2, SEQ, wide), BF16),
                pltpu.SemaphoreType.DMA((4,)),
            ],
        ),
        compiler_params=params(3),
        cost_estimate=cost(4 * SEQ * model * half, 40e6),
    )(core, *mine, *other, *ys)


def solution(mesh):
    row_spec = P(("dp", "cp"), None)
    rep_spec = P(None, None, None)
    part_spec = P("dp", None, None)
    core_swap = [(0, 1), (1, 0), (2, 3), (3, 2)]
    chip_swap = [(0, 2), (2, 0), (1, 3), (3, 1)]

    def device_layer(x, dy, w_query, w_key, w_value, w_out):
        _, model = x.shape
        num_heads, hd = w_query.shape[1:]
        kv_heads = w_key.shape[1]
        scale = hd ** -0.5
        rank = lax.axis_index("cp").astype(jnp.int32)
        c = rank & 1
        core = c.reshape(1)
        devs = [rank, rank ^ 1, rank ^ 2, rank ^ 3]
        kv_pos = [p for e in devs for p in (e, 7 - e)]
        own_slots = [p for e in devs[:2] for p in ((e & 1) * 2, (e & 1) * 2 + 1)]
        far_slots = []
        for e in devs[2:]:
            far_slots += [jnp.where((e & 1) == 1, 4, 6) + (e & 1), jnp.where((e & 1) == 0, 4, 6) + (e & 1)]
        pos_a = [jnp.where((e & 1) == 0, 7 - e, e) for e in devs[2:]]
        pos_b = [jnp.where((e & 1) == 0, e, 7 - e) for e in devs[2:]]
        far = [c, 1 - c]
        tail = own_slots + far_slots + [c]
        sc_chip = jnp.stack(kv_pos + kv_pos[:4] + own_slots + tail)
        sc_a = jnp.stack(kv_pos + pos_a * 2 + far * 2 + tail)
        sc_b = jnp.stack(kv_pos + pos_b * 2 + far * 2 + tail)

        to_core = lambda v: lax.ppermute(v, "cp", core_swap)
        to_chip = lambda v: lax.ppermute(v, "cp", chip_swap)

        wk = w_key.reshape(model * kv_heads, hd)
        wv = w_value.reshape(model * kv_heads, hd)
        wo = w_out.reshape(num_heads * hd, model)
        x_p = to_core(x)
        dy_p = to_core(dy)

        kv, wkv, x_a, x_b, dy_a, dy_b = project_kv(core, x, dy, wk, wv)
        far_kv, kv_p = to_chip(kv), to_core(kv)
        w_s, _ = lax.optimization_barrier((w_query, kv))
        x_a, dy_a = to_chip(x_a), to_chip(dy_a)
        x_b, dy_b = to_chip(x_b), to_chip(dy_b)
        wq = flat_heads(w_s)
        kv_r, wq = lax.optimization_barrier((far_kv, wq))
        kv_rp = to_core(kv_r)
        pieces = (kv, kv_p, kv_r, kv_rp)

        o_c, dq_c, part = attention(
            sc_chip, wq, wo, (x, x_p), (dy, dy_p), pieces, None, False, scale)
        x_a, dy_a, o_c, dq_c = lax.optimization_barrier((x_a, dy_a, o_c, dq_c))
        x_pa, dy_pa, o_co, dq_co = to_core(x_a), to_core(dy_a), to_core(o_c), to_core(dq_c)

        o_a, dq_a, part = attention(sc_a, wq, wo, (x_a, x_pa), (dy_a, dy_pa), pieces, part, False, scale)
        x_b, dy_b, o_a, dq_a = lax.optimization_barrier((x_b, dy_b, o_a, dq_a))
        x_pb, dy_pb, o_ao, dq_ao = to_core(x_b), to_core(dy_b), to_core(o_a), to_core(dq_a)

        o_b, dq_b, dkv = attention(sc_b, wq, wo, (x_b, x_pb), (dy_b, dy_pb), pieces, part, True, scale)
        o_co, dkv = lax.optimization_barrier((o_co, dkv))
        dkv_o, o_bo, dq_bo = to_core(dkv), to_core(o_b), to_core(dq_b)
        y = out_rows(core, o_c, o_co, wo)

        xs = (x, x_p, x_a, x_pa, x_b, x_pb)
        ys = (dy, dy_p, dy_a, dy_pa, dy_b, dy_pb)
        gwo = grad_wo(core, ys, (o_c, o_a, o_b), (o_co, o_ao, o_bo))
        dx = grad_rows(core, dq_c, dq_co, dkv, dkv_o, wq, wkv)
        gwq, gwk, gwv = grad_wq(core, xs, (dq_c, dq_a, dq_b), (dq_co, dq_ao, dq_bo), dkv, dkv_o)
        return y, dx, gwq, gwk, gwv, gwo.reshape(num_heads, hd, model)

    return jax.shard_map(
        device_layer,
        mesh=mesh,
        in_specs=(row_spec, row_spec, rep_spec, rep_spec, rep_spec, rep_spec),
        out_specs=(row_spec, row_spec, part_spec, part_spec, part_spec, part_spec),
        check_vma=False,
    )
```

```python
import functools
import math

import jax
import jax.numpy as jnp
from jax import lax
from jax.experimental import pallas as pl
from jax.experimental.pallas import tpu as pltpu
from jax.sharding import PartitionSpec as P


BLK = 256
HD = 128
DUO = 512
HALF = 1024
SEQ = 2048
TILE_WQ = 512
LOW = -3.0e38
F32 = jnp.float32
BF16 = jnp.bfloat16


def dot(a, b):
    return jnp.dot(a, b, preferred_element_type=F32)


def dot_nt(a, b):
    return lax.dot_general(a, b, (((1,), (1,)), ((), ())), preferred_element_type=F32)


def params(n=1, mib=60):
    return pltpu.CompilerParams(
        dimension_semantics=("arbitrary",) * n, vmem_limit_bytes=mib * HALF * HALF
    )


def cost(flops, nbytes):
    return pl.CostEstimate(flops=int(flops), bytes_accessed=int(nbytes), transcendentals=0)


def heads_kernel(perm_ref, w_hbm, out_hbm, w_in, w_out, in_sem, out_sem):
    chunks, rows, num, hd = w_in.shape
    group = perm_ref.shape[0]
    loads = [
        pltpu.make_async_copy(w_hbm.at[c * rows : (c + 1) * rows], w_in.at[c], in_sem.at[c]) for c in range(chunks)
    ]
    stores = [
        pltpu.make_async_copy(w_out.at[c], out_hbm.at[c * rows : (c + 1) * rows, :], out_sem.at[c]) for c in range(chunks)
    ]
    for cp in loads:
        cp.start()

    def chunk(c, _):
        pltpu.make_async_copy(w_hbm.at[:rows], w_in.at[c], in_sem.at[c]).wait()
        flat = w_in.at[c].reshape(rows * num, hd)
        for g in range(0, rows // 16, 2):
            pair = [flat[(g + n) * group : (g + n + 1) * group, :] for n in range(2)]
            res = dot(perm_ref[...], jnp.concatenate(pair, axis=1)).astype(BF16)
            for n in range(2):
                for h in range(num):
                    w_out[c, (g + n) * 16 : (g + n + 1) * 16, h * hd : (h + 1) * hd] = res[
                        h * 16 : (h + 1) * 16, n * hd : (n + 1) * hd
                    ]
        at = pl.ds(pl.multiple_of(c * rows, rows), rows)
        pltpu.make_async_copy(w_out.at[c], out_hbm.at[at, :], out_sem.at[c]).start()
        return 0

    lax.fori_loop(0, chunks, chunk, 0)
    for cp in stores:
        cp.wait()


def gather_heads(num, rows):
    row = jnp.arange(num * rows)
    return ((row % rows * num + row // rows)[:, None] == row[None, :]).astype(BF16)


def flat_heads(w):
    model, num, hd = w.shape
    chunks = 8
    rows = model // chunks
    return pl.pallas_call(
        heads_kernel,
        out_shape=jax.ShapeDtypeStruct((model, num * hd), BF16),
        in_specs=[pl.BlockSpec(memory_space=pltpu.VMEM), pl.BlockSpec(memory_space=pl.ANY)],
        out_specs=pl.BlockSpec(memory_space=pl.ANY),
        scratch_shapes=[
            pltpu.VMEM((chunks, rows, num, hd), BF16),
            pltpu.VMEM((chunks, rows, num * hd), BF16),
            pltpu.SemaphoreType.DMA((chunks,)),
            pltpu.SemaphoreType.DMA((chunks,)),
        ],
        compiler_params=pltpu.CompilerParams(vmem_limit_bytes=params(1).vmem_limit_bytes),
        cost_estimate=cost(4e9, 4 * model * num * hd),
    )(gather_heads(num, 16), w)


def kv_kernel(sc, x_ref, dy_ref, wk_ref, wv_ref, perm_ref, out_ref, w_ref, rows_a, rows_b):
    @pl.when(pl.program_id(0) == 0)
    def _():
        for g in range(w_ref.shape[0] // HD):
            rows = slice(g * BLK, (g + 1) * BLK)
            pair = jnp.concatenate([wk_ref[rows, :], wv_ref[rows, :]], axis=1)
            res = dot(perm_ref[...], pair).astype(BF16)
            for h in range(2):
                for v in range(2):
                    col = (v * 2 + h) * HD
                    w_ref[g * HD : (g + 1) * HD, col : col + HD] = res[h * HD : (h + 1) * HD, v * HD : (v + 1) * HD]

    out_ref[...] = dot(x_ref[...], w_ref[...]).astype(BF16)

    @pl.when(pl.program_id(0) == 1 - sc[0])
    def _():
        rows_a[:BLK, :] = x_ref[...]
        rows_a[BLK:, :] = dy_ref[...]

    @pl.when(pl.program_id(0) == sc[0])
    def _():
        rows_b[:BLK, :] = x_ref[...]
        rows_b[BLK:, :] = dy_ref[...]


def project_kv(core, x, dy, wk, wv):
    rows, depth = x.shape
    row = pl.BlockSpec((BLK, depth), lambda i, s: (i, 0))
    fixed = lambda shape: pl.BlockSpec(shape, lambda i, s: (0, 0))
    chunk = jax.ShapeDtypeStruct((rows, depth), BF16)
    return pl.pallas_call(
        kv_kernel,
        out_shape=(jax.ShapeDtypeStruct((rows, DUO), BF16), jax.ShapeDtypeStruct((depth, DUO), BF16), chunk, chunk),
        grid_spec=pltpu.PrefetchScalarGridSpec(
            num_scalar_prefetch=1,
            grid=(rows // BLK,),
            in_specs=[row, row, fixed(wk.shape), fixed(wv.shape), fixed((BLK, BLK))],
            out_specs=(pl.BlockSpec((BLK, DUO), lambda i, s: (i, 0)), fixed((depth, DUO))) + (fixed((rows, depth)),) * 2,
        ),
        compiler_params=params(),
        cost_estimate=cost(2 * rows * depth * DUO, 8e6),
    )(core, x, dy, wk, wv, gather_heads(2, HD))


def attn_kernel(heads, scale, first, final, steps, base, sc, wq_hbm, wo_hbm, *refs):
    x_hbm, dy_hbm, kv_refs, refs = refs[:2], refs[2:4], refs[4:12], refs[12:]
    if first:
        o_ref, dq_ref, dkv_ref, xt_ref = refs[:4]
        scratch = refs[4:]
    else:
        init_ref, o_ref, dq_ref, dkv_ref, xt_ref = refs[:5]
        scratch = refs[5:]
    ks, vs, kt, vt, dk, dv, qt, dot_t, qst, dost, s_ref, p_ref, ds_ref, ot, dqt, m_ref, l_ref, ref, wq, wo, xs, dys, w_sem, x_sem, dy_sem = scratch
    step = pl.program_id(0)
    hd = HD
    c2 = scale * math.log2(math.e)

    core = pl.multiple_of(sc[24] * heads * hd, heads * hd)
    load_wq, load_wo = [], []
    for n in range(4):
        span = slice(n * DUO, (n + 1) * DUO)
        load_wq.append(pltpu.make_async_copy(wq_hbm.at[span, pl.ds(core, heads * hd)], wq.at[span, :], w_sem.at[0]))
        rows = heads * hd // 4
        dst = wo.at[n * rows : (n + 1) * rows, :]
        load_wo.append(pltpu.make_async_copy(wo_hbm.at[pl.ds(core + n * rows, rows), :], dst, w_sem.at[1]))

    def load_rows(n):
        piece, row = divmod(n, steps // 2)
        src = pl.ds(row * BLK, BLK)
        return (
            pltpu.make_async_copy(x_hbm[piece].at[src, :], xs.at[n % 2], x_sem.at[n % 2]),
            pltpu.make_async_copy(dy_hbm[piece].at[pl.ds(base + row * BLK, BLK), :], dys.at[n % 2], dy_sem.at[n % 2]),
        )

    @pl.when(step == 0)
    def _():
        load_x, load_dy = load_rows(0)
        load_x.start()
        for cp in load_wq:
            cp.start()
        load_dy.start()
        for cp in load_wo:
            cp.start()

    for n in range(1, steps):

        @pl.when(step == n - 1)
        def _():
            for cp in load_rows(n):
                cp.start()

    @pl.when(step == 0)
    def _():
        for i in range(8):
            rows = slice((i % 2) * BLK, (i % 2 + 1) * BLK)
            at = pl.ds(pl.multiple_of(sc[i] * BLK, BLK), BLK)
            kk, vv = kv_refs[i // 2][rows, :], kv_refs[4 + i // 2][rows, :]
            ks[at, :] = kk
            vs[at, :] = vv
            kt[:, at] = kk.T
            vt[:, at] = vv.T
            if not first:
                init_rows = slice(i * BLK, (i + 1) * BLK)
                dk[at, :] = init_ref[init_rows, :hd]
                dv[at, :] = init_ref[init_rows, hd:]
            else:
                dk[at, :] = jnp.zeros((BLK, hd), F32)
                dv[at, :] = jnp.zeros((BLK, hd), F32)

    @pl.when(step == 0)
    def _():
        for cp in load_wq:
            cp.wait()

    slot = step % 2
    pltpu.make_async_copy(x_hbm[0].at[0:BLK, :], xs.at[slot], x_sem.at[slot]).wait()
    q = dot(xs[slot], wq[...]).astype(BF16)
    xt_ref[...] = xs[slot].T
    for h in range(heads):
        qh = q[:, h * hd : (h + 1) * hd]
        qst[h * BLK : (h + 1) * BLK, :] = qh
        qt[:, h * BLK : (h + 1) * BLK] = qh.T

    @pl.when(step == 0)
    def _():
        for cp in load_wo:
            cp.wait()

    pltpu.make_async_copy(dy_hbm[0].at[0:BLK, :], dys.at[slot], dy_sem.at[slot]).wait()
    do = dot_nt(dys[slot], wo[...]).astype(BF16)
    for h in range(heads):
        dh = do[:, h * hd : (h + 1) * hd]
        dost[h * BLK : (h + 1) * BLK, :] = dh
        dot_t[:, h * BLK : (h + 1) * BLK] = dh.T

    b = sc[8 + step]

    def scores(j, h):
        at = pl.ds(pl.multiple_of(j * BLK, BLK), BLK)
        return at, slice(h * BLK, (h + 1) * BLK), dot(ks[at, :], qt[:, h * BLK : (h + 1) * BLK]) * c2

    def rows_of(t):
        return t.reshape(BLK // 8, 8, BLK)

    key = lax.broadcasted_iota(jnp.int32, (BLK, BLK), 0)
    query = lax.broadcasted_iota(jnp.int32, (BLK, BLK), 1)
    for h in range(heads):
        at, span, t = scores(b, h)
        t = jnp.where(key <= query, t, LOW)
        s_ref[at, span] = t
        m8 = jnp.max(rows_of(t), axis=0)
        base = jnp.max(m8, axis=0, keepdims=True)
        ref[:, span] = base
        m_ref[:, span] = m8
        l_ref[:, span] = jnp.sum(jnp.exp2(rows_of(t - base)), axis=0)

    def open_block(j, _):
        for h in range(heads):
            at, span, t = scores(j, h)
            s_ref[at, span] = t
            m_ref[:, span] = jnp.maximum(m_ref[:, span], jnp.max(rows_of(t), axis=0))
            l_ref[:, span] += jnp.sum(jnp.exp2(rows_of(t - ref[:, span])), axis=0)
        return 0

    lax.fori_loop(0, b, open_block, 0)

    @pl.when(jnp.max(m_ref[...] - ref[...]) > 60.0)
    def _():
        ref[...] = jnp.max(m_ref[...], axis=0, keepdims=True)
        l_ref[...] = jnp.zeros_like(l_ref)

        def again(j, _):
            at = pl.ds(pl.multiple_of(j * BLK, BLK), BLK)
            for h in range(heads):
                span = slice(h * BLK, (h + 1) * BLK)
                l_ref[:, span] += jnp.sum(jnp.exp2(rows_of(s_ref[at, span] - ref[:, span])), axis=0)
            return 0

        lax.fori_loop(0, b + 1, again, 0)

    lse = ref[...] + jnp.log2(jnp.sum(l_ref[...], axis=0, keepdims=True))

    ot[...] = jnp.zeros_like(ot)

    def value_block(j, _):
        at = pl.ds(pl.multiple_of(j * BLK, BLK), BLK)
        for h in range(heads):
            span = slice(h * BLK, (h + 1) * BLK)
            p = jnp.exp2(s_ref[at, span] - lse[:, span]).astype(BF16)
            p_ref[at, span] = p
            ot[:, span] += dot(vt[:, at], p)
        return 0

    lax.fori_loop(0, b + 1, value_block, 0)

    o_round = ot[...].astype(BF16)
    delta = jnp.sum(o_round.astype(F32) * dot_t[...].astype(F32), axis=0, keepdims=True)
    for h in range(heads):
        o_ref[h * hd : (h + 1) * hd, :] = o_round[:, h * BLK : (h + 1) * BLK]
    dqt[...] = jnp.zeros_like(dqt)

    def grad_block(j, _):
        at = pl.ds(pl.multiple_of(j * BLK, BLK), BLK)
        dp = dot(vs[at, :], dot_t[...])
        dv[at, :] += dot(p_ref[at, :], dost[...])
        ds = (p_ref[at, :].astype(F32) * (dp - delta)).astype(BF16)
        ds_ref[...] = ds
        dqt[...] += dot(kt[:, at], ds_ref[...])
        dk[at, :] += dot(ds_ref[...], qst[...])
        return 0

    lax.fori_loop(0, b + 1, grad_block, 0)

    for h in range(heads):
        dq_ref[:, h * hd : (h + 1) * hd] = (dqt[:, h * BLK : (h + 1) * BLK] * scale).astype(BF16).T

    @pl.when(step == pl.num_programs(0) - 1)
    def _():
        for i in range(8):
            at = pl.ds(pl.multiple_of(sc[i] * BLK, BLK), BLK)
            if final:
                out = pl.ds(pl.multiple_of(sc[16 + i] * BLK, BLK), BLK)
                dkv_ref[out, :hd] = (dk[at, :] * scale).astype(BF16)
                dkv_ref[out, hd:] = dv[at, :].astype(BF16)
            else:
                out = slice(i * BLK, (i + 1) * BLK)
                dkv_ref[out, :hd] = dk[at, :]
                dkv_ref[out, hd:] = dv[at, :]


def attention(sc, wq, wo, x_pieces, dy_pieces, base, kv_pieces, init, final, scale):
    first = init is None
    rows, width, model = 2 * (x_pieces[0].shape[0] - base), wq.shape[1] // 2, wq.shape[0]
    hd = HD
    heads = width // hd
    wide = heads * BLK
    seq = SEQ
    o_spec = pl.BlockSpec((width, BLK), lambda i, s: (0, s[12 + i]))
    out_spec = pl.BlockSpec((BLK, width), lambda i, s: (s[12 + i], 0))
    full = lambda shape: pl.BlockSpec(shape, lambda i, s: (0, 0), pipeline_mode=pl.Buffered(1))
    ins = [wq, wo, *x_pieces, *dy_pieces] + list(kv_pieces) * 2 + ([] if first else [init])
    in_specs = [pl.BlockSpec(memory_space=pl.ANY)] * 6
    in_specs += [pl.BlockSpec((2 * BLK, hd), lambda i, s: (0, s[24]))] * 4
    in_specs += [pl.BlockSpec((2 * BLK, hd), lambda i, s: (0, 2 + s[24]))] * 4
    if not first:
        in_specs.append(full(init.shape))
    return pl.pallas_call(
        functools.partial(attn_kernel, heads, scale, first, final, rows // BLK, base),
        out_shape=(
            jax.ShapeDtypeStruct((width, rows), BF16),
            jax.ShapeDtypeStruct((rows, width), BF16),
            jax.ShapeDtypeStruct((seq, BLK), BF16 if final else F32),
            jax.ShapeDtypeStruct((model, rows), BF16),
        ),
        grid_spec=pltpu.PrefetchScalarGridSpec(
            num_scalar_prefetch=1,
            grid=(rows // BLK,),
            in_specs=in_specs,
            out_specs=(o_spec, out_spec, full((seq, BLK)), pl.BlockSpec((model, BLK), lambda i, s: (0, s[12 + i]))),
            scratch_shapes=[
                *[pltpu.VMEM((seq, hd), BF16) for _ in "kv"],
                *[pltpu.VMEM((hd, seq), BF16) for _ in "kv"],
                *[pltpu.VMEM((seq, hd), F32) for _ in "kv"],
                *[pltpu.VMEM((hd, wide), BF16) for _ in "qd"],
                *[pltpu.VMEM((wide, hd), BF16) for _ in "qd"],
                pltpu.VMEM((seq, wide), F32),
                pltpu.VMEM((seq, wide), BF16),
                pltpu.VMEM((BLK, wide), BF16),
                *[pltpu.VMEM((hd, wide), F32) for _ in "od"],
                *[pltpu.VMEM((8, wide), F32) for _ in "ml"],
                pltpu.VMEM((1, wide), F32),
                pltpu.VMEM((model, width), BF16),
                pltpu.VMEM((width, model), BF16),
                *[pltpu.VMEM((2, BLK, model), BF16) for _ in "xd"],
                *[pltpu.SemaphoreType.DMA((2,)) for _ in "wxd"],
            ],
        ),
        compiler_params=params(1, 63),
        cost_estimate=cost(8e9 * (rows // BLK), 20e6),
    )(sc, *ins)


def y_kernel(sc, o_mine, o_other, w_mine, w_other, out_ref, os):
    half = o_mine.shape[0]

    @pl.when(pl.program_id(0) == 0)
    def _():
        os[:, :half] = o_mine[...].T
        os[:, half:] = o_other[...].T

    out_ref[...] = (dot(os[:, :half], w_mine[...]) + dot(os[:, half:], w_other[...])).astype(BF16)


def out_rows(core, o_mine, o_other, wo):
    rows, half, model, tile = DUO, o_mine.shape[0], wo.shape[1], DUO
    return pl.pallas_call(
        y_kernel,
        out_shape=jax.ShapeDtypeStruct((rows, model), BF16),
        grid_spec=pltpu.PrefetchScalarGridSpec(
            num_scalar_prefetch=1,
            grid=(model // tile,),
            in_specs=[
                pl.BlockSpec((half, rows), lambda i, s: (0, s[0])),
                pl.BlockSpec((half, rows), lambda i, s: (0, s[0])),
                pl.BlockSpec((half, tile), lambda i, s: (s[0], i)),
                pl.BlockSpec((half, tile), lambda i, s: (1 - s[0], i)),
            ],
            out_specs=pl.BlockSpec((rows, tile), lambda i, s: (0, i)),
            scratch_shapes=[pltpu.VMEM((rows, 2 * half), BF16)],
        ),
        compiler_params=params(),
        cost_estimate=cost(4 * rows * half * model, 12e6),
    )(core, o_mine, o_other, wo, wo)


def dx_kernel(sc, q_mine, q_other, kv_mine, kv_other, wq_mine, wq_other, wkv, out_ref, kv):
    hd = HD

    @pl.when(pl.program_id(0) == 0)
    def _():
        for n, src in ((sc[0], kv_mine), (1 - sc[0], kv_other)):
            kv[:, pl.ds(pl.multiple_of(n * hd, hd), hd)] = src[:, :hd]
            kv[:, pl.ds(pl.multiple_of((2 + n) * hd, hd), hd)] = src[:, hd:]

    acc = dot_nt(q_mine[...], wq_mine[...]) + dot_nt(q_other[...], wq_other[...])
    out_ref[...] = (acc + dot_nt(kv[...], wkv[...])).astype(BF16)


def grad_rows(core, dq_mine, dq_other, dkv_mine, dkv_other, wq, wkv):
    rows, half, model, tile = DUO, dq_mine.shape[1], wq.shape[0], DUO
    mine = lambda i, s: (s[0], 0)
    near, far = lambda i, s: (i, s[0]), lambda i, s: (i, 1 - s[0])
    return pl.pallas_call(
        dx_kernel,
        out_shape=jax.ShapeDtypeStruct((rows, model), BF16),
        grid_spec=pltpu.PrefetchScalarGridSpec(
            num_scalar_prefetch=1,
            grid=(model // tile,),
            in_specs=[
                *[pl.BlockSpec((rows, n), mine) for n in (half, half, BLK, BLK)],
                *[pl.BlockSpec((tile, half), at) for at in (near, far)],
                pl.BlockSpec((tile, DUO), lambda i, s: (i, 0)),
            ],
            out_specs=pl.BlockSpec((rows, tile), lambda i, s: (0, i)),
            scratch_shapes=[pltpu.VMEM((rows, DUO), BF16)],
        ),
        compiler_params=params(),
        cost_estimate=cost(4 * rows * half * model * 1.25, 14e6),
    )(core, dq_mine, dq_other, dkv_mine, dkv_other, wq, wq, wkv)


PIECES = ((0, DUO), (1, DUO), (0, BLK), (1, BLK), (0, BLK), (1, BLK))
STARTS = (0, DUO, HALF, 1280, 1536, 1792)


def piece_copies(core, arrays, dst, sem, along):
    copies = []
    for n, ((flip, size), start) in enumerate(zip(PIECES, STARTS)):
        at = pl.ds(pl.multiple_of((1 - core if flip else core) * size, size), size)
        src = arrays[n // 2]
        if along:
            copies.append(pltpu.make_async_copy(src.at[:, at], dst.at[:, start : start + size], sem))
        else:
            copies.append(pltpu.make_async_copy(src.at[at, :], dst.at[start : start + size, :], sem))
    return copies


def dwq_kernel(sc, *refs):
    xts, mine, other, kv_in = refs[:3], refs[3:6], refs[6:9], refs[9:11]
    out_ref, gk_ref, gv_ref, dq, kv, sems = refs[11:]
    g, i = pl.program_id(0), pl.program_id(1)
    tile, core, hd = out_ref.shape[0], sc[0], HD
    spans = [slice(0, HALF), slice(HALF, HALF + DUO), slice(HALF + DUO, SEQ)]
    first = [pltpu.make_async_copy(a, dq.at[0, at, :], sems.at[0]) for a, at in zip(mine, spans)]
    later = [pltpu.make_async_copy(a, dq.at[1, at, :], sems.at[1]) for a, at in zip(other, spans)]
    later += [
        pltpu.make_async_copy(a, kv.at[:, n * BLK : (n + 1) * BLK], sems.at[1]) for n, a in enumerate(kv_in)
    ]

    def when(gg, ii, copies, start):
        @pl.when((g == gg) & (i == ii))
        def _():
            for cp in copies:
                cp.start() if start else cp.wait()

    when(0, 0, first, True)
    when(0, 1, later, True)
    when(0, 0, first, False)
    when(1, 0, later, False)

    acc = sum(dot(x[...], dq[g, at, :]) for x, at in zip(xts, spans))
    flat = out_ref.reshape(tile * 8, hd)
    for h in range(8):
        flat[pl.ds(h, tile, stride=8), :] = acc[:, h * hd : (h + 1) * hd]

    @pl.when(g == 1)
    def _():
        k_flat, v_flat = gk_ref.reshape(tile * 2, hd), gv_ref.reshape(tile * 2, hd)
        both = sum(dot(x[...], kv[at, :]) for x, at in zip(xts, spans))
        for n, head in enumerate((core, 1 - core)):
            k_flat[pl.ds(head, tile, stride=2), :] = both[:, 2 * n * hd : (2 * n + 1) * hd]
            v_flat[pl.ds(head, tile, stride=2), :] = both[:, (2 * n + 1) * hd : (2 * n + 2) * hd]


def grad_wq(core, xts, mine, other, kvm, kvo):
    model, half, tile = xts[0].shape[0], mine[0].shape[1], TILE_WQ
    tiles = model // tile
    small = pl.BlockSpec((tile, 2, HD), lambda g, i, s: (i * g, 0, 0))
    return pl.pallas_call(
        dwq_kernel,
        out_shape=(
            jax.ShapeDtypeStruct((model, 16, HD), F32),
            jax.ShapeDtypeStruct((model, 2, HD), F32),
            jax.ShapeDtypeStruct((model, 2, HD), F32),
        ),
        grid_spec=pltpu.PrefetchScalarGridSpec(
            num_scalar_prefetch=1,
            grid=(2, tiles),
            in_specs=[pl.BlockSpec((tile, x.shape[1]), lambda g, i, s: (i, 0)) for x in xts]
            + [pl.BlockSpec(memory_space=pl.ANY)] * 8,
            out_specs=(
                pl.BlockSpec((tile, 8, HD), lambda g, i, s: (i, (s[0] + g) % 2, 0)),
                small,
                small,
            ),
            scratch_shapes=[
                pltpu.VMEM((2, SEQ, half), BF16),
                pltpu.VMEM((SEQ, DUO), BF16),
                pltpu.SemaphoreType.DMA((2,)),
            ],
        ),
        compiler_params=params(2),
        cost_estimate=cost(2 * SEQ * model * (2 * half + DUO), 40e6),
    )(core, *xts, *mine, *other, kvm, kvo)


def dwo_kernel(sc, *refs):
    mine, other, ys, (out_ref, o_all, y_all, sems) = refs[:3], refs[3:6], refs[6:12], refs[12:]
    j, g, i = pl.program_id(0), pl.program_id(1), pl.program_id(2)
    tile, wide = out_ref.shape
    o_first = piece_copies(sc[0], mine, o_all.at[0], sems.at[0], True)
    o_later = piece_copies(sc[0], other, o_all.at[1], sems.at[1], True)
    y_copies = [
        [
            pltpu.make_async_copy(
                y.at[y.shape[0] - r if r == BLK else 0 :, n * wide : (n + 1) * wide], y_all.at[n, s : s + r, :], sems.at[2 + n]
            )
            for y, s, (_, r) in zip(ys, STARTS, PIECES)
        ]
        for n in range(2)
    ]

    def when(jj, gg, ii, copies, start):
        @pl.when((j == jj) & (g == gg) & (i == ii))
        def _():
            for cp in copies:
                cp.start() if start else cp.wait()

    when(0, 0, 0, y_copies[0] + o_first, True)
    when(0, 0, 1, o_later, True)
    when(0, 1, 0, y_copies[1], True)
    when(0, 0, 0, y_copies[0] + o_first, False)
    when(0, 1, 0, o_later, False)
    when(1, 0, 0, y_copies[1], False)
    out_ref[...] = dot(o_all[g, pl.ds(pl.multiple_of(i * tile, tile), tile), :], y_all[j])


def grad_wo(core, ys, mine, other):
    model, half, tile, wide = ys[0].shape[1], mine[0].shape[0], DUO, HALF
    steps = half // tile
    return pl.pallas_call(
        dwo_kernel,
        out_shape=jax.ShapeDtypeStruct((2 * half, model), F32),
        grid_spec=pltpu.PrefetchScalarGridSpec(
            num_scalar_prefetch=1,
            grid=(2, 2, steps),
            in_specs=[pl.BlockSpec(memory_space=pl.ANY)] * 12,
            out_specs=pl.BlockSpec((tile, wide), lambda j, g, i, s: ((s[0] + g) % 2 * steps + i, j)),
            scratch_shapes=[
                pltpu.VMEM((2, half, SEQ), BF16),
                pltpu.VMEM((2, SEQ, wide), BF16),
                pltpu.SemaphoreType.DMA((4,)),
            ],
        ),
        compiler_params=params(3),
        cost_estimate=cost(4 * SEQ * model * half, 40e6),
    )(core, *mine, *other, *ys)


def solution(mesh):
    row_spec = P(("dp", "cp"), None)
    rep_spec = P(None, None, None)
    part_spec = P("dp", None, None)
    core_swap = [(0, 1), (1, 0), (2, 3), (3, 2)]
    chip_swap = [(0, 2), (2, 0), (1, 3), (3, 1)]

    def device_layer(x, dy, w_query, w_key, w_value, w_out):
        _, model = x.shape
        num_heads, hd = w_query.shape[1:]
        kv_heads = w_key.shape[1]
        scale = hd ** -0.5
        rank = lax.axis_index("cp").astype(jnp.int32)
        c = rank & 1
        core = c.reshape(1)
        devs = [rank, rank ^ 1, rank ^ 2, rank ^ 3]
        kv_pos = [p for e in devs for p in (e, 7 - e)]
        own_slots = [p for e in devs[:2] for p in ((e & 1) * 2, (e & 1) * 2 + 1)]
        far_slots = []
        for e in devs[2:]:
            far_slots += [jnp.where((e & 1) == 1, 4, 6) + (e & 1), jnp.where((e & 1) == 0, 4, 6) + (e & 1)]
        pos_a = [jnp.where((e & 1) == 0, 7 - e, e) for e in devs[2:]]
        pos_b = [jnp.where((e & 1) == 0, e, 7 - e) for e in devs[2:]]
        far = [c, 1 - c]
        tail = own_slots + far_slots + [c]
        sc_chip = jnp.stack(kv_pos + kv_pos[:4] + own_slots + tail)
        sc_a = jnp.stack(kv_pos + pos_a * 2 + far * 2 + tail)
        sc_b = jnp.stack(kv_pos + pos_b * 2 + far * 2 + tail)

        to_core = lambda v: lax.ppermute(v, "cp", core_swap)
        to_chip = lambda v: lax.ppermute(v, "cp", chip_swap)

        wk = w_key.reshape(model * kv_heads, hd)
        wv = w_value.reshape(model * kv_heads, hd)
        wo = w_out.reshape(num_heads * hd, model)
        x_p = to_core(x)
        dy_p = to_core(dy)

        kv, wkv, r_a, r_b = project_kv(core, x, dy, wk, wv)
        far_kv, kv_p = to_chip(kv), to_core(kv)
        w_s, _ = lax.optimization_barrier((w_query, kv))
        r_a, r_b = to_chip(r_a), to_chip(r_b)
        wq = flat_heads(w_s)
        kv_r, wq = lax.optimization_barrier((far_kv, wq))
        kv_rp = to_core(kv_r)
        pieces = (kv, kv_p, kv_r, kv_rp)

        o_c, dq_c, part, xt_c = attention(
            sc_chip, wq, wo, (x, x_p), (dy, dy_p), 0, pieces, None, False, scale)
        r_a, o_c, dq_c = lax.optimization_barrier((r_a, o_c, dq_c))
        r_pa, o_co, dq_co = to_core(r_a), to_core(o_c), to_core(dq_c)

        o_a, dq_a, part, xt_a = attention(sc_a, wq, wo, (r_a, r_pa), (r_a, r_pa), BLK, pieces, part, False, scale)
        r_b, o_a, dq_a = lax.optimization_barrier((r_b, o_a, dq_a))
        r_pb, o_ao, dq_ao = to_core(r_b), to_core(o_a), to_core(dq_a)

        o_b, dq_b, dkv, xt_b = attention(sc_b, wq, wo, (r_b, r_pb), (r_b, r_pb), BLK, pieces, part, True, scale)
        o_co, dkv = lax.optimization_barrier((o_co, dkv))
        dkv_o, o_bo, dq_bo = to_core(dkv), to_core(o_b), to_core(dq_b)
        y = out_rows(core, o_c, o_co, wo)

        ys = (dy, dy_p, r_a, r_pa, r_b, r_pb)
        gwo = grad_wo(core, ys, (o_c, o_a, o_b), (o_co, o_ao, o_bo))
        dx = grad_rows(core, dq_c, dq_co, dkv, dkv_o, wq, wkv)
        gwq, gwk, gwv = grad_wq(core, (xt_c, xt_a, xt_b), (dq_c, dq_a, dq_b), (dq_co, dq_ao, dq_bo), dkv, dkv_o)
        return y, dx, gwq, gwk, gwv, gwo.reshape(num_heads, hd, model)

    return jax.shard_map(
        device_layer,
        mesh=mesh,
        in_specs=(row_spec, row_spec, rep_spec, rep_spec, rep_spec, rep_spec),
        out_specs=(row_spec, row_spec, part_spec, part_spec, part_spec, part_spec),
        check_vma=False,
    )
```

```python
import functools
import math

import jax
import jax.numpy as jnp
import numpy as np
from jax import lax
from jax.experimental import pallas as pl
from jax.experimental.pallas import tpu as pltpu
from jax.sharding import PartitionSpec as P


BLK = 256
HD = 128
DUO = 512
HALF = 1024
SEQ = 2048
TILE_WQ = 512
LOW = -3.0e38
F32 = jnp.float32
BF16 = jnp.bfloat16


def dot(a, b):
    return jnp.dot(a, b, preferred_element_type=F32)


def dot_nt(a, b):
    return lax.dot_general(a, b, (((1,), (1,)), ((), ())), preferred_element_type=F32)


def params(n=1, mib=60):
    return pltpu.CompilerParams(
        dimension_semantics=("arbitrary",) * n, vmem_limit_bytes=mib * HALF * HALF
    )


def cost(flops, nbytes):
    return pl.CostEstimate(flops=int(flops), bytes_accessed=int(nbytes), transcendentals=0)


def heads_kernel(perm_ref, w_hbm, out_hbm, w_in, w_out, in_sem, out_sem):
    chunks, rows, num, hd = w_in.shape
    group = perm_ref.shape[0]
    loads = [
        pltpu.make_async_copy(w_hbm.at[c * rows : (c + 1) * rows], w_in.at[c], in_sem.at[c]) for c in range(chunks)
    ]
    stores = [
        pltpu.make_async_copy(w_out.at[c], out_hbm.at[c * rows : (c + 1) * rows, :], out_sem.at[c]) for c in range(chunks)
    ]
    for cp in loads:
        cp.start()

    def chunk(c, _):
        pltpu.make_async_copy(w_hbm.at[:rows], w_in.at[c], in_sem.at[c]).wait()
        flat = w_in.at[c].reshape(rows * num, hd)
        for g in range(0, rows // 16, 2):
            pair = [flat[(g + n) * group : (g + n + 1) * group, :] for n in range(2)]
            res = dot(perm_ref[...], jnp.concatenate(pair, axis=1)).astype(BF16)
            for n in range(2):
                for h in range(num):
                    w_out[c, (g + n) * 16 : (g + n + 1) * 16, h * hd : (h + 1) * hd] = res[
                        h * 16 : (h + 1) * 16, n * hd : (n + 1) * hd
                    ]
        at = pl.ds(pl.multiple_of(c * rows, rows), rows)
        pltpu.make_async_copy(w_out.at[c], out_hbm.at[at, :], out_sem.at[c]).start()
        return 0

    lax.fori_loop(0, chunks, chunk, 0)
    for cp in stores:
        cp.wait()


def gather_heads(num, rows):
    row = np.arange(num * rows)
    return jnp.asarray((row % rows * num + row // rows)[:, None] == row[None, :], BF16)


def flat_heads(w):
    model, num, hd = w.shape
    chunks = 8
    rows = model // chunks
    return pl.pallas_call(
        heads_kernel,
        out_shape=jax.ShapeDtypeStruct((model, num * hd), BF16),
        in_specs=[pl.BlockSpec(memory_space=pltpu.VMEM), pl.BlockSpec(memory_space=pl.ANY)],
        out_specs=pl.BlockSpec(memory_space=pl.ANY),
        scratch_shapes=[
            pltpu.VMEM((chunks, rows, num, hd), BF16),
            pltpu.VMEM((chunks, rows, num * hd), BF16),
            pltpu.SemaphoreType.DMA((chunks,)),
            pltpu.SemaphoreType.DMA((chunks,)),
        ],
        compiler_params=pltpu.CompilerParams(vmem_limit_bytes=params(1).vmem_limit_bytes),
        cost_estimate=cost(4e9, 4 * model * num * hd),
    )(gather_heads(num, 16), w)


def kv_kernel(sc, x_ref, dy_ref, wk_ref, wv_ref, perm_ref, out_ref, w_ref, rows_a, rows_b):
    @pl.when(pl.program_id(0) == 0)
    def _():
        for g in range(w_ref.shape[0] // HD):
            rows = slice(g * BLK, (g + 1) * BLK)
            pair = jnp.concatenate([wk_ref[rows, :], wv_ref[rows, :]], axis=1)
            res = dot(perm_ref[...], pair).astype(BF16)
            for h in range(2):
                for v in range(2):
                    col = (v * 2 + h) * HD
                    w_ref[g * HD : (g + 1) * HD, col : col + HD] = res[h * HD : (h + 1) * HD, v * HD : (v + 1) * HD]

    out_ref[...] = dot(x_ref[...], w_ref[...]).astype(BF16)

    @pl.when(pl.program_id(0) == 1 - sc[0])
    def _():
        rows_a[:BLK, :] = x_ref[...]
        rows_a[BLK:, :] = dy_ref[...]

    @pl.when(pl.program_id(0) == sc[0])
    def _():
        rows_b[:BLK, :] = x_ref[...]
        rows_b[BLK:, :] = dy_ref[...]


def project_kv(core, x, dy, wk, wv):
    rows, depth = x.shape
    row = pl.BlockSpec((BLK, depth), lambda i, s: (i, 0))
    fixed = lambda shape: pl.BlockSpec(shape, lambda i, s: (0, 0))
    chunk = jax.ShapeDtypeStruct((rows, depth), BF16)
    return pl.pallas_call(
        kv_kernel,
        out_shape=(jax.ShapeDtypeStruct((rows, DUO), BF16), jax.ShapeDtypeStruct((depth, DUO), BF16), chunk, chunk),
        grid_spec=pltpu.PrefetchScalarGridSpec(
            num_scalar_prefetch=1,
            grid=(rows // BLK,),
            in_specs=[row, row, fixed(wk.shape), fixed(wv.shape), fixed((BLK, BLK))],
            out_specs=(pl.BlockSpec((BLK, DUO), lambda i, s: (i, 0)), fixed((depth, DUO))) + (fixed((rows, depth)),) * 2,
        ),
        compiler_params=params(),
        cost_estimate=cost(2 * rows * depth * DUO, 8e6),
    )(core, x, dy, wk, wv, gather_heads(2, HD))


def ranks(rank):
    return rank, rank + 1 - rank % 2 * 2, (rank + 2) % 4, 3 - rank


def block_at(kind, rank, i):
    own, pair, far, far_pair = ranks(rank)
    if kind == "near":
        e = jnp.where(i < 2, own, pair)
        return jnp.where(i % 2 == 0, e, 7 - e)
    e = jnp.where(i == 0, far, far_pair)
    return jnp.where(e % 2 == (1 if kind == "a" else 0), e, 7 - e)


def slot_at(kind, rank, i):
    if kind == "near":
        return (rank + i // 2) % 2 * 2 + i % 2
    return (rank + i) % 2


def attn_kernel(kind, heads, scale, steps, base, sc, wq_hbm, wo_hbm, *refs):
    x_hbm, dy_hbm, kv_hbm, refs = refs[:2], refs[2:4], refs[4:8], refs[8:]
    first, final = kind == "near", kind == "b"
    if first:
        o_ref, dq_ref, dkv_ref, xt_ref = refs[:4]
        scratch = refs[4:]
    else:
        init_hbm, o_ref, dq_ref, dkv_ref, xt_ref = refs[:5]
        scratch = refs[5:]
    ks, vs, kt, vt, dk, dv, qt, dot_t, qst, dost, s_ref, p_ref, ds_ref, ot, dqt, m_ref, l_ref, ref, wq, wo, xs, dys, w_sem, x_sem, dy_sem, g_sem = scratch
    step = pl.program_id(0)
    hd = HD
    c2 = scale * math.log2(math.e)

    rank = sc[0]
    pos = [p for e in ranks(rank) for p in (e, 7 - e)]
    core = pl.multiple_of(rank % 2 * heads * hd, heads * hd)
    load_kv = []
    for n, p in enumerate(pos):
        src = kv_hbm[n // 2].at[n % 2 * BLK : (n % 2 + 1) * BLK, :]
        at = pl.ds(pl.multiple_of(p * BLK, BLK), BLK)
        for v, dst in enumerate((ks, vs)):
            col = pl.ds(pl.multiple_of((2 * v + rank % 2) * hd, hd), hd)
            load_kv.append(pltpu.make_async_copy(src.at[:, col], dst.at[at, :], g_sem.at[0]))

    def grads(hbm, out):
        pairs = [(hbm.at[:, :hd], dk), (hbm.at[:, hd:], dv)]
        return [pltpu.make_async_copy(*(p[::-1] if out else p), g_sem.at[1]) for p in pairs]

    load_wq, load_wo = [], []
    for n in range(4):
        span = slice(n * DUO, (n + 1) * DUO)
        load_wq.append(pltpu.make_async_copy(wq_hbm.at[span, pl.ds(core, heads * hd)], wq.at[span, :], w_sem.at[0]))
        rows = heads * hd // 4
        dst = wo.at[n * rows : (n + 1) * rows, :]
        load_wo.append(pltpu.make_async_copy(wo_hbm.at[pl.ds(core + n * rows, rows), :], dst, w_sem.at[1]))

    def load_rows(n):
        piece, row = divmod(n, steps // 2)
        src = pl.ds(row * BLK, BLK)
        return (
            pltpu.make_async_copy(x_hbm[piece].at[src, :], xs.at[n % 2], x_sem.at[n % 2]),
            pltpu.make_async_copy(dy_hbm[piece].at[pl.ds(base + row * BLK, BLK), :], dys.at[n % 2], dy_sem.at[n % 2]),
        )

    @pl.when(step == 0)
    def _():
        load_x, load_dy = load_rows(0)
        for cp in load_kv:
            cp.start()
        load_x.start()
        for cp in load_wq:
            cp.start()
        load_dy.start()
        for cp in load_wo:
            cp.start()
        for cp in [] if first else grads(init_hbm, False):
            cp.start()

    for n in range(1, steps):

        @pl.when(step == n - 1)
        def _():
            for cp in load_rows(n):
                cp.start()

    @pl.when(step == 0)
    def _():
        if first:
            dk[...] = jnp.zeros_like(dk)
            dv[...] = jnp.zeros_like(dv)
        for cp in load_kv:
            cp.wait()
        for i in range(8):
            at = slice(i * BLK, (i + 1) * BLK)
            kt[:, at] = ks[at, :].T
            vt[:, at] = vs[at, :].T

    @pl.when(step == 0)
    def _():
        for cp in load_wq:
            cp.wait()

    slot = step % 2
    pltpu.make_async_copy(x_hbm[0].at[0:BLK, :], xs.at[slot], x_sem.at[slot]).wait()
    q = dot(xs[slot], wq[...]).astype(BF16)
    xt_ref[...] = xs[slot].T
    for h in range(heads):
        qh = q[:, h * hd : (h + 1) * hd]
        qst[h * BLK : (h + 1) * BLK, :] = qh
        qt[:, h * BLK : (h + 1) * BLK] = qh.T

    @pl.when(step == 0)
    def _():
        for cp in load_wo:
            cp.wait()

    pltpu.make_async_copy(dy_hbm[0].at[0:BLK, :], dys.at[slot], dy_sem.at[slot]).wait()
    do = dot_nt(dys[slot], wo[...]).astype(BF16)
    for h in range(heads):
        dh = do[:, h * hd : (h + 1) * hd]
        dost[h * BLK : (h + 1) * BLK, :] = dh
        dot_t[:, h * BLK : (h + 1) * BLK] = dh.T

    b = block_at(kind, rank, step)

    def scores(j, h):
        at = pl.ds(pl.multiple_of(j * BLK, BLK), BLK)
        return at, slice(h * BLK, (h + 1) * BLK), dot(ks[at, :], qt[:, h * BLK : (h + 1) * BLK]) * c2

    def rows_of(t):
        return t.reshape(BLK // 8, 8, BLK)

    key = lax.broadcasted_iota(jnp.int32, (BLK, BLK), 0)
    query = lax.broadcasted_iota(jnp.int32, (BLK, BLK), 1)
    for h in range(heads):
        at, span, t = scores(b, h)
        t = jnp.where(key <= query, t, LOW)
        s_ref[at, span] = t
        m8 = jnp.max(rows_of(t), axis=0)
        base = jnp.max(m8, axis=0, keepdims=True)
        ref[:, span] = base
        m_ref[:, span] = m8
        l_ref[:, span] = jnp.sum(jnp.exp2(rows_of(t - base)), axis=0)

    def open_block(j, _):
        for h in range(heads):
            at, span, t = scores(j, h)
            s_ref[at, span] = t
            m_ref[:, span] = jnp.maximum(m_ref[:, span], jnp.max(rows_of(t), axis=0))
            l_ref[:, span] += jnp.sum(jnp.exp2(rows_of(t - ref[:, span])), axis=0)
        return 0

    lax.fori_loop(0, b, open_block, 0)

    @pl.when(jnp.max(m_ref[...] - ref[...]) > 60.0)
    def _():
        ref[...] = jnp.max(m_ref[...], axis=0, keepdims=True)
        l_ref[...] = jnp.zeros_like(l_ref)

        def again(j, _):
            at = pl.ds(pl.multiple_of(j * BLK, BLK), BLK)
            for h in range(heads):
                span = slice(h * BLK, (h + 1) * BLK)
                l_ref[:, span] += jnp.sum(jnp.exp2(rows_of(s_ref[at, span] - ref[:, span])), axis=0)
            return 0

        lax.fori_loop(0, b + 1, again, 0)

    lse = ref[...] + jnp.log2(jnp.sum(l_ref[...], axis=0, keepdims=True))

    ot[...] = jnp.zeros_like(ot)

    def value_block(j, _):
        at = pl.ds(pl.multiple_of(j * BLK, BLK), BLK)
        for h in range(heads):
            span = slice(h * BLK, (h + 1) * BLK)
            p = jnp.exp2(s_ref[at, span] - lse[:, span]).astype(BF16)
            p_ref[at, span] = p
            ot[:, span] += dot(vt[:, at], p)
        return 0

    lax.fori_loop(0, b + 1, value_block, 0)

    o_round = ot[...].astype(BF16)
    delta = jnp.sum(o_round.astype(F32) * dot_t[...].astype(F32), axis=0, keepdims=True)
    for h in range(heads):
        o_ref[h * hd : (h + 1) * hd, :] = o_round[:, h * BLK : (h + 1) * BLK]
    dqt[...] = jnp.zeros_like(dqt)

    def grad_block(j, _):
        at = pl.ds(pl.multiple_of(j * BLK, BLK), BLK)
        dp = dot(vs[at, :], dot_t[...])
        dv[at, :] += dot(p_ref[at, :], dost[...])
        ds = (p_ref[at, :].astype(F32) * (dp - delta)).astype(BF16)
        ds_ref[...] = ds
        dqt[...] += dot(kt[:, at], ds_ref[...])
        dk[at, :] += dot(ds_ref[...], qst[...])
        return 0

    if not first:

        @pl.when(step == 0)
        def _():
            for cp in grads(init_hbm, False):
                cp.wait()

    lax.fori_loop(0, b + 1, grad_block, 0)

    for h in range(heads):
        dq_ref[:, h * hd : (h + 1) * hd] = (dqt[:, h * BLK : (h + 1) * BLK] * scale).astype(BF16).T

    @pl.when(step == steps - 1)
    def _():
        if not final:
            for cp in grads(dkv_ref, True):
                cp.start()
            for cp in grads(dkv_ref, True):
                cp.wait()
        else:
            for n, (p, e) in enumerate(zip(pos, [e for e in ranks(rank) for _ in "ab"])):
                at = pl.ds(pl.multiple_of(p * BLK, BLK), BLK)
                if n < 4:
                    row = e % 2 * 2 + n % 2
                else:
                    row = jnp.where((e + n) % 2 == 1, 4, 6) + e % 2
                out = pl.ds(pl.multiple_of(row * BLK, BLK), BLK)
                dkv_ref[out, :hd] = (dk[at, :] * scale).astype(BF16)
                dkv_ref[out, hd:] = dv[at, :].astype(BF16)


def attention(kind, rank, wq, wo, x_pieces, dy_pieces, base, kv_pieces, init, scale):
    final = kind == "b"
    rows, width, model = 2 * (x_pieces[0].shape[0] - base), wq.shape[1] // 2, wq.shape[0]
    hd = HD
    heads = width // hd
    wide = heads * BLK
    seq = SEQ
    slot = functools.partial(slot_at, kind)
    o_spec = pl.BlockSpec((width, BLK), lambda i, s: (0, slot(s[0], i)))
    out_spec = pl.BlockSpec((BLK, width), lambda i, s: (slot(s[0], i), 0))
    xt_spec = pl.BlockSpec((model, BLK), lambda i, s: (0, slot(s[0], i)))
    dkv_spec = pl.BlockSpec((seq, BLK), lambda i, s: (0, 0)) if final else pl.BlockSpec(memory_space=pl.ANY)
    ins = [wq, wo, *x_pieces, *dy_pieces, *kv_pieces] + ([] if init is None else [init])
    return pl.pallas_call(
        functools.partial(attn_kernel, kind, heads, scale, rows // BLK, base),
        out_shape=(
            jax.ShapeDtypeStruct((width, rows), BF16),
            jax.ShapeDtypeStruct((rows, width), BF16),
            jax.ShapeDtypeStruct((seq, BLK), BF16 if final else F32),
            jax.ShapeDtypeStruct((model, rows), BF16),
        ),
        grid_spec=pltpu.PrefetchScalarGridSpec(
            num_scalar_prefetch=1,
            grid=(rows // BLK,),
            in_specs=[pl.BlockSpec(memory_space=pl.ANY) for _ in ins],
            out_specs=(o_spec, out_spec, dkv_spec, xt_spec),
            scratch_shapes=[
                *[pltpu.VMEM((seq, hd), BF16) for _ in "kv"],
                *[pltpu.VMEM((hd, seq), BF16) for _ in "kv"],
                *[pltpu.VMEM((seq, hd), F32) for _ in "kv"],
                *[pltpu.VMEM((hd, wide), BF16) for _ in "qd"],
                *[pltpu.VMEM((wide, hd), BF16) for _ in "qd"],
                pltpu.VMEM((seq, wide), F32),
                pltpu.VMEM((seq, wide), BF16),
                pltpu.VMEM((BLK, wide), BF16),
                *[pltpu.VMEM((hd, wide), F32) for _ in "od"],
                *[pltpu.VMEM((8, wide), F32) for _ in "ml"],
                pltpu.VMEM((1, wide), F32),
                pltpu.VMEM((model, width), BF16),
                pltpu.VMEM((width, model), BF16),
                *[pltpu.VMEM((2, BLK, model), BF16) for _ in "xd"],
                *[pltpu.SemaphoreType.DMA((2,)) for _ in "wxdg"],
            ],
        ),
        compiler_params=params(1, 63),
        cost_estimate=cost(8e9 * (rows // BLK), 20e6),
    )(rank, *ins)


def y_kernel(sc, o_mine, o_other, w_mine, w_other, out_ref, os):
    half = o_mine.shape[0]

    @pl.when(pl.program_id(0) == 0)
    def _():
        os[:, :half] = o_mine[...].T
        os[:, half:] = o_other[...].T

    out_ref[...] = (dot(os[:, :half], w_mine[...]) + dot(os[:, half:], w_other[...])).astype(BF16)


def out_rows(core, o_mine, o_other, wo):
    rows, half, model, tile = DUO, o_mine.shape[0], wo.shape[1], DUO
    return pl.pallas_call(
        y_kernel,
        out_shape=jax.ShapeDtypeStruct((rows, model), BF16),
        grid_spec=pltpu.PrefetchScalarGridSpec(
            num_scalar_prefetch=1,
            grid=(model // tile,),
            in_specs=[
                pl.BlockSpec((half, rows), lambda i, s: (0, s[0])),
                pl.BlockSpec((half, rows), lambda i, s: (0, s[0])),
                pl.BlockSpec((half, tile), lambda i, s: (s[0], i)),
                pl.BlockSpec((half, tile), lambda i, s: (1 - s[0], i)),
            ],
            out_specs=pl.BlockSpec((rows, tile), lambda i, s: (0, i)),
            scratch_shapes=[pltpu.VMEM((rows, 2 * half), BF16)],
        ),
        compiler_params=params(),
        cost_estimate=cost(4 * rows * half * model, 12e6),
    )(core, o_mine, o_other, wo, wo)


def dx_kernel(sc, q_mine, q_other, kv_mine, kv_other, wq_mine, wq_other, wkv, out_ref, kv):
    hd = HD

    @pl.when(pl.program_id(0) == 0)
    def _():
        for n, src in ((sc[0], kv_mine), (1 - sc[0], kv_other)):
            kv[:, pl.ds(pl.multiple_of(n * hd, hd), hd)] = src[:, :hd]
            kv[:, pl.ds(pl.multiple_of((2 + n) * hd, hd), hd)] = src[:, hd:]

    acc = dot_nt(q_mine[...], wq_mine[...]) + dot_nt(q_other[...], wq_other[...])
    out_ref[...] = (acc + dot_nt(kv[...], wkv[...])).astype(BF16)


def grad_rows(core, dq_mine, dq_other, dkv_mine, dkv_other, wq, wkv):
    rows, half, model, tile = DUO, dq_mine.shape[1], wq.shape[0], DUO
    mine = lambda i, s: (s[0], 0)
    near, far = lambda i, s: (i, s[0]), lambda i, s: (i, 1 - s[0])
    return pl.pallas_call(
        dx_kernel,
        out_shape=jax.ShapeDtypeStruct((rows, model), BF16),
        grid_spec=pltpu.PrefetchScalarGridSpec(
            num_scalar_prefetch=1,
            grid=(model // tile,),
            in_specs=[
                *[pl.BlockSpec((rows, n), mine) for n in (half, half, BLK, BLK)],
                *[pl.BlockSpec((tile, half), at) for at in (near, far)],
                pl.BlockSpec((tile, DUO), lambda i, s: (i, 0)),
            ],
            out_specs=pl.BlockSpec((rows, tile), lambda i, s: (0, i)),
            scratch_shapes=[pltpu.VMEM((rows, DUO), BF16)],
        ),
        compiler_params=params(),
        cost_estimate=cost(4 * rows * half * model * 1.25, 14e6),
    )(core, dq_mine, dq_other, dkv_mine, dkv_other, wq, wq, wkv)


PIECES = ((0, DUO), (1, DUO), (0, BLK), (1, BLK), (0, BLK), (1, BLK))
STARTS = (0, DUO, HALF, 1280, 1536, 1792)


def piece_copies(core, arrays, dst, sem, along):
    copies = []
    for n, ((flip, size), start) in enumerate(zip(PIECES, STARTS)):
        at = pl.ds(pl.multiple_of((1 - core if flip else core) * size, size), size)
        src = arrays[n // 2]
        if along:
            copies.append(pltpu.make_async_copy(src.at[:, at], dst.at[:, start : start + size], sem))
        else:
            copies.append(pltpu.make_async_copy(src.at[at, :], dst.at[start : start + size, :], sem))
    return copies


def dwq_kernel(sc, *refs):
    xts, mine, other, kv_in = refs[:3], refs[3:6], refs[6:9], refs[9:11]
    out_ref, gk_ref, gv_ref, dq, kv, sems = refs[11:]
    g, i = pl.program_id(0), pl.program_id(1)
    tile, core, hd = out_ref.shape[0], sc[0], HD
    spans = [slice(0, HALF), slice(HALF, HALF + DUO), slice(HALF + DUO, SEQ)]
    first = [pltpu.make_async_copy(a, dq.at[0, at, :], sems.at[0]) for a, at in zip(mine, spans)]
    later = [pltpu.make_async_copy(a, dq.at[1, at, :], sems.at[1]) for a, at in zip(other, spans)]
    later += [
        pltpu.make_async_copy(a, kv.at[:, n * BLK : (n + 1) * BLK], sems.at[1]) for n, a in enumerate(kv_in)
    ]

    def when(gg, ii, copies, start):
        @pl.when((g == gg) & (i == ii))
        def _():
            for cp in copies:
                cp.start() if start else cp.wait()

    when(0, 0, first, True)
    when(0, 1, later, True)
    when(0, 0, first, False)
    when(1, 0, later, False)

    acc = sum(dot(x[...], dq[g, at, :]) for x, at in zip(xts, spans))
    flat = out_ref.reshape(tile * 8, hd)
    for h in range(8):
        flat[pl.ds(h, tile, stride=8), :] = acc[:, h * hd : (h + 1) * hd]

    @pl.when(g == 1)
    def _():
        k_flat, v_flat = gk_ref.reshape(tile * 2, hd), gv_ref.reshape(tile * 2, hd)
        both = sum(dot(x[...], kv[at, :]) for x, at in zip(xts, spans))
        for n, head in enumerate((core, 1 - core)):
            k_flat[pl.ds(head, tile, stride=2), :] = both[:, 2 * n * hd : (2 * n + 1) * hd]
            v_flat[pl.ds(head, tile, stride=2), :] = both[:, (2 * n + 1) * hd : (2 * n + 2) * hd]


def grad_wq(core, xts, mine, other, kvm, kvo):
    model, half, tile = xts[0].shape[0], mine[0].shape[1], TILE_WQ
    tiles = model // tile
    small = pl.BlockSpec((tile, 2, HD), lambda g, i, s: (i * g, 0, 0))
    return pl.pallas_call(
        dwq_kernel,
        out_shape=(
            jax.ShapeDtypeStruct((model, 16, HD), F32),
            jax.ShapeDtypeStruct((model, 2, HD), F32),
            jax.ShapeDtypeStruct((model, 2, HD), F32),
        ),
        grid_spec=pltpu.PrefetchScalarGridSpec(
            num_scalar_prefetch=1,
            grid=(2, tiles),
            in_specs=[pl.BlockSpec((tile, x.shape[1]), lambda g, i, s: (i, 0)) for x in xts]
            + [pl.BlockSpec(memory_space=pl.ANY)] * 8,
            out_specs=(
                pl.BlockSpec((tile, 8, HD), lambda g, i, s: (i, (s[0] + g) % 2, 0)),
                small,
                small,
            ),
            scratch_shapes=[
                pltpu.VMEM((2, SEQ, half), BF16),
                pltpu.VMEM((SEQ, DUO), BF16),
                pltpu.SemaphoreType.DMA((2,)),
            ],
        ),
        compiler_params=params(2),
        cost_estimate=cost(2 * SEQ * model * (2 * half + DUO), 40e6),
    )(core, *xts, *mine, *other, kvm, kvo)


def dwo_kernel(sc, *refs):
    mine, other, ys, (out_ref, o_all, y_all, sems) = refs[:3], refs[3:6], refs[6:12], refs[12:]
    j, g, i = pl.program_id(0), pl.program_id(1), pl.program_id(2)
    tile, wide = out_ref.shape
    o_first = piece_copies(sc[0], mine, o_all.at[0], sems.at[0], True)
    o_later = piece_copies(sc[0], other, o_all.at[1], sems.at[1], True)
    y_copies = [
        [
            pltpu.make_async_copy(
                y.at[y.shape[0] - r if r == BLK else 0 :, n * wide : (n + 1) * wide], y_all.at[n, s : s + r, :], sems.at[2 + n]
            )
            for y, s, (_, r) in zip(ys, STARTS, PIECES)
        ]
        for n in range(2)
    ]

    def when(jj, gg, ii, copies, start):
        @pl.when((j == jj) & (g == gg) & (i == ii))
        def _():
            for cp in copies:
                cp.start() if start else cp.wait()

    when(0, 0, 0, y_copies[0] + o_first, True)
    when(0, 0, 1, o_later, True)
    when(0, 1, 0, y_copies[1], True)
    when(0, 0, 0, y_copies[0] + o_first, False)
    when(0, 1, 0, o_later, False)
    when(1, 0, 0, y_copies[1], False)
    out_ref[...] = dot(o_all[g, pl.ds(pl.multiple_of(i * tile, tile), tile), :], y_all[j])


def grad_wo(core, ys, mine, other):
    model, half, tile, wide = ys[0].shape[1], mine[0].shape[0], DUO, HALF
    steps = half // tile
    return pl.pallas_call(
        dwo_kernel,
        out_shape=jax.ShapeDtypeStruct((2 * half, model), F32),
        grid_spec=pltpu.PrefetchScalarGridSpec(
            num_scalar_prefetch=1,
            grid=(2, 2, steps),
            in_specs=[pl.BlockSpec(memory_space=pl.ANY)] * 12,
            out_specs=pl.BlockSpec((tile, wide), lambda j, g, i, s: ((s[0] + g) % 2 * steps + i, j)),
            scratch_shapes=[
                pltpu.VMEM((2, half, SEQ), BF16),
                pltpu.VMEM((2, SEQ, wide), BF16),
                pltpu.SemaphoreType.DMA((4,)),
            ],
        ),
        compiler_params=params(3),
        cost_estimate=cost(4 * SEQ * model * half, 40e6),
    )(core, *mine, *other, *ys)


def solution(mesh):
    row_spec = P(("dp", "cp"), None)
    rep_spec = P(None, None, None)
    part_spec = P("dp", None, None)
    core_swap = [(0, 1), (1, 0), (2, 3), (3, 2)]
    chip_swap = [(0, 2), (2, 0), (1, 3), (3, 1)]

    def device_layer(x, dy, w_query, w_key, w_value, w_out):
        _, model = x.shape
        num_heads, hd = w_query.shape[1:]
        kv_heads = w_key.shape[1]
        scale = hd ** -0.5
        rank = lax.axis_index("cp").astype(jnp.int32)
        c = rank & 1
        core = c.reshape(1)
        rank = rank.reshape(1)

        to_core = lambda v: lax.ppermute(v, "cp", core_swap)
        to_chip = lambda v: lax.ppermute(v, "cp", chip_swap)

        wk = w_key.reshape(model * kv_heads, hd)
        wv = w_value.reshape(model * kv_heads, hd)
        wo = w_out.reshape(num_heads * hd, model)
        x_p = to_core(x)
        dy_p = to_core(dy)

        kv, wkv, r_a, r_b = project_kv(core, x, dy, wk, wv)
        far_kv, kv_p = to_chip(kv), to_core(kv)
        w_s, _ = lax.optimization_barrier((w_query, kv))
        r_a, r_b = to_chip(r_a), to_chip(r_b)
        wq = flat_heads(w_s)
        kv_r, wq = lax.optimization_barrier((far_kv, wq))
        kv_rp = to_core(kv_r)
        pieces = (kv, kv_p, kv_r, kv_rp)

        o_c, dq_c, part, xt_c = attention(
            "near", rank, wq, wo, (x, x_p), (dy, dy_p), 0, pieces, None, scale)
        r_a, o_c, dq_c = lax.optimization_barrier((r_a, o_c, dq_c))
        r_pa, o_co, dq_co = to_core(r_a), to_core(o_c), to_core(dq_c)

        o_a, dq_a, part, xt_a = attention("a", rank, wq, wo, (r_a, r_pa), (r_a, r_pa), BLK, pieces, part, scale)
        r_b, o_a, dq_a = lax.optimization_barrier((r_b, o_a, dq_a))
        r_pb, o_ao, dq_ao = to_core(r_b), to_core(o_a), to_core(dq_a)

        o_b, dq_b, dkv, xt_b = attention("b", rank, wq, wo, (r_b, r_pb), (r_b, r_pb), BLK, pieces, part, scale)
        o_co, dkv = lax.optimization_barrier((o_co, dkv))
        dkv_o, o_bo, dq_bo = to_core(dkv), to_core(o_b), to_core(dq_b)
        y = out_rows(core, o_c, o_co, wo)

        ys = (dy, dy_p, r_a, r_pa, r_b, r_pb)
        gwo = grad_wo(core, ys, (o_c, o_a, o_b), (o_co, o_ao, o_bo))
        dx = grad_rows(core, dq_c, dq_co, dkv, dkv_o, wq, wkv)
        gwq, gwk, gwv = grad_wq(core, (xt_c, xt_a, xt_b), (dq_c, dq_a, dq_b), (dq_co, dq_ao, dq_bo), dkv, dkv_o)
        return y, dx, gwq, gwk, gwv, gwo.reshape(num_heads, hd, model)

    return jax.shard_map(
        device_layer,
        mesh=mesh,
        in_specs=(row_spec, row_spec, rep_spec, rep_spec, rep_spec, rep_spec),
        out_specs=(row_spec, row_spec, part_spec, part_spec, part_spec, part_spec),
        check_vma=False,
    )
```

```python
import functools
import math

import jax
import jax.numpy as jnp
import numpy as np
from jax import lax
from jax.experimental import pallas as pl
from jax.experimental.pallas import tpu as pltpu
from jax.sharding import PartitionSpec as P


BLK = 256
HD = 128
DUO = 512
HALF = 1024
SEQ = 2048
TILE_WQ = 512
LARGE = 2.0**60
LOW = -3.0e38
F32 = jnp.float32
BF16 = jnp.bfloat16


def dot(a, b):
    return jnp.dot(a, b, preferred_element_type=F32)


def dot_nt(a, b):
    return lax.dot_general(a, b, (((1,), (1,)), ((), ())), preferred_element_type=F32)


def params(n=1, mib=60):
    return pltpu.CompilerParams(
        dimension_semantics=("arbitrary",) * n, vmem_limit_bytes=mib * HALF * HALF
    )


def cost(flops, nbytes):
    return pl.CostEstimate(flops=int(flops), bytes_accessed=int(nbytes), transcendentals=0)


def heads_kernel(perm_ref, w_hbm, out_hbm, w_in, w_out, in_sem, out_sem):
    chunks, rows, num, hd = w_in.shape
    group = perm_ref.shape[0]
    loads = [
        pltpu.make_async_copy(w_hbm.at[c * rows : (c + 1) * rows], w_in.at[c], in_sem.at[c]) for c in range(chunks)
    ]
    stores = [
        pltpu.make_async_copy(w_out.at[c], out_hbm.at[c * rows : (c + 1) * rows, :], out_sem.at[c]) for c in range(chunks)
    ]
    for cp in loads:
        cp.start()

    def chunk(c, _):
        pltpu.make_async_copy(w_hbm.at[:rows], w_in.at[c], in_sem.at[c]).wait()
        flat = w_in.at[c].reshape(rows * num, hd)
        for g in range(0, rows // 16, 2):
            pair = [flat[(g + n) * group : (g + n + 1) * group, :] for n in range(2)]
            res = dot(perm_ref[...], jnp.concatenate(pair, axis=1)).astype(BF16)
            for n in range(2):
                for h in range(num):
                    w_out[c, (g + n) * 16 : (g + n + 1) * 16, h * hd : (h + 1) * hd] = res[
                        h * 16 : (h + 1) * 16, n * hd : (n + 1) * hd
                    ]
        at = pl.ds(pl.multiple_of(c * rows, rows), rows)
        pltpu.make_async_copy(w_out.at[c], out_hbm.at[at, :], out_sem.at[c]).start()
        return 0

    lax.fori_loop(0, chunks, chunk, 0)
    for cp in stores:
        cp.wait()


def gather_heads(num, rows):
    row = np.arange(num * rows)
    return jnp.asarray((row % rows * num + row // rows)[:, None] == row[None, :], BF16)


def flat_heads(w):
    model, num, hd = w.shape
    chunks = 8
    rows = model // chunks
    return pl.pallas_call(
        heads_kernel,
        out_shape=jax.ShapeDtypeStruct((model, num * hd), BF16),
        in_specs=[pl.BlockSpec(memory_space=pltpu.VMEM), pl.BlockSpec(memory_space=pl.ANY)],
        out_specs=pl.BlockSpec(memory_space=pl.ANY),
        scratch_shapes=[
            pltpu.VMEM((chunks, rows, num, hd), BF16),
            pltpu.VMEM((chunks, rows, num * hd), BF16),
            pltpu.SemaphoreType.DMA((chunks,)),
            pltpu.SemaphoreType.DMA((chunks,)),
        ],
        compiler_params=pltpu.CompilerParams(vmem_limit_bytes=params(1).vmem_limit_bytes),
        cost_estimate=cost(4e9, 4 * model * num * hd),
    )(gather_heads(num, 16), w)


def kv_kernel(sc, x_ref, dy_ref, wk_ref, wv_ref, perm_ref, out_ref, w_ref, rows_a, rows_b):
    @pl.when(pl.program_id(0) == 0)
    def _():
        for g in range(w_ref.shape[0] // HD):
            rows = slice(g * BLK, (g + 1) * BLK)
            pair = jnp.concatenate([wk_ref[rows, :], wv_ref[rows, :]], axis=1)
            res = dot(perm_ref[...], pair).astype(BF16)
            for h in range(2):
                for v in range(2):
                    col = (v * 2 + h) * HD
                    w_ref[g * HD : (g + 1) * HD, col : col + HD] = res[h * HD : (h + 1) * HD, v * HD : (v + 1) * HD]

    out_ref[...] = dot(x_ref[...], w_ref[...]).astype(BF16)

    @pl.when(pl.program_id(0) == 1 - sc[0])
    def _():
        rows_a[:BLK, :] = x_ref[...]
        rows_a[BLK:, :] = dy_ref[...]

    @pl.when(pl.program_id(0) == sc[0])
    def _():
        rows_b[:BLK, :] = x_ref[...]
        rows_b[BLK:, :] = dy_ref[...]


def project_kv(core, x, dy, wk, wv):
    rows, depth = x.shape
    row = pl.BlockSpec((BLK, depth), lambda i, s: (i, 0))
    fixed = lambda shape: pl.BlockSpec(shape, lambda i, s: (0, 0))
    chunk = jax.ShapeDtypeStruct((rows, depth), BF16)
    return pl.pallas_call(
        kv_kernel,
        out_shape=(jax.ShapeDtypeStruct((rows, DUO), BF16), jax.ShapeDtypeStruct((depth, DUO), BF16), chunk, chunk),
        grid_spec=pltpu.PrefetchScalarGridSpec(
            num_scalar_prefetch=1,
            grid=(rows // BLK,),
            in_specs=[row, row, fixed(wk.shape), fixed(wv.shape), fixed((BLK, BLK))],
            out_specs=(pl.BlockSpec((BLK, DUO), lambda i, s: (i, 0)), fixed((depth, DUO))) + (fixed((rows, depth)),) * 2,
        ),
        compiler_params=params(),
        cost_estimate=cost(2 * rows * depth * DUO, 8e6),
    )(core, x, dy, wk, wv, gather_heads(2, HD))


def ranks(rank):
    return rank, rank + 1 - rank % 2 * 2, (rank + 2) % 4, 3 - rank


def block_at(kind, rank, i):
    own, pair, far, far_pair = ranks(rank)
    if kind == "near":
        e = jnp.where(i < 2, own, pair)
        return jnp.where(i % 2 == 0, e, 7 - e)
    e = jnp.where(i == 0, far, far_pair)
    return jnp.where(e % 2 == (1 if kind == "a" else 0), e, 7 - e)


def slot_at(kind, rank, i):
    if kind == "near":
        return (rank + i // 2) % 2 * 2 + i % 2
    return (rank + i) % 2


def attn_kernel(kind, heads, scale, steps, base, sc, wq_hbm, wo_hbm, *refs):
    x_hbm, dy_hbm, kv_hbm, refs = refs[:2], refs[2:4], refs[4:8], refs[8:]
    first, final = kind == "near", kind == "b"
    if first:
        o_ref, dq_ref, dkv_ref, xt_ref = refs[:4]
        scratch = refs[4:]
    else:
        init_hbm, o_ref, dq_ref, dkv_ref, xt_ref = refs[:5]
        scratch = refs[5:]
    ks, vs, kt, vt, dk, dv, qt, dot_t, qst, dost, s_ref, p_ref, ds_ref, ot, dqt, l_ref, ref, wq, wo, xs, dys, w_sem, x_sem, dy_sem, g_sem = scratch
    step = pl.program_id(0)
    hd = HD
    c2 = scale * math.log2(math.e)

    rank = sc[0]
    pos = [p for e in ranks(rank) for p in (e, 7 - e)]
    core = pl.multiple_of(rank % 2 * heads * hd, heads * hd)
    load_kv = []
    for n, p in enumerate(pos):
        src = kv_hbm[n // 2].at[n % 2 * BLK : (n % 2 + 1) * BLK, :]
        at = pl.ds(pl.multiple_of(p * BLK, BLK), BLK)
        for v, dst in enumerate((ks, vs)):
            col = pl.ds(pl.multiple_of((2 * v + rank % 2) * hd, hd), hd)
            load_kv.append(pltpu.make_async_copy(src.at[:, col], dst.at[at, :], g_sem.at[0]))

    def grads(hbm, out):
        pairs = [(hbm.at[:, :hd], dk), (hbm.at[:, hd:], dv)]
        return [pltpu.make_async_copy(*(p[::-1] if out else p), g_sem.at[1]) for p in pairs]

    load_wq, load_wo = [], []
    for n in range(4):
        span = slice(n * DUO, (n + 1) * DUO)
        load_wq.append(pltpu.make_async_copy(wq_hbm.at[span, pl.ds(core, heads * hd)], wq.at[span, :], w_sem.at[0]))
        rows = heads * hd // 4
        dst = wo.at[n * rows : (n + 1) * rows, :]
        load_wo.append(pltpu.make_async_copy(wo_hbm.at[pl.ds(core + n * rows, rows), :], dst, w_sem.at[1]))

    def load_rows(n):
        piece, row = divmod(n, steps // 2)
        src = pl.ds(row * BLK, BLK)
        return (
            pltpu.make_async_copy(x_hbm[piece].at[src, :], xs.at[n % 2], x_sem.at[n % 2]),
            pltpu.make_async_copy(dy_hbm[piece].at[pl.ds(base + row * BLK, BLK), :], dys.at[n % 2], dy_sem.at[n % 2]),
        )

    @pl.when(step == 0)
    def _():
        load_x, load_dy = load_rows(0)
        for cp in load_kv:
            cp.start()
        load_x.start()
        for cp in load_wq:
            cp.start()
        load_dy.start()
        for cp in load_wo:
            cp.start()
        for cp in [] if first else grads(init_hbm, False):
            cp.start()

    for n in range(1, steps):

        @pl.when(step == n - 1)
        def _():
            for cp in load_rows(n):
                cp.start()

    @pl.when(step == 0)
    def _():
        if first:
            dk[...] = jnp.zeros_like(dk)
            dv[...] = jnp.zeros_like(dv)
        for cp in load_kv:
            cp.wait()
        for i in range(8):
            at = slice(i * BLK, (i + 1) * BLK)
            kt[:, at] = ks[at, :].T
            vt[:, at] = vs[at, :].T

    @pl.when(step == 0)
    def _():
        for cp in load_wq:
            cp.wait()

    slot = step % 2
    pltpu.make_async_copy(x_hbm[0].at[0:BLK, :], xs.at[slot], x_sem.at[slot]).wait()
    q = dot(xs[slot], wq[...]).astype(BF16)
    xt_ref[...] = xs[slot].T
    for h in range(heads):
        qh = q[:, h * hd : (h + 1) * hd]
        qst[h * BLK : (h + 1) * BLK, :] = qh
        qt[:, h * BLK : (h + 1) * BLK] = qh.T

    @pl.when(step == 0)
    def _():
        for cp in load_wo:
            cp.wait()

    pltpu.make_async_copy(dy_hbm[0].at[0:BLK, :], dys.at[slot], dy_sem.at[slot]).wait()
    do = dot_nt(dys[slot], wo[...]).astype(BF16)
    for h in range(heads):
        dh = do[:, h * hd : (h + 1) * hd]
        dost[h * BLK : (h + 1) * BLK, :] = dh
        dot_t[:, h * BLK : (h + 1) * BLK] = dh.T

    b = block_at(kind, rank, step)

    def sweep(count, block):
        def pair(j, _):
            block(pl.multiple_of(j * 2 * BLK, 2 * BLK), 2 * BLK)
            return 0

        lax.fori_loop(0, count // 2, pair, 0)

        @pl.when(count % 2 == 1)
        def _():
            block(pl.multiple_of((count - 1) * BLK, BLK), BLK)

    def scores(start, rows, h):
        at = pl.ds(start, rows)
        return at, slice(h * BLK, (h + 1) * BLK), dot(ks[at, :], qt[:, h * BLK : (h + 1) * BLK]) * c2

    def rows_of(t):
        return t.reshape(t.shape[0] // 8, 8, BLK)

    key = lax.broadcasted_iota(jnp.int32, (BLK, BLK), 0)
    query = lax.broadcasted_iota(jnp.int32, (BLK, BLK), 1)
    for h in range(heads):
        at, span, t = scores(pl.multiple_of(b * BLK, BLK), BLK, h)
        t = jnp.where(key <= query, t, LOW)
        s_ref[at, span] = t
        base = jnp.max(t, axis=0, keepdims=True)
        ref[:, span] = base
        l_ref[:, span] = jnp.sum(jnp.exp2(rows_of(t - base)), axis=0)

    def open_block(start, rows):
        for h in range(heads):
            at, span, t = scores(start, rows, h)
            s_ref[at, span] = t
            l_ref[:, span] += jnp.sum(jnp.exp2(rows_of(t - ref[:, span])), axis=0)

    sweep(b, open_block)

    @pl.when(jnp.max(l_ref[...]) > LARGE)
    def _():
        def each(start, fn):
            for h in range(heads):
                span = slice(h * BLK, (h + 1) * BLK)
                fn(span, s_ref[pl.ds(start, BLK), span])

        def peak(span, t):
            ref[:, span] = jnp.maximum(ref[:, span], jnp.max(t, axis=0, keepdims=True))

        def total(span, t):
            l_ref[:, span] += jnp.sum(jnp.exp2(rows_of(t - ref[:, span])), axis=0)

        def over(fn):
            def body(j, _):
                each(pl.multiple_of(j * BLK, BLK), fn)
                return 0

            lax.fori_loop(0, b + 1, body, 0)

        over(peak)
        l_ref[...] = jnp.zeros_like(l_ref)
        over(total)

    lse = ref[...] + jnp.log2(jnp.sum(l_ref[...], axis=0, keepdims=True))

    ot[...] = jnp.zeros_like(ot)

    def value_block(start, rows):
        at = pl.ds(start, rows)
        for h in range(heads):
            span = slice(h * BLK, (h + 1) * BLK)
            p = jnp.exp2(s_ref[at, span] - lse[:, span]).astype(BF16)
            p_ref[at, span] = p
            ot[:, span] += dot(vt[:, at], p)

    sweep(b + 1, value_block)

    o_round = ot[...].astype(BF16)
    delta = jnp.sum(o_round.astype(F32) * dot_t[...].astype(F32), axis=0, keepdims=True)
    for h in range(heads):
        o_ref[h * hd : (h + 1) * hd, :] = o_round[:, h * BLK : (h + 1) * BLK]
    dqt[...] = jnp.zeros_like(dqt)

    def grad_block(j, _):
        at = pl.ds(pl.multiple_of(j * BLK, BLK), BLK)
        dp = dot(vs[at, :], dot_t[...])
        dv[at, :] += dot(p_ref[at, :], dost[...])
        ds = (p_ref[at, :].astype(F32) * (dp - delta)).astype(BF16)
        ds_ref[...] = ds
        dqt[...] += dot(kt[:, at], ds_ref[...])
        dk[at, :] += dot(ds_ref[...], qst[...])
        return 0

    if not first:

        @pl.when(step == 0)
        def _():
            for cp in grads(init_hbm, False):
                cp.wait()

    lax.fori_loop(0, b + 1, grad_block, 0)

    for h in range(heads):
        dq_ref[:, h * hd : (h + 1) * hd] = (dqt[:, h * BLK : (h + 1) * BLK] * scale).astype(BF16).T

    @pl.when(step == steps - 1)
    def _():
        if not final:
            for cp in grads(dkv_ref, True):
                cp.start()
            for cp in grads(dkv_ref, True):
                cp.wait()
        else:
            for n, (p, e) in enumerate(zip(pos, [e for e in ranks(rank) for _ in "ab"])):
                at = pl.ds(pl.multiple_of(p * BLK, BLK), BLK)
                if n < 4:
                    row = e % 2 * 2 + n % 2
                else:
                    row = jnp.where((e + n) % 2 == 1, 4, 6) + e % 2
                out = pl.ds(pl.multiple_of(row * BLK, BLK), BLK)
                dkv_ref[out, :hd] = (dk[at, :] * scale).astype(BF16)
                dkv_ref[out, hd:] = dv[at, :].astype(BF16)


def attention(kind, rank, wq, wo, x_pieces, dy_pieces, base, kv_pieces, init, scale):
    final = kind == "b"
    rows, width, model = 2 * (x_pieces[0].shape[0] - base), wq.shape[1] // 2, wq.shape[0]
    hd = HD
    heads = width // hd
    wide = heads * BLK
    seq = SEQ
    slot = functools.partial(slot_at, kind)
    o_spec = pl.BlockSpec((width, BLK), lambda i, s: (0, slot(s[0], i)))
    out_spec = pl.BlockSpec((BLK, width), lambda i, s: (slot(s[0], i), 0))
    xt_spec = pl.BlockSpec((model, BLK), lambda i, s: (0, slot(s[0], i)))
    dkv_spec = pl.BlockSpec((seq, BLK), lambda i, s: (0, 0)) if final else pl.BlockSpec(memory_space=pl.ANY)
    ins = [wq, wo, *x_pieces, *dy_pieces, *kv_pieces] + ([] if init is None else [init])
    return pl.pallas_call(
        functools.partial(attn_kernel, kind, heads, scale, rows // BLK, base),
        out_shape=(
            jax.ShapeDtypeStruct((width, rows), BF16),
            jax.ShapeDtypeStruct((rows, width), BF16),
            jax.ShapeDtypeStruct((seq, BLK), BF16 if final else F32),
            jax.ShapeDtypeStruct((model, rows), BF16),
        ),
        grid_spec=pltpu.PrefetchScalarGridSpec(
            num_scalar_prefetch=1,
            grid=(rows // BLK,),
            in_specs=[pl.BlockSpec(memory_space=pl.ANY) for _ in ins],
            out_specs=(o_spec, out_spec, dkv_spec, xt_spec),
            scratch_shapes=[
                *[pltpu.VMEM((seq, hd), BF16) for _ in "kv"],
                *[pltpu.VMEM((hd, seq), BF16) for _ in "kv"],
                *[pltpu.VMEM((seq, hd), F32) for _ in "kv"],
                *[pltpu.VMEM((hd, wide), BF16) for _ in "qd"],
                *[pltpu.VMEM((wide, hd), BF16) for _ in "qd"],
                pltpu.VMEM((seq, wide), F32),
                pltpu.VMEM((seq, wide), BF16),
                pltpu.VMEM((BLK, wide), BF16),
                *[pltpu.VMEM((hd, wide), F32) for _ in "od"],
                pltpu.VMEM((8, wide), F32),
                pltpu.VMEM((1, wide), F32),
                pltpu.VMEM((model, width), BF16),
                pltpu.VMEM((width, model), BF16),
                *[pltpu.VMEM((2, BLK, model), BF16) for _ in "xd"],
                *[pltpu.SemaphoreType.DMA((2,)) for _ in "wxdg"],
            ],
        ),
        compiler_params=params(1, 63),
        cost_estimate=cost(8e9 * (rows // BLK), 20e6),
    )(rank, *ins)


def y_kernel(sc, o_mine, o_other, w_mine, w_other, out_ref, os):
    half = o_mine.shape[0]

    @pl.when(pl.program_id(0) == 0)
    def _():
        os[:, :half] = o_mine[...].T
        os[:, half:] = o_other[...].T

    out_ref[...] = (dot(os[:, :half], w_mine[...]) + dot(os[:, half:], w_other[...])).astype(BF16)


def out_rows(core, o_mine, o_other, wo):
    rows, half, model, tile = DUO, o_mine.shape[0], wo.shape[1], DUO
    return pl.pallas_call(
        y_kernel,
        out_shape=jax.ShapeDtypeStruct((rows, model), BF16),
        grid_spec=pltpu.PrefetchScalarGridSpec(
            num_scalar_prefetch=1,
            grid=(model // tile,),
            in_specs=[
                pl.BlockSpec((half, rows), lambda i, s: (0, s[0])),
                pl.BlockSpec((half, rows), lambda i, s: (0, s[0])),
                pl.BlockSpec((half, tile), lambda i, s: (s[0], i)),
                pl.BlockSpec((half, tile), lambda i, s: (1 - s[0], i)),
            ],
            out_specs=pl.BlockSpec((rows, tile), lambda i, s: (0, i)),
            scratch_shapes=[pltpu.VMEM((rows, 2 * half), BF16)],
        ),
        compiler_params=params(),
        cost_estimate=cost(4 * rows * half * model, 12e6),
    )(core, o_mine, o_other, wo, wo)


def dx_kernel(sc, q_mine, q_other, kv_mine, kv_other, wq_mine, wq_other, wkv, out_ref, kv):
    hd = HD

    @pl.when(pl.program_id(0) == 0)
    def _():
        for n, src in ((sc[0], kv_mine), (1 - sc[0], kv_other)):
            kv[:, pl.ds(pl.multiple_of(n * hd, hd), hd)] = src[:, :hd]
            kv[:, pl.ds(pl.multiple_of((2 + n) * hd, hd), hd)] = src[:, hd:]

    acc = dot_nt(q_mine[...], wq_mine[...]) + dot_nt(q_other[...], wq_other[...])
    out_ref[...] = (acc + dot_nt(kv[...], wkv[...])).astype(BF16)


def grad_rows(core, dq_mine, dq_other, dkv_mine, dkv_other, wq, wkv):
    rows, half, model, tile = DUO, dq_mine.shape[1], wq.shape[0], DUO
    mine = lambda i, s: (s[0], 0)
    near, far = lambda i, s: (i, s[0]), lambda i, s: (i, 1 - s[0])
    return pl.pallas_call(
        dx_kernel,
        out_shape=jax.ShapeDtypeStruct((rows, model), BF16),
        grid_spec=pltpu.PrefetchScalarGridSpec(
            num_scalar_prefetch=1,
            grid=(model // tile,),
            in_specs=[
                *[pl.BlockSpec((rows, n), mine) for n in (half, half, BLK, BLK)],
                *[pl.BlockSpec((tile, half), at) for at in (near, far)],
                pl.BlockSpec((tile, DUO), lambda i, s: (i, 0)),
            ],
            out_specs=pl.BlockSpec((rows, tile), lambda i, s: (0, i)),
            scratch_shapes=[pltpu.VMEM((rows, DUO), BF16)],
        ),
        compiler_params=params(),
        cost_estimate=cost(4 * rows * half * model * 1.25, 14e6),
    )(core, dq_mine, dq_other, dkv_mine, dkv_other, wq, wq, wkv)


PIECES = ((0, DUO), (1, DUO), (0, BLK), (1, BLK), (0, BLK), (1, BLK))
STARTS = (0, DUO, HALF, 1280, 1536, 1792)


def piece_copies(core, arrays, dst, sem, along):
    copies = []
    for n, ((flip, size), start) in enumerate(zip(PIECES, STARTS)):
        at = pl.ds(pl.multiple_of((1 - core if flip else core) * size, size), size)
        src = arrays[n // 2]
        if along:
            copies.append(pltpu.make_async_copy(src.at[:, at], dst.at[:, start : start + size], sem))
        else:
            copies.append(pltpu.make_async_copy(src.at[at, :], dst.at[start : start + size, :], sem))
    return copies


def dwq_kernel(sc, *refs):
    xts, mine, other, kv_in = refs[:3], refs[3:6], refs[6:9], refs[9:11]
    out_ref, gk_ref, gv_ref, dq, kv, sems = refs[11:]
    g, i = pl.program_id(0), pl.program_id(1)
    tile, core, hd = out_ref.shape[0], sc[0], HD
    spans = [slice(0, HALF), slice(HALF, HALF + DUO), slice(HALF + DUO, SEQ)]
    first = [pltpu.make_async_copy(a, dq.at[0, at, :], sems.at[0]) for a, at in zip(mine, spans)]
    later = [pltpu.make_async_copy(a, dq.at[1, at, :], sems.at[1]) for a, at in zip(other, spans)]
    later += [
        pltpu.make_async_copy(a, kv.at[:, n * BLK : (n + 1) * BLK], sems.at[1]) for n, a in enumerate(kv_in)
    ]

    def when(gg, ii, copies, start):
        @pl.when((g == gg) & (i == ii))
        def _():
            for cp in copies:
                cp.start() if start else cp.wait()

    when(0, 0, first, True)
    when(0, 1, later, True)
    when(0, 0, first, False)
    when(1, 0, later, False)

    acc = sum(dot(x[...], dq[g, at, :]) for x, at in zip(xts, spans))
    flat = out_ref.reshape(tile * 8, hd)
    for h in range(8):
        flat[pl.ds(h, tile, stride=8), :] = acc[:, h * hd : (h + 1) * hd]

    @pl.when(g == 1)
    def _():
        k_flat, v_flat = gk_ref.reshape(tile * 2, hd), gv_ref.reshape(tile * 2, hd)
        both = sum(dot(x[...], kv[at, :]) for x, at in zip(xts, spans))
        for n, head in enumerate((core, 1 - core)):
            k_flat[pl.ds(head, tile, stride=2), :] = both[:, 2 * n * hd : (2 * n + 1) * hd]
            v_flat[pl.ds(head, tile, stride=2), :] = both[:, (2 * n + 1) * hd : (2 * n + 2) * hd]


def grad_wq(core, xts, mine, other, kvm, kvo):
    model, half, tile = xts[0].shape[0], mine[0].shape[1], TILE_WQ
    tiles = model // tile
    small = pl.BlockSpec((tile, 2, HD), lambda g, i, s: (i * g, 0, 0))
    return pl.pallas_call(
        dwq_kernel,
        out_shape=(
            jax.ShapeDtypeStruct((model, 16, HD), F32),
            jax.ShapeDtypeStruct((model, 2, HD), F32),
            jax.ShapeDtypeStruct((model, 2, HD), F32),
        ),
        grid_spec=pltpu.PrefetchScalarGridSpec(
            num_scalar_prefetch=1,
            grid=(2, tiles),
            in_specs=[pl.BlockSpec((tile, x.shape[1]), lambda g, i, s: (i, 0)) for x in xts]
            + [pl.BlockSpec(memory_space=pl.ANY)] * 8,
            out_specs=(
                pl.BlockSpec((tile, 8, HD), lambda g, i, s: (i, (s[0] + g) % 2, 0)),
                small,
                small,
            ),
            scratch_shapes=[
                pltpu.VMEM((2, SEQ, half), BF16),
                pltpu.VMEM((SEQ, DUO), BF16),
                pltpu.SemaphoreType.DMA((2,)),
            ],
        ),
        compiler_params=params(2),
        cost_estimate=cost(2 * SEQ * model * (2 * half + DUO), 40e6),
    )(core, *xts, *mine, *other, kvm, kvo)


def dwo_kernel(sc, *refs):
    mine, other, ys, (out_ref, o_all, y_all, sems) = refs[:3], refs[3:6], refs[6:12], refs[12:]
    j, g, i = pl.program_id(0), pl.program_id(1), pl.program_id(2)
    tile, wide = out_ref.shape
    o_first = piece_copies(sc[0], mine, o_all.at[0], sems.at[0], True)
    o_later = piece_copies(sc[0], other, o_all.at[1], sems.at[1], True)
    y_copies = [
        [
            pltpu.make_async_copy(
                y.at[y.shape[0] - r if r == BLK else 0 :, n * wide : (n + 1) * wide], y_all.at[n, s : s + r, :], sems.at[2 + n]
            )
            for y, s, (_, r) in zip(ys, STARTS, PIECES)
        ]
        for n in range(2)
    ]

    def when(jj, gg, ii, copies, start):
        @pl.when((j == jj) & (g == gg) & (i == ii))
        def _():
            for cp in copies:
                cp.start() if start else cp.wait()

    when(0, 0, 0, y_copies[0] + o_first, True)
    when(0, 0, 1, o_later, True)
    when(0, 1, 0, y_copies[1], True)
    when(0, 0, 0, y_copies[0] + o_first, False)
    when(0, 1, 0, o_later, False)
    when(1, 0, 0, y_copies[1], False)
    out_ref[...] = dot(o_all[g, pl.ds(pl.multiple_of(i * tile, tile), tile), :], y_all[j])


def grad_wo(core, ys, mine, other):
    model, half, tile, wide = ys[0].shape[1], mine[0].shape[0], DUO, HALF
    steps = half // tile
    return pl.pallas_call(
        dwo_kernel,
        out_shape=jax.ShapeDtypeStruct((2 * half, model), F32),
        grid_spec=pltpu.PrefetchScalarGridSpec(
            num_scalar_prefetch=1,
            grid=(2, 2, steps),
            in_specs=[pl.BlockSpec(memory_space=pl.ANY)] * 12,
            out_specs=pl.BlockSpec((tile, wide), lambda j, g, i, s: ((s[0] + g) % 2 * steps + i, j)),
            scratch_shapes=[
                pltpu.VMEM((2, half, SEQ), BF16),
                pltpu.VMEM((2, SEQ, wide), BF16),
                pltpu.SemaphoreType.DMA((4,)),
            ],
        ),
        compiler_params=params(3),
        cost_estimate=cost(4 * SEQ * model * half, 40e6),
    )(core, *mine, *other, *ys)


def solution(mesh):
    row_spec = P(("dp", "cp"), None)
    rep_spec = P(None, None, None)
    part_spec = P("dp", None, None)
    core_swap = [(0, 1), (1, 0), (2, 3), (3, 2)]
    chip_swap = [(0, 2), (2, 0), (1, 3), (3, 1)]

    def device_layer(x, dy, w_query, w_key, w_value, w_out):
        _, model = x.shape
        num_heads, hd = w_query.shape[1:]
        kv_heads = w_key.shape[1]
        scale = hd ** -0.5
        rank = lax.axis_index("cp").astype(jnp.int32)
        c = rank & 1
        core = c.reshape(1)
        rank = rank.reshape(1)

        to_core = lambda v: lax.ppermute(v, "cp", core_swap)
        to_chip = lambda v: lax.ppermute(v, "cp", chip_swap)

        wk = w_key.reshape(model * kv_heads, hd)
        wv = w_value.reshape(model * kv_heads, hd)
        wo = w_out.reshape(num_heads * hd, model)
        x_p = to_core(x)
        dy_p = to_core(dy)

        kv, wkv, r_a, r_b = project_kv(core, x, dy, wk, wv)
        far_kv, kv_p = to_chip(kv), to_core(kv)
        w_s, _ = lax.optimization_barrier((w_query, kv))
        r_a, r_b = to_chip(r_a), to_chip(r_b)
        wq = flat_heads(w_s)
        kv_r, wq = lax.optimization_barrier((far_kv, wq))
        kv_rp = to_core(kv_r)
        pieces = (kv, kv_p, kv_r, kv_rp)

        o_c, dq_c, part, xt_c = attention(
            "near", rank, wq, wo, (x, x_p), (dy, dy_p), 0, pieces, None, scale)
        r_a, o_c, dq_c = lax.optimization_barrier((r_a, o_c, dq_c))
        r_pa, o_co, dq_co = to_core(r_a), to_core(o_c), to_core(dq_c)

        o_a, dq_a, part, xt_a = attention("a", rank, wq, wo, (r_a, r_pa), (r_a, r_pa), BLK, pieces, part, scale)
        r_b, o_a, dq_a = lax.optimization_barrier((r_b, o_a, dq_a))
        r_pb, o_ao, dq_ao = to_core(r_b), to_core(o_a), to_core(dq_a)

        o_b, dq_b, dkv, xt_b = attention("b", rank, wq, wo, (r_b, r_pb), (r_b, r_pb), BLK, pieces, part, scale)
        o_co, dkv = lax.optimization_barrier((o_co, dkv))
        dkv_o, o_bo, dq_bo = to_core(dkv), to_core(o_b), to_core(dq_b)
        y = out_rows(core, o_c, o_co, wo)

        ys = (dy, dy_p, r_a, r_pa, r_b, r_pb)
        gwo = grad_wo(core, ys, (o_c, o_a, o_b), (o_co, o_ao, o_bo))
        dx = grad_rows(core, dq_c, dq_co, dkv, dkv_o, wq, wkv)
        gwq, gwk, gwv = grad_wq(core, (xt_c, xt_a, xt_b), (dq_c, dq_a, dq_b), (dq_co, dq_ao, dq_bo), dkv, dkv_o)
        return y, dx, gwq, gwk, gwv, gwo.reshape(num_heads, hd, model)

    return jax.shard_map(
        device_layer,
        mesh=mesh,
        in_specs=(row_spec, row_spec, rep_spec, rep_spec, rep_spec, rep_spec),
        out_specs=(row_spec, row_spec, part_spec, part_spec, part_spec, part_spec),
        check_vma=False,
    )
```

```python
import functools
import math

import jax
import jax.numpy as jnp
import numpy as np
from jax import lax
from jax.experimental import pallas as pl
from jax.experimental.pallas import tpu as pltpu
from jax.sharding import PartitionSpec as P


BLK = 256
HD = 128
DUO = 512
HALF = 1024
SEQ = 2048
WO_STEPS = 8
DX_STEP = 16
LARGE = 2.0**60
LOW = -3.0e38
F32 = jnp.float32
BF16 = jnp.bfloat16


def dot(a, b):
    return jnp.dot(a, b, preferred_element_type=F32)


def dot_nt(a, b):
    return lax.dot_general(a, b, (((1,), (1,)), ((), ())), preferred_element_type=F32)


def params(n=1, mib=60):
    return pltpu.CompilerParams(
        dimension_semantics=("arbitrary",) * n, vmem_limit_bytes=mib * HALF * HALF
    )


def cost(flops, nbytes):
    return pl.CostEstimate(flops=int(flops), bytes_accessed=int(nbytes), transcendentals=0)


def heads_kernel(perm_ref, w_hbm, out_hbm, w_in, w_out, in_sem, out_sem):
    chunks, rows, num, hd = w_in.shape
    group = perm_ref.shape[0]
    loads = [
        pltpu.make_async_copy(w_hbm.at[c * rows : (c + 1) * rows], w_in.at[c], in_sem.at[c]) for c in range(chunks)
    ]
    stores = [
        pltpu.make_async_copy(w_out.at[c], out_hbm.at[c * rows : (c + 1) * rows, :], out_sem.at[c]) for c in range(chunks)
    ]
    for cp in loads:
        cp.start()

    def chunk(c, _):
        pltpu.make_async_copy(w_hbm.at[:rows], w_in.at[c], in_sem.at[c]).wait()
        flat = w_in.at[c].reshape(rows * num, hd)
        for g in range(0, rows // 16, 2):
            pair = [flat[(g + n) * group : (g + n + 1) * group, :] for n in range(2)]
            res = dot(perm_ref[...], jnp.concatenate(pair, axis=1)).astype(BF16)
            for n in range(2):
                for h in range(num):
                    w_out[c, (g + n) * 16 : (g + n + 1) * 16, h * hd : (h + 1) * hd] = res[
                        h * 16 : (h + 1) * 16, n * hd : (n + 1) * hd
                    ]
        at = pl.ds(pl.multiple_of(c * rows, rows), rows)
        pltpu.make_async_copy(w_out.at[c], out_hbm.at[at, :], out_sem.at[c]).start()
        return 0

    lax.fori_loop(0, chunks, chunk, 0)
    for cp in stores:
        cp.wait()


def gather_heads(num, rows):
    row = np.arange(num * rows)
    return jnp.asarray((row % rows * num + row // rows)[:, None] == row[None, :], BF16)


def flat_heads(w):
    model, num, hd = w.shape
    chunks = 8
    rows = model // chunks
    return pl.pallas_call(
        heads_kernel,
        out_shape=jax.ShapeDtypeStruct((model, num * hd), BF16),
        in_specs=[pl.BlockSpec(memory_space=pltpu.VMEM), pl.BlockSpec(memory_space=pl.ANY)],
        out_specs=pl.BlockSpec(memory_space=pl.ANY),
        scratch_shapes=[
            pltpu.VMEM((chunks, rows, num, hd), BF16),
            pltpu.VMEM((chunks, rows, num * hd), BF16),
            pltpu.SemaphoreType.DMA((chunks,)),
            pltpu.SemaphoreType.DMA((chunks,)),
        ],
        compiler_params=pltpu.CompilerParams(vmem_limit_bytes=params(1).vmem_limit_bytes),
        cost_estimate=cost(4e9, 4 * model * num * hd),
    )(gather_heads(num, 16), w)


def kv_kernel(sc, x_ref, dy_ref, wk_ref, wv_ref, perm_ref, out_ref, w_hbm, rows_a, rows_b, w_ref, sems):
    step, core = pl.program_id(0), sc[0]
    save_w = pltpu.make_async_copy(w_ref, w_hbm, sems.at[2])

    def cut(dst, n):
        return [
            pltpu.make_async_copy(src, dst.at[at : at + BLK, :], sems.at[n])
            for src, at in ((x_ref, 0), (dy_ref, BLK))
        ]

    for n, dst in enumerate((rows_a, rows_b)):

        @pl.when(step == (1 - core if n == 0 else core))
        def _():
            for cp in cut(dst, n):
                cp.start()

    @pl.when(pl.program_id(0) == 0)
    def _():
        for g in range(w_ref.shape[0] // HD):
            rows = slice(g * BLK, (g + 1) * BLK)
            pair = jnp.concatenate([wk_ref[rows, :], wv_ref[rows, :]], axis=1)
            res = dot(perm_ref[...], pair).astype(BF16)
            for h in range(2):
                for v in range(2):
                    col = (v * 2 + h) * HD
                    w_ref[g * HD : (g + 1) * HD, col : col + HD] = res[h * HD : (h + 1) * HD, v * HD : (v + 1) * HD]

        save_w.start()

    out_ref[...] = dot(x_ref[...], w_ref[...]).astype(BF16)

    @pl.when(step == 1)
    def _():
        save_w.wait()
        for n, dst in enumerate((rows_a, rows_b)):
            for cp in cut(dst, n):
                cp.wait()


def project_kv(core, x, dy, wk, wv):
    rows, depth = x.shape
    row = pl.BlockSpec((BLK, depth), lambda i, s: (i, 0))
    fixed = lambda shape: pl.BlockSpec(shape, lambda i, s: (0, 0))
    chunk = jax.ShapeDtypeStruct((rows, depth), BF16)
    return pl.pallas_call(
        kv_kernel,
        out_shape=(jax.ShapeDtypeStruct((rows, DUO), BF16), jax.ShapeDtypeStruct((depth, DUO), BF16), chunk, chunk),
        grid_spec=pltpu.PrefetchScalarGridSpec(
            num_scalar_prefetch=1,
            grid=(rows // BLK,),
            in_specs=[row, row, fixed(wk.shape), fixed(wv.shape), fixed((BLK, BLK))],
            out_specs=(pl.BlockSpec((BLK, DUO), lambda i, s: (i, 0)),) + (pl.BlockSpec(memory_space=pl.ANY),) * 3,
            scratch_shapes=[pltpu.VMEM((depth, DUO), BF16), pltpu.SemaphoreType.DMA((3,))],
        ),
        compiler_params=params(),
        cost_estimate=cost(2 * rows * depth * DUO, 8e6),
    )(core, x, dy, wk, wv, gather_heads(2, HD))


def ranks(rank):
    return rank, rank + 1 - rank % 2 * 2, (rank + 2) % 4, 3 - rank


def block_at(kind, rank, i):
    own, pair, far, far_pair = ranks(rank)
    if kind == "near":
        e = jnp.where(i < 2, own, pair)
        return jnp.where(i % 2 == 0, e, 7 - e)
    e = jnp.where(i == 0, far, far_pair)
    return jnp.where(e % 2 == (1 if kind == "a" else 0), e, 7 - e)


def slot_at(kind, rank, i):
    if kind == "near":
        return (rank + i // 2) % 2 * 2 + i % 2
    return (rank + i) % 2


def attn_kernel(kind, heads, scale, steps, base, sc, wq_hbm, wo_hbm, *refs):
    x_hbm, dy_hbm, kv_hbm, refs = refs[:2], refs[2:4], refs[4:8], refs[8:]
    first, final = kind == "near", kind == "b"
    if first:
        o_ref, dq_ref, dkv_ref, xt_ref = refs[:4]
        scratch = refs[4:]
    else:
        init_hbm, o_ref, dq_ref, dkv_ref, xt_ref = refs[:5]
        scratch = refs[5:]
    ks, vs, kt, vt, dk, dv, qt, dot_t, qst, dost, s_ref, p_ref, ds_ref, ot, dqt, l_ref, ref, wq, wo, xs, dys, w_sem, x_sem, dy_sem, g_sem = scratch
    step = pl.program_id(0)
    hd = HD
    c2 = scale * math.log2(math.e)

    rank = sc[0]
    pos = [p for e in ranks(rank) for p in (e, 7 - e)]
    core = pl.multiple_of(rank % 2 * heads * hd, heads * hd)
    load_kv = []
    for n, p in enumerate(pos):
        src = kv_hbm[n // 2].at[n % 2 * BLK : (n % 2 + 1) * BLK, :]
        at = pl.ds(pl.multiple_of(p * BLK, BLK), BLK)
        for v, dst in enumerate((ks, vs)):
            col = pl.ds(pl.multiple_of((2 * v + rank % 2) * hd, hd), hd)
            load_kv.append(pltpu.make_async_copy(src.at[:, col], dst.at[at, :], g_sem.at[0]))

    def grads(hbm, out):
        pairs = [(hbm.at[:, :hd], dk), (hbm.at[:, hd:], dv)]
        return [pltpu.make_async_copy(*(p[::-1] if out else p), g_sem.at[1]) for p in pairs]

    load_wq, load_wo = [], []
    for n in range(4):
        span = slice(n * DUO, (n + 1) * DUO)
        load_wq.append(pltpu.make_async_copy(wq_hbm.at[span, pl.ds(core, heads * hd)], wq.at[span, :], w_sem.at[0]))
        rows = heads * hd // 4
        dst = wo.at[n * rows : (n + 1) * rows, :]
        load_wo.append(pltpu.make_async_copy(wo_hbm.at[pl.ds(core + n * rows, rows), :], dst, w_sem.at[1]))

    def load_rows(n):
        piece, row = divmod(n, steps // 2)
        src = pl.ds(row * BLK, BLK)
        return (
            pltpu.make_async_copy(x_hbm[piece].at[src, :], xs.at[n % 2], x_sem.at[n % 2]),
            pltpu.make_async_copy(dy_hbm[piece].at[pl.ds(base + row * BLK, BLK), :], dys.at[n % 2], dy_sem.at[n % 2]),
        )

    @pl.when(step == 0)
    def _():
        load_x, load_dy = load_rows(0)
        for cp in load_kv:
            cp.start()
        load_x.start()
        for cp in load_wq:
            cp.start()
        load_dy.start()
        for cp in load_wo:
            cp.start()
        for cp in [] if first else grads(init_hbm, False):
            cp.start()

    for n in range(1, steps):

        @pl.when(step == n - 1)
        def _():
            for cp in load_rows(n):
                cp.start()

    @pl.when(step == 0)
    def _():
        if first:
            dk[...] = jnp.zeros_like(dk)
            dv[...] = jnp.zeros_like(dv)
        for cp in load_kv:
            cp.wait()
        for i in range(8):
            at = slice(i * BLK, (i + 1) * BLK)
            kt[:, at] = ks[at, :].T
            vt[:, at] = vs[at, :].T

    @pl.when(step == 0)
    def _():
        for cp in load_wq:
            cp.wait()

    slot = step % 2
    pltpu.make_async_copy(x_hbm[0].at[0:BLK, :], xs.at[slot], x_sem.at[slot]).wait()
    q = dot(xs[slot], wq[...]).astype(BF16)
    xt_ref[...] = xs[slot].T
    for h in range(heads):
        qh = q[:, h * hd : (h + 1) * hd]
        qst[h * BLK : (h + 1) * BLK, :] = qh
        qt[:, h * BLK : (h + 1) * BLK] = qh.T

    @pl.when(step == 0)
    def _():
        for cp in load_wo:
            cp.wait()

    pltpu.make_async_copy(dy_hbm[0].at[0:BLK, :], dys.at[slot], dy_sem.at[slot]).wait()
    do = dot_nt(dys[slot], wo[...]).astype(BF16)
    for h in range(heads):
        dh = do[:, h * hd : (h + 1) * hd]
        dost[h * BLK : (h + 1) * BLK, :] = dh
        dot_t[:, h * BLK : (h + 1) * BLK] = dh.T

    b = block_at(kind, rank, step)

    def sweep(count, block):
        def pair(j, _):
            block(pl.multiple_of(j * 2 * BLK, 2 * BLK), 2 * BLK)
            return 0

        lax.fori_loop(0, count // 2, pair, 0)

        @pl.when(count % 2 == 1)
        def _():
            block(pl.multiple_of((count - 1) * BLK, BLK), BLK)

    def scores(start, rows, h):
        at = pl.ds(start, rows)
        return at, slice(h * BLK, (h + 1) * BLK), dot(ks[at, :], qt[:, h * BLK : (h + 1) * BLK]) * c2

    def rows_of(t):
        return t.reshape(t.shape[0] // 8, 8, BLK)

    key = lax.broadcasted_iota(jnp.int32, (BLK, BLK), 0)
    query = lax.broadcasted_iota(jnp.int32, (BLK, BLK), 1)
    for h in range(heads):
        at, span, t = scores(pl.multiple_of(b * BLK, BLK), BLK, h)
        t = jnp.where(key <= query, t, LOW)
        s_ref[at, span] = t
        base = jnp.max(t, axis=0, keepdims=True)
        ref[:, span] = base
        l_ref[:, span] = jnp.sum(jnp.exp2(rows_of(t - base)), axis=0)

    def open_block(start, rows):
        for h in range(heads):
            at, span, t = scores(start, rows, h)
            s_ref[at, span] = t
            l_ref[:, span] += jnp.sum(jnp.exp2(rows_of(t - ref[:, span])), axis=0)

    sweep(b, open_block)

    @pl.when(jnp.max(l_ref[...]) > LARGE)
    def _():
        def each(start, fn):
            for h in range(heads):
                span = slice(h * BLK, (h + 1) * BLK)
                fn(span, s_ref[pl.ds(start, BLK), span])

        def peak(span, t):
            ref[:, span] = jnp.maximum(ref[:, span], jnp.max(t, axis=0, keepdims=True))

        def total(span, t):
            l_ref[:, span] += jnp.sum(jnp.exp2(rows_of(t - ref[:, span])), axis=0)

        def over(fn):
            def body(j, _):
                each(pl.multiple_of(j * BLK, BLK), fn)
                return 0

            lax.fori_loop(0, b + 1, body, 0)

        over(peak)
        l_ref[...] = jnp.zeros_like(l_ref)
        over(total)

    lse = ref[...] + jnp.log2(jnp.sum(l_ref[...], axis=0, keepdims=True))

    ot[...] = jnp.zeros_like(ot)

    def value_block(start, rows):
        at = pl.ds(start, rows)
        for h in range(heads):
            span = slice(h * BLK, (h + 1) * BLK)
            p = jnp.exp2(s_ref[at, span] - lse[:, span]).astype(BF16)
            p_ref[at, span] = p
            ot[:, span] += dot(vt[:, at], p)

    sweep(b + 1, value_block)

    o_round = ot[...].astype(BF16)
    delta = jnp.sum(o_round.astype(F32) * dot_t[...].astype(F32), axis=0, keepdims=True)
    for h in range(heads):
        o_ref[h * hd : (h + 1) * hd, :] = o_round[:, h * BLK : (h + 1) * BLK]
    dqt[...] = jnp.zeros_like(dqt)

    def grad_block(j, _):
        at = pl.ds(pl.multiple_of(j * BLK, BLK), BLK)
        dp = dot(vs[at, :], dot_t[...])
        dv[at, :] += dot(p_ref[at, :], dost[...])
        ds = (p_ref[at, :].astype(F32) * (dp - delta)).astype(BF16)
        ds_ref[...] = ds
        dqt[...] += dot(kt[:, at], ds_ref[...])
        dk[at, :] += dot(ds_ref[...], qst[...])
        return 0

    if not first:

        @pl.when(step == 0)
        def _():
            for cp in grads(init_hbm, False):
                cp.wait()

    lax.fori_loop(0, b + 1, grad_block, 0)

    for h in range(heads):
        dq_ref[:, h * hd : (h + 1) * hd] = (dqt[:, h * BLK : (h + 1) * BLK] * scale).astype(BF16).T

    @pl.when(step == steps - 1)
    def _():
        if not final:
            for cp in grads(dkv_ref, True):
                cp.start()
            for cp in grads(dkv_ref, True):
                cp.wait()
        else:
            for n, (p, e) in enumerate(zip(pos, [e for e in ranks(rank) for _ in "ab"])):
                at = pl.ds(pl.multiple_of(p * BLK, BLK), BLK)
                if n < 4:
                    row = e % 2 * 2 + n % 2
                else:
                    row = jnp.where((e + n) % 2 == 1, 4, 6) + e % 2
                out = pl.ds(pl.multiple_of(row * BLK, BLK), BLK)
                dkv_ref[out, :hd] = (dk[at, :] * scale).astype(BF16)
                dkv_ref[out, hd:] = dv[at, :].astype(BF16)


def attention(kind, rank, wq, wo, x_pieces, dy_pieces, base, kv_pieces, init, scale):
    final = kind == "b"
    rows, width, model = 2 * (x_pieces[0].shape[0] - base), wq.shape[1] // 2, wq.shape[0]
    hd = HD
    heads = width // hd
    wide = heads * BLK
    seq = SEQ
    slot = functools.partial(slot_at, kind)
    o_spec = pl.BlockSpec((width, BLK), lambda i, s: (0, slot(s[0], i)))
    out_spec = pl.BlockSpec((BLK, width), lambda i, s: (slot(s[0], i), 0))
    xt_spec = pl.BlockSpec((model, BLK), lambda i, s: (0, slot(s[0], i)))
    dkv_spec = pl.BlockSpec((seq, BLK), lambda i, s: (0, 0)) if final else pl.BlockSpec(memory_space=pl.ANY)
    ins = [wq, wo, *x_pieces, *dy_pieces, *kv_pieces] + ([] if init is None else [init])
    return pl.pallas_call(
        functools.partial(attn_kernel, kind, heads, scale, rows // BLK, base),
        out_shape=(
            jax.ShapeDtypeStruct((width, rows), BF16),
            jax.ShapeDtypeStruct((rows, width), BF16),
            jax.ShapeDtypeStruct((seq, BLK), BF16 if final else F32),
            jax.ShapeDtypeStruct((model, rows), BF16),
        ),
        grid_spec=pltpu.PrefetchScalarGridSpec(
            num_scalar_prefetch=1,
            grid=(rows // BLK,),
            in_specs=[pl.BlockSpec(memory_space=pl.ANY) for _ in ins],
            out_specs=(o_spec, out_spec, dkv_spec, xt_spec),
            scratch_shapes=[
                *[pltpu.VMEM((seq, hd), BF16) for _ in "kv"],
                *[pltpu.VMEM((hd, seq), BF16) for _ in "kv"],
                *[pltpu.VMEM((seq, hd), F32) for _ in "kv"],
                *[pltpu.VMEM((hd, wide), BF16) for _ in "qd"],
                *[pltpu.VMEM((wide, hd), BF16) for _ in "qd"],
                pltpu.VMEM((seq, wide), F32),
                pltpu.VMEM((seq, wide), BF16),
                pltpu.VMEM((BLK, wide), BF16),
                *[pltpu.VMEM((hd, wide), F32) for _ in "od"],
                pltpu.VMEM((8, wide), F32),
                pltpu.VMEM((1, wide), F32),
                pltpu.VMEM((model, width), BF16),
                pltpu.VMEM((width, model), BF16),
                *[pltpu.VMEM((2, BLK, model), BF16) for _ in "xd"],
                *[pltpu.SemaphoreType.DMA((2,)) for _ in "wxdg"],
            ],
        ),
        compiler_params=params(1, 63),
        cost_estimate=cost(8e9 * (rows // BLK), 20e6),
    )(rank, *ins)


def y_kernel(sc, o_mine, o_other, w_mine, w_other, out_ref, os):
    half = o_mine.shape[0]

    @pl.when(pl.program_id(0) == 0)
    def _():
        os[:, :half] = o_mine[...].T
        os[:, half:] = o_other[...].T

    out_ref[...] = (dot(os[:, :half], w_mine[...]) + dot(os[:, half:], w_other[...])).astype(BF16)


def out_rows(core, o_mine, o_other, wo):
    rows, half, model, tile = DUO, o_mine.shape[0], wo.shape[1], DUO
    return pl.pallas_call(
        y_kernel,
        out_shape=jax.ShapeDtypeStruct((rows, model), BF16),
        grid_spec=pltpu.PrefetchScalarGridSpec(
            num_scalar_prefetch=1,
            grid=(model // tile,),
            in_specs=[
                pl.BlockSpec((half, rows), lambda i, s: (0, s[0])),
                pl.BlockSpec((half, rows), lambda i, s: (0, s[0])),
                pl.BlockSpec((half, tile), lambda i, s: (s[0], i)),
                pl.BlockSpec((half, tile), lambda i, s: (1 - s[0], i)),
            ],
            out_specs=pl.BlockSpec((rows, tile), lambda i, s: (0, i)),
            scratch_shapes=[pltpu.VMEM((rows, 2 * half), BF16)],
        ),
        compiler_params=params(),
        cost_estimate=cost(4 * rows * half * model, 12e6),
    )(core, o_mine, o_other, wo, wo)


PIECES = ((0, DUO), (1, DUO), (0, BLK), (1, BLK), (0, BLK), (1, BLK))
STARTS = (0, DUO, HALF, 1280, 1536, 1792)


def piece_copies(core, arrays, dst, sem):
    copies = []
    for n, ((flip, size), start) in enumerate(zip(PIECES, STARTS)):
        at = pl.ds(pl.multiple_of((1 - core if flip else core) * size, size), size)
        copies.append(pltpu.make_async_copy(arrays[n // 2].at[:, at], dst.at[:, start : start + size], sem))
    return copies


def tail_kernel(sc, *refs):
    o_mine, o_other, ys, q_mine, q_other, kv_in = (refs[a:b] for a, b in ((0, 3), (3, 6), (6, 12), (12, 15), (15, 18), (18, 20)))
    xts, (wq_mine, wq_other, wkv), refs = refs[20:23], refs[23:26], refs[26:]
    gwo_ref, gwq_ref, gk_ref, gv_ref, dx_ref, o_all, y_all, dq, kv, kv_rows, sems = refs
    step, core, hd = pl.program_id(0), sc[0], HD
    tile, wide = gwo_ref.shape
    spans = [slice(0, HALF), slice(HALF, HALF + DUO), slice(HALF + DUO, SEQ)]
    o_copies = [piece_copies(core, o, o_all.at[n], sems.at[n]) for n, o in enumerate((o_mine, o_other))]
    y_copies = [
        [
            pltpu.make_async_copy(
                y.at[y.shape[0] - r if r == BLK else 0 :, n * wide : (n + 1) * wide], y_all.at[n, s : s + r, :], sems.at[2 + n]
            )
            for y, s, (_, r) in zip(ys, STARTS, PIECES)
        ]
        for n in range(2)
    ]
    q_copies = [
        [pltpu.make_async_copy(a, dq.at[n, at, :], sems.at[4]) for a, at in zip(part, spans)]
        for n, part in enumerate((q_mine, q_other))
    ]
    kv_copies = [pltpu.make_async_copy(a, kv.at[:, n * BLK : (n + 1) * BLK], sems.at[4]) for n, a in enumerate(kv_in)]

    def start(at, copies):
        @pl.when(step == at)
        def _():
            for cp in copies:
                cp.start()

    def wait(at, copies):
        @pl.when(step == at)
        def _():
            for cp in copies:
                cp.wait()

    rest = q_copies[0] + q_copies[1] + kv_copies
    start(0, y_copies[0] + o_copies[0])
    start(1, o_copies[1])
    start(2, y_copies[1])
    start(3, rest)
    wait(0, y_copies[0] + o_copies[0])
    wait(2, o_copies[1])
    wait(4, y_copies[1])
    wait(WO_STEPS, rest)

    @pl.when(step < WO_STEPS)
    def _():
        rows = pl.ds(pl.multiple_of(step % 2 * tile, tile), tile)
        gwo_ref[...] = dot(o_all[step // 2 % 2, rows, :], y_all[step // 4])

    @pl.when((step >= WO_STEPS) & (step < DX_STEP))
    def _():
        part = (step - WO_STEPS) // 4
        acc = sum(dot(x[...], dq[part, at, :]) for x, at in zip(xts, spans))
        flat = gwq_ref.reshape(tile * 8, hd)
        for h in range(8):
            flat[pl.ds(h, tile, stride=8), :] = acc[:, h * hd : (h + 1) * hd]

    @pl.when((step >= DX_STEP - 4) & (step < DX_STEP))
    def _():
        k_flat, v_flat = gk_ref.reshape(tile * 2, hd), gv_ref.reshape(tile * 2, hd)
        both = sum(dot(x[...], kv[at, :]) for x, at in zip(xts, spans))
        for n, head in enumerate((core, 1 - core)):
            k_flat[pl.ds(head, tile, stride=2), :] = both[:, 2 * n * hd : (2 * n + 1) * hd]
            v_flat[pl.ds(head, tile, stride=2), :] = both[:, (2 * n + 1) * hd : (2 * n + 2) * hd]

    own = pl.ds(pl.multiple_of(core * DUO, DUO), DUO)

    @pl.when(step == DX_STEP)
    def _():
        for n, head in enumerate((core, 1 - core)):
            for v in range(2):
                col = pl.ds(pl.multiple_of((2 * v + head) * hd, hd), hd)
                kv_rows[:, col] = kv[own, (2 * n + v) * hd : (2 * n + v + 1) * hd]

    @pl.when(step >= DX_STEP)
    def _():
        acc = dot_nt(dq[0, own, :], wq_mine[...]) + dot_nt(dq[1, own, :], wq_other[...])
        dx_ref[...] = (acc + dot_nt(kv_rows[...], wkv[...])).astype(BF16)


def tail(core, o_mine, o_other, ys, q_mine, q_other, kvm, kvo, xts, wq, wkv):
    model, half, tile, wide = ys[0].shape[1], o_mine[0].shape[0], DUO, HALF
    wo = lambda i: jnp.minimum(i, WO_STEPS - 1)
    q = lambda i: jnp.clip(i - WO_STEPS, 0, 7)
    kv = lambda i: jnp.clip(i - DX_STEP + 4, 0, 3)
    dx = lambda i: jnp.maximum(i - DX_STEP, 0)
    hbm = [*o_mine, *o_other, *ys, *q_mine, *q_other, kvm, kvo]
    small = pl.BlockSpec((tile, 2, HD), lambda i, s: (kv(i), 0, 0))
    return pl.pallas_call(
        tail_kernel,
        out_shape=(
            jax.ShapeDtypeStruct((2 * half, model), F32),
            jax.ShapeDtypeStruct((model, 16, HD), F32),
            jax.ShapeDtypeStruct((model, 2, HD), F32),
            jax.ShapeDtypeStruct((model, 2, HD), F32),
            jax.ShapeDtypeStruct((DUO, model), BF16),
        ),
        grid_spec=pltpu.PrefetchScalarGridSpec(
            num_scalar_prefetch=1,
            grid=(DX_STEP + 4,),
            in_specs=[pl.BlockSpec(memory_space=pl.ANY) for _ in hbm]
            + [pl.BlockSpec((tile, x.shape[1]), lambda i, s: (q(i) % 4, 0)) for x in xts]
            + [
                pl.BlockSpec((tile, half), lambda i, s: (dx(i), s[0])),
                pl.BlockSpec((tile, half), lambda i, s: (dx(i), 1 - s[0])),
                pl.BlockSpec((tile, DUO), lambda i, s: (dx(i), 0)),
            ],
            out_specs=(
                pl.BlockSpec((tile, wide), lambda i, s: ((s[0] + wo(i) // 2) % 2 * 2 + wo(i) % 2, wo(i) // 4)),
                pl.BlockSpec((tile, 8, HD), lambda i, s: (q(i) % 4, (s[0] + q(i) // 4) % 2, 0)),
                small,
                small,
                pl.BlockSpec((DUO, tile), lambda i, s: (0, dx(i))),
            ),
            scratch_shapes=[
                pltpu.VMEM((2, half, SEQ), BF16),
                pltpu.VMEM((2, SEQ, wide), BF16),
                pltpu.VMEM((2, SEQ, half), BF16),
                pltpu.VMEM((SEQ, DUO), BF16),
                pltpu.VMEM((DUO, DUO), BF16),
                pltpu.SemaphoreType.DMA((5,)),
            ],
        ),
        compiler_params=params(1, 63),
        cost_estimate=cost(5e10, 8e7),
    )(core, *hbm, *xts, wq, wq, wkv)


def solution(mesh):
    row_spec = P(("dp", "cp"), None)
    rep_spec = P(None, None, None)
    part_spec = P("dp", None, None)
    core_swap = [(0, 1), (1, 0), (2, 3), (3, 2)]
    chip_swap = [(0, 2), (2, 0), (1, 3), (3, 1)]

    def device_layer(x, dy, w_query, w_key, w_value, w_out):
        _, model = x.shape
        num_heads, hd = w_query.shape[1:]
        kv_heads = w_key.shape[1]
        scale = hd ** -0.5
        rank = lax.axis_index("cp").astype(jnp.int32)
        c = rank & 1
        core = c.reshape(1)
        rank = rank.reshape(1)

        to_core = lambda v: lax.ppermute(v, "cp", core_swap)
        to_chip = lambda v: lax.ppermute(v, "cp", chip_swap)

        wk = w_key.reshape(model * kv_heads, hd)
        wv = w_value.reshape(model * kv_heads, hd)
        wo = w_out.reshape(num_heads * hd, model)
        x_p = to_core(x)
        dy_p = to_core(dy)

        kv, wkv, r_a, r_b = project_kv(core, x, dy, wk, wv)
        far_kv, kv_p = to_chip(kv), to_core(kv)
        w_s, _ = lax.optimization_barrier((w_query, kv))
        r_a, r_b = to_chip(r_a), to_chip(r_b)
        wq = flat_heads(w_s)
        kv_r, wq = lax.optimization_barrier((far_kv, wq))
        kv_rp = to_core(kv_r)
        pieces = (kv, kv_p, kv_r, kv_rp)

        o_c, dq_c, part, xt_c = attention(
            "near", rank, wq, wo, (x, x_p), (dy, dy_p), 0, pieces, None, scale)
        r_a, o_c, dq_c = lax.optimization_barrier((r_a, o_c, dq_c))
        r_pa, o_co, dq_co = to_core(r_a), to_core(o_c), to_core(dq_c)

        o_a, dq_a, part, xt_a = attention("a", rank, wq, wo, (r_a, r_pa), (r_a, r_pa), BLK, pieces, part, scale)
        r_b, o_a, dq_a = lax.optimization_barrier((r_b, o_a, dq_a))
        r_pb, o_ao, dq_ao = to_core(r_b), to_core(o_a), to_core(dq_a)

        o_b, dq_b, dkv, xt_b = attention("b", rank, wq, wo, (r_b, r_pb), (r_b, r_pb), BLK, pieces, part, scale)
        o_co, dkv = lax.optimization_barrier((o_co, dkv))
        dkv_o, o_bo, dq_bo = to_core(dkv), to_core(o_b), to_core(dq_b)
        y = out_rows(core, o_c, o_co, wo)

        ys = (dy, dy_p, r_a, r_pa, r_b, r_pb)
        gwo, gwq, gwk, gwv, dx = tail(
            core, (o_c, o_a, o_b), (o_co, o_ao, o_bo), ys,
            (dq_c, dq_a, dq_b), (dq_co, dq_ao, dq_bo), dkv, dkv_o, (xt_c, xt_a, xt_b), wq, wkv,
        )
        return y, dx, gwq, gwk, gwv, gwo.reshape(num_heads, hd, model)

    return jax.shard_map(
        device_layer,
        mesh=mesh,
        in_specs=(row_spec, row_spec, rep_spec, rep_spec, rep_spec, rep_spec),
        out_specs=(row_spec, row_spec, part_spec, part_spec, part_spec, part_spec),
        check_vma=False,
    )
```

```python
import functools
import math

import jax
import jax.numpy as jnp
import numpy as np
from jax import lax
from jax.experimental import pallas as pl
from jax.experimental.pallas import tpu as pltpu
from jax.sharding import PartitionSpec as P


BLK = 256
HD = 128
DUO = 512
HALF = 1024
SEQ = 2048
WO_STEPS = 8
DX_STEP = 16
LARGE = 2.0**60
LOW = -3.0e38
F32 = jnp.float32
BF16 = jnp.bfloat16


def dot(a, b):
    return jnp.dot(a, b, preferred_element_type=F32)


def dot_nt(a, b):
    return lax.dot_general(a, b, (((1,), (1,)), ((), ())), preferred_element_type=F32)


def params(n=1, mib=60):
    return pltpu.CompilerParams(
        dimension_semantics=("arbitrary",) * n, vmem_limit_bytes=mib * HALF * HALF
    )


def cost(flops, nbytes):
    return pl.CostEstimate(flops=int(flops), bytes_accessed=int(nbytes), transcendentals=0)


def heads_kernel(perm_ref, w_hbm, out_hbm, w_in, w_out, in_sem, out_sem):
    chunks, rows, num, hd = w_in.shape
    group = perm_ref.shape[0]
    loads = [
        pltpu.make_async_copy(w_hbm.at[c * rows : (c + 1) * rows], w_in.at[c], in_sem.at[c]) for c in range(chunks)
    ]
    stores = [
        pltpu.make_async_copy(w_out.at[c], out_hbm.at[c * rows : (c + 1) * rows, :], out_sem.at[c]) for c in range(chunks)
    ]
    for cp in loads:
        cp.start()

    def chunk(c, _):
        pltpu.make_async_copy(w_hbm.at[:rows], w_in.at[c], in_sem.at[c]).wait()
        flat = w_in.at[c].reshape(rows * num, hd)
        for g in range(0, rows // 16, 2):
            pair = [flat[(g + n) * group : (g + n + 1) * group, :] for n in range(2)]
            res = dot(perm_ref[...], jnp.concatenate(pair, axis=1)).astype(BF16)
            for n in range(2):
                for h in range(num):
                    w_out[c, (g + n) * 16 : (g + n + 1) * 16, h * hd : (h + 1) * hd] = res[
                        h * 16 : (h + 1) * 16, n * hd : (n + 1) * hd
                    ]
        at = pl.ds(pl.multiple_of(c * rows, rows), rows)
        pltpu.make_async_copy(w_out.at[c], out_hbm.at[at, :], out_sem.at[c]).start()
        return 0

    lax.fori_loop(0, chunks, chunk, 0)
    for cp in stores:
        cp.wait()


def gather_heads(num, rows):
    row = np.arange(num * rows)
    return jnp.asarray((row % rows * num + row // rows)[:, None] == row[None, :], BF16)


def flat_heads(w):
    model, num, hd = w.shape
    chunks = 8
    rows = model // chunks
    return pl.pallas_call(
        heads_kernel,
        out_shape=jax.ShapeDtypeStruct((model, num * hd), BF16),
        in_specs=[pl.BlockSpec(memory_space=pltpu.VMEM), pl.BlockSpec(memory_space=pl.ANY)],
        out_specs=pl.BlockSpec(memory_space=pl.ANY),
        scratch_shapes=[
            pltpu.VMEM((chunks, rows, num, hd), BF16),
            pltpu.VMEM((chunks, rows, num * hd), BF16),
            pltpu.SemaphoreType.DMA((chunks,)),
            pltpu.SemaphoreType.DMA((chunks,)),
        ],
        compiler_params=pltpu.CompilerParams(vmem_limit_bytes=params(1).vmem_limit_bytes),
        cost_estimate=cost(4e9, 4 * model * num * hd),
    )(gather_heads(num, 16), w)


def kv_kernel(sc, x_ref, dy_ref, wk_ref, wv_ref, perm_ref, out_ref, w_hbm, rows_a, rows_b, w_ref, sems):
    step, core = pl.program_id(0), sc[0]
    save_w = pltpu.make_async_copy(w_ref, w_hbm, sems.at[2])

    def cut(dst, n):
        return [
            pltpu.make_async_copy(src, dst.at[at : at + BLK, :], sems.at[n])
            for src, at in ((x_ref, 0), (dy_ref, BLK))
        ]

    for n, dst in enumerate((rows_a, rows_b)):

        @pl.when(step == (1 - core if n == 0 else core))
        def _():
            for cp in cut(dst, n):
                cp.start()

    @pl.when(pl.program_id(0) == 0)
    def _():
        for g in range(w_ref.shape[0] // HD):
            rows = slice(g * BLK, (g + 1) * BLK)
            pair = jnp.concatenate([wk_ref[rows, :], wv_ref[rows, :]], axis=1)
            res = dot(perm_ref[...], pair).astype(BF16)
            for h in range(2):
                for v in range(2):
                    col = (v * 2 + h) * HD
                    w_ref[g * HD : (g + 1) * HD, col : col + HD] = res[h * HD : (h + 1) * HD, v * HD : (v + 1) * HD]

        save_w.start()

    out_ref[...] = dot(x_ref[...], w_ref[...]).astype(BF16)

    @pl.when(step == 1)
    def _():
        save_w.wait()
        for n, dst in enumerate((rows_a, rows_b)):
            for cp in cut(dst, n):
                cp.wait()


def project_kv(core, x, dy, wk, wv):
    rows, depth = x.shape
    row = pl.BlockSpec((BLK, depth), lambda i, s: (i, 0))
    fixed = lambda shape: pl.BlockSpec(shape, lambda i, s: (0, 0))
    chunk = jax.ShapeDtypeStruct((rows, depth), BF16)
    return pl.pallas_call(
        kv_kernel,
        out_shape=(jax.ShapeDtypeStruct((rows, DUO), BF16), jax.ShapeDtypeStruct((depth, DUO), BF16), chunk, chunk),
        grid_spec=pltpu.PrefetchScalarGridSpec(
            num_scalar_prefetch=1,
            grid=(rows // BLK,),
            in_specs=[row, row, fixed(wk.shape), fixed(wv.shape), fixed((BLK, BLK))],
            out_specs=(pl.BlockSpec((BLK, DUO), lambda i, s: (i, 0)),) + (pl.BlockSpec(memory_space=pl.ANY),) * 3,
            scratch_shapes=[pltpu.VMEM((depth, DUO), BF16), pltpu.SemaphoreType.DMA((3,))],
        ),
        compiler_params=params(),
        cost_estimate=cost(2 * rows * depth * DUO, 8e6),
    )(core, x, dy, wk, wv, gather_heads(2, HD))


def ranks(rank):
    return rank, rank + 1 - rank % 2 * 2, (rank + 2) % 4, 3 - rank


def block_at(kind, rank, i):
    own, pair, far, far_pair = ranks(rank)
    if kind == "near":
        e = jnp.where(i < 2, own, pair)
        return jnp.where(i % 2 == 0, e, 7 - e)
    e = jnp.where(i == 0, far, far_pair)
    return jnp.where(e % 2 == (1 if kind == "a" else 0), e, 7 - e)


def slot_at(kind, rank, i):
    if kind == "near":
        return (rank + i // 2) % 2 * 2 + i % 2
    return (rank + i) % 2


def attn_kernel(kind, heads, scale, steps, base, sc, wq_hbm, wo_hbm, *refs):
    x_hbm, dy_hbm, kv_hbm, refs = refs[:2], refs[2:4], refs[4:8], refs[8:]
    first, final = kind == "near", kind == "b"
    if first:
        o_ref, dq_ref, dkv_ref, xt_ref = refs[:4]
        scratch = refs[4:]
    else:
        init_hbm, o_ref, dq_ref, dkv_ref, xt_ref = refs[:5]
        scratch = refs[5:]
    ks, vs, kt, vt, dk, dv, qt, dot_t, qst, dost, s_ref, p_ref, ds_ref, ot, dqt, l_ref, ref, wq, wo, xs, dys, w_sem, x_sem, dy_sem, g_sem = scratch
    step = pl.program_id(0)
    hd = HD
    c2 = scale * math.log2(math.e)

    rank = sc[0]
    pos = [p for e in ranks(rank) for p in (e, 7 - e)]
    core = pl.multiple_of(rank % 2 * heads * hd, heads * hd)
    load_kv = []
    for n, p in enumerate(pos):
        src = kv_hbm[n // 2].at[n % 2 * BLK : (n % 2 + 1) * BLK, :]
        at = pl.ds(pl.multiple_of(p * BLK, BLK), BLK)
        for v, dst in enumerate((ks, vs)):
            col = pl.ds(pl.multiple_of((2 * v + rank % 2) * hd, hd), hd)
            load_kv.append(pltpu.make_async_copy(src.at[:, col], dst.at[at, :], g_sem.at[0]))

    def grads(hbm, out):
        pairs = [(hbm.at[:, :hd], dk), (hbm.at[:, hd:], dv)]
        return [pltpu.make_async_copy(*(p[::-1] if out else p), g_sem.at[1]) for p in pairs]

    load_wq, load_wo = [], []
    for n in range(4):
        span = slice(n * DUO, (n + 1) * DUO)
        load_wq.append(pltpu.make_async_copy(wq_hbm.at[span, pl.ds(core, heads * hd)], wq.at[span, :], w_sem.at[0]))
        rows = heads * hd // 4
        dst = wo.at[n * rows : (n + 1) * rows, :]
        load_wo.append(pltpu.make_async_copy(wo_hbm.at[pl.ds(core + n * rows, rows), :], dst, w_sem.at[1]))

    def load_rows(n):
        piece, row = divmod(n, steps // 2)
        src = pl.ds(row * BLK, BLK)
        return (
            pltpu.make_async_copy(x_hbm[piece].at[src, :], xs.at[n % 2], x_sem.at[n % 2]),
            pltpu.make_async_copy(dy_hbm[piece].at[pl.ds(base + row * BLK, BLK), :], dys.at[n % 2], dy_sem.at[n % 2]),
        )

    @pl.when(step == 0)
    def _():
        load_x, _ = load_rows(0)
        for cp in load_kv:
            cp.start()
        load_x.start()
        for cp in load_wq:
            cp.start()

    @pl.when(step == 0)
    def _():
        if first:
            dk[...] = jnp.zeros_like(dk)
            dv[...] = jnp.zeros_like(dv)
        for cp in load_kv:
            cp.wait()
        for i in range(8):
            at = slice(i * BLK, (i + 1) * BLK)
            kt[:, at] = ks[at, :].T
            vt[:, at] = vs[at, :].T
        for cp in [load_rows(0)[1], *load_wo, *([] if first else grads(init_hbm, False))]:
            cp.start()

    @pl.when(step == 0)
    def _():
        for cp in load_wq:
            cp.wait()

    slot = step % 2
    pltpu.make_async_copy(x_hbm[0].at[0:BLK, :], xs.at[slot], x_sem.at[slot]).wait()
    q = dot(xs[slot], wq[...]).astype(BF16)
    xt_ref[...] = xs[slot].T
    for h in range(heads):
        qh = q[:, h * hd : (h + 1) * hd]
        qst[h * BLK : (h + 1) * BLK, :] = qh
        qt[:, h * BLK : (h + 1) * BLK] = qh.T

    @pl.when(step == 0)
    def _():
        for cp in load_wo:
            cp.wait()

    pltpu.make_async_copy(dy_hbm[0].at[0:BLK, :], dys.at[slot], dy_sem.at[slot]).wait()
    do = dot_nt(dys[slot], wo[...]).astype(BF16)

    for n in range(1, steps):

        @pl.when(step == n - 1)
        def _():
            for cp in load_rows(n):
                cp.start()

    for h in range(heads):
        dh = do[:, h * hd : (h + 1) * hd]
        dost[h * BLK : (h + 1) * BLK, :] = dh
        dot_t[:, h * BLK : (h + 1) * BLK] = dh.T

    b = block_at(kind, rank, step)

    def sweep(count, block):
        def pair(j, _):
            block(pl.multiple_of(j * 2 * BLK, 2 * BLK), 2 * BLK)
            return 0

        lax.fori_loop(0, count // 2, pair, 0)

        @pl.when(count % 2 == 1)
        def _():
            block(pl.multiple_of((count - 1) * BLK, BLK), BLK)

    def scores(start, rows, h):
        at = pl.ds(start, rows)
        return at, slice(h * BLK, (h + 1) * BLK), dot(ks[at, :], qt[:, h * BLK : (h + 1) * BLK]) * c2

    def rows_of(t):
        return t.reshape(t.shape[0] // 8, 8, BLK)

    key = lax.broadcasted_iota(jnp.int32, (BLK, BLK), 0)
    query = lax.broadcasted_iota(jnp.int32, (BLK, BLK), 1)
    for h in range(heads):
        at, span, t = scores(pl.multiple_of(b * BLK, BLK), BLK, h)
        t = jnp.where(key <= query, t, LOW)
        s_ref[at, span] = t
        base = jnp.max(t, axis=0, keepdims=True)
        ref[:, span] = base
        l_ref[:, span] = jnp.sum(jnp.exp2(rows_of(t - base)), axis=0)

    def open_block(start, rows):
        for h in range(heads):
            at, span, t = scores(start, rows, h)
            s_ref[at, span] = t
            l_ref[:, span] += jnp.sum(jnp.exp2(rows_of(t - ref[:, span])), axis=0)

    sweep(b, open_block)

    @pl.when(jnp.max(l_ref[...]) > LARGE)
    def _():
        def each(start, fn):
            for h in range(heads):
                span = slice(h * BLK, (h + 1) * BLK)
                fn(span, s_ref[pl.ds(start, BLK), span])

        def peak(span, t):
            ref[:, span] = jnp.maximum(ref[:, span], jnp.max(t, axis=0, keepdims=True))

        def total(span, t):
            l_ref[:, span] += jnp.sum(jnp.exp2(rows_of(t - ref[:, span])), axis=0)

        def over(fn):
            def body(j, _):
                each(pl.multiple_of(j * BLK, BLK), fn)
                return 0

            lax.fori_loop(0, b + 1, body, 0)

        over(peak)
        l_ref[...] = jnp.zeros_like(l_ref)
        over(total)

    lse = ref[...] + jnp.log2(jnp.sum(l_ref[...], axis=0, keepdims=True))

    ot[...] = jnp.zeros_like(ot)

    def value_block(start, rows):
        at = pl.ds(start, rows)
        for h in range(heads):
            span = slice(h * BLK, (h + 1) * BLK)
            p = jnp.exp2(s_ref[at, span] - lse[:, span]).astype(BF16)
            p_ref[at, span] = p
            ot[:, span] += dot(vt[:, at], p)

    sweep(b + 1, value_block)

    o_round = ot[...].astype(BF16)
    delta = jnp.sum(o_round.astype(F32) * dot_t[...].astype(F32), axis=0, keepdims=True)
    for h in range(heads):
        o_ref[h * hd : (h + 1) * hd, :] = o_round[:, h * BLK : (h + 1) * BLK]
    dqt[...] = jnp.zeros_like(dqt)

    def grad_block(j, _):
        at = pl.ds(pl.multiple_of(j * BLK, BLK), BLK)
        dp = dot(vs[at, :], dot_t[...])
        dv[at, :] += dot(p_ref[at, :], dost[...])
        ds = (p_ref[at, :].astype(F32) * (dp - delta)).astype(BF16)
        ds_ref[...] = ds
        dqt[...] += dot(kt[:, at], ds_ref[...])
        dk[at, :] += dot(ds_ref[...], qst[...])
        return 0

    if not first:

        @pl.when(step == 0)
        def _():
            for cp in grads(init_hbm, False):
                cp.wait()

    lax.fori_loop(0, b + 1, grad_block, 0)

    for h in range(heads):
        dq_ref[:, h * hd : (h + 1) * hd] = (dqt[:, h * BLK : (h + 1) * BLK] * scale).astype(BF16).T

    @pl.when(step == steps - 1)
    def _():
        if not final:
            for cp in grads(dkv_ref, True):
                cp.start()
            for cp in grads(dkv_ref, True):
                cp.wait()
        else:
            for n, (p, e) in enumerate(zip(pos, [e for e in ranks(rank) for _ in "ab"])):
                at = pl.ds(pl.multiple_of(p * BLK, BLK), BLK)
                if n < 4:
                    row = e % 2 * 2 + n % 2
                else:
                    row = jnp.where((e + n) % 2 == 1, 4, 6) + e % 2
                out = pl.ds(pl.multiple_of(row * BLK, BLK), BLK)
                dkv_ref[out, :hd] = (dk[at, :] * scale).astype(BF16)
                dkv_ref[out, hd:] = dv[at, :].astype(BF16)


def attention(kind, rank, wq, wo, x_pieces, dy_pieces, base, kv_pieces, init, scale):
    final = kind == "b"
    rows, width, model = 2 * (x_pieces[0].shape[0] - base), wq.shape[1] // 2, wq.shape[0]
    hd = HD
    heads = width // hd
    wide = heads * BLK
    seq = SEQ
    slot = functools.partial(slot_at, kind)
    o_spec = pl.BlockSpec((width, BLK), lambda i, s: (0, slot(s[0], i)))
    out_spec = pl.BlockSpec((BLK, width), lambda i, s: (slot(s[0], i), 0))
    xt_spec = pl.BlockSpec((model, BLK), lambda i, s: (0, slot(s[0], i)))
    dkv_spec = pl.BlockSpec((seq, BLK), lambda i, s: (0, 0)) if final else pl.BlockSpec(memory_space=pl.ANY)
    ins = [wq, wo, *x_pieces, *dy_pieces, *kv_pieces] + ([] if init is None else [init])
    return pl.pallas_call(
        functools.partial(attn_kernel, kind, heads, scale, rows // BLK, base),
        out_shape=(
            jax.ShapeDtypeStruct((width, rows), BF16),
            jax.ShapeDtypeStruct((rows, width), BF16),
            jax.ShapeDtypeStruct((seq, BLK), BF16 if final else F32),
            jax.ShapeDtypeStruct((model, rows), BF16),
        ),
        grid_spec=pltpu.PrefetchScalarGridSpec(
            num_scalar_prefetch=1,
            grid=(rows // BLK,),
            in_specs=[pl.BlockSpec(memory_space=pl.ANY) for _ in ins],
            out_specs=(o_spec, out_spec, dkv_spec, xt_spec),
            scratch_shapes=[
                *[pltpu.VMEM((seq, hd), BF16) for _ in "kv"],
                *[pltpu.VMEM((hd, seq), BF16) for _ in "kv"],
                *[pltpu.VMEM((seq, hd), F32) for _ in "kv"],
                *[pltpu.VMEM((hd, wide), BF16) for _ in "qd"],
                *[pltpu.VMEM((wide, hd), BF16) for _ in "qd"],
                pltpu.VMEM((seq, wide), F32),
                pltpu.VMEM((seq, wide), BF16),
                pltpu.VMEM((BLK, wide), BF16),
                *[pltpu.VMEM((hd, wide), F32) for _ in "od"],
                pltpu.VMEM((8, wide), F32),
                pltpu.VMEM((1, wide), F32),
                pltpu.VMEM((model, width), BF16),
                pltpu.VMEM((width, model), BF16),
                *[pltpu.VMEM((2, BLK, model), BF16) for _ in "xd"],
                *[pltpu.SemaphoreType.DMA((2,)) for _ in "wxdg"],
            ],
        ),
        compiler_params=params(1, 63),
        cost_estimate=cost(8e9 * (rows // BLK), 20e6),
    )(rank, *ins)


def y_kernel(sc, o_mine, o_other, w_mine, w_other, out_ref, os):
    half = o_mine.shape[0]

    @pl.when(pl.program_id(0) == 0)
    def _():
        os[:, :half] = o_mine[...].T
        os[:, half:] = o_other[...].T

    out_ref[...] = (dot(os[:, :half], w_mine[...]) + dot(os[:, half:], w_other[...])).astype(BF16)


def out_rows(core, o_mine, o_other, wo):
    rows, half, model, tile = DUO, o_mine.shape[0], wo.shape[1], DUO
    return pl.pallas_call(
        y_kernel,
        out_shape=jax.ShapeDtypeStruct((rows, model), BF16),
        grid_spec=pltpu.PrefetchScalarGridSpec(
            num_scalar_prefetch=1,
            grid=(model // tile,),
            in_specs=[
                pl.BlockSpec((half, rows), lambda i, s: (0, s[0])),
                pl.BlockSpec((half, rows), lambda i, s: (0, s[0])),
                pl.BlockSpec((half, tile), lambda i, s: (s[0], i)),
                pl.BlockSpec((half, tile), lambda i, s: (1 - s[0], i)),
            ],
            out_specs=pl.BlockSpec((rows, tile), lambda i, s: (0, i)),
            scratch_shapes=[pltpu.VMEM((rows, 2 * half), BF16)],
        ),
        compiler_params=params(),
        cost_estimate=cost(4 * rows * half * model, 12e6),
    )(core, o_mine, o_other, wo, wo)


PIECES = ((0, DUO), (1, DUO), (0, BLK), (1, BLK), (0, BLK), (1, BLK))
STARTS = (0, DUO, HALF, 1280, 1536, 1792)


def piece_copies(core, arrays, dst, sem, rows):
    copies = []
    for n, ((flip, size), start) in enumerate(zip(PIECES, STARTS)):
        at = pl.ds(pl.multiple_of((1 - core if flip else core) * size, size), size)
        copies.append(pltpu.make_async_copy(arrays[n // 2].at[rows, at], dst.at[rows, start : start + size], sem))
    return copies


def tail_kernel(sc, *refs):
    o_mine, o_other, ys, q_mine, q_other, kv_in = (refs[a:b] for a, b in ((0, 3), (3, 6), (6, 12), (12, 15), (15, 18), (18, 20)))
    xts, (wq_mine, wq_other, wkv), refs = refs[20:23], refs[23:26], refs[26:]
    gwo_ref, gwq_ref, gk_ref, gv_ref, dx_ref, o_all, y_all, dq, kv, kv_rows, sems = refs
    step, core, hd = pl.program_id(0), sc[0], HD
    tile, wide = gwo_ref.shape
    spans = [slice(0, HALF), slice(HALF, HALF + DUO), slice(HALF + DUO, SEQ)]
    o_copies = [
        [piece_copies(core, o, o_all.at[n], sems.at[n, t], slice(t * tile, (t + 1) * tile)) for t in range(2)]
        for n, o in enumerate((o_mine, o_other))
    ]
    y_copies = [
        [
            pltpu.make_async_copy(
                y.at[y.shape[0] - r if r == BLK else 0 :, n * wide : (n + 1) * wide], y_all.at[n, s : s + r, :], sems.at[2, n]
            )
            for y, s, (_, r) in zip(ys, STARTS, PIECES)
        ]
        for n in range(2)
    ]
    q_copies = [
        [pltpu.make_async_copy(a, dq.at[n, at, :], sems.at[3, 0]) for a, at in zip(part, spans)]
        for n, part in enumerate((q_mine, q_other))
    ]
    kv_copies = [pltpu.make_async_copy(a, kv.at[:, n * BLK : (n + 1) * BLK], sems.at[3, 0]) for n, a in enumerate(kv_in)]

    def start(at, copies):
        @pl.when(step == at)
        def _():
            for cp in copies:
                cp.start()

    def wait(at, copies):
        @pl.when(step == at)
        def _():
            for cp in copies:
                cp.wait()

    rest = q_copies[0] + q_copies[1] + kv_copies
    start(0, o_copies[0][0] + y_copies[0])
    wait(0, o_copies[0][0] + y_copies[0])
    start(0, o_copies[0][1] + o_copies[1][0] + o_copies[1][1])
    start(2, y_copies[1])
    start(3, rest)
    wait(1, o_copies[0][1])
    wait(2, o_copies[1][0] + o_copies[1][1])
    wait(4, y_copies[1])
    wait(WO_STEPS, rest)

    @pl.when(step < WO_STEPS)
    def _():
        rows = pl.ds(pl.multiple_of(step % 2 * tile, tile), tile)
        gwo_ref[...] = dot(o_all[step // 2 % 2, rows, :], y_all[step // 4])

    @pl.when((step >= WO_STEPS) & (step < DX_STEP))
    def _():
        part = (step - WO_STEPS) // 4
        acc = sum(dot(x[...], dq[part, at, :]) for x, at in zip(xts, spans))
        flat = gwq_ref.reshape(tile * 8, hd)
        for h in range(8):
            flat[pl.ds(h, tile, stride=8), :] = acc[:, h * hd : (h + 1) * hd]

    @pl.when((step >= DX_STEP - 4) & (step < DX_STEP))
    def _():
        k_flat, v_flat = gk_ref.reshape(tile * 2, hd), gv_ref.reshape(tile * 2, hd)
        both = sum(dot(x[...], kv[at, :]) for x, at in zip(xts, spans))
        for n, head in enumerate((core, 1 - core)):
            k_flat[pl.ds(head, tile, stride=2), :] = both[:, 2 * n * hd : (2 * n + 1) * hd]
            v_flat[pl.ds(head, tile, stride=2), :] = both[:, (2 * n + 1) * hd : (2 * n + 2) * hd]

    own = pl.ds(pl.multiple_of(core * DUO, DUO), DUO)

    @pl.when(step == DX_STEP)
    def _():
        for n, head in enumerate((core, 1 - core)):
            for v in range(2):
                col = pl.ds(pl.multiple_of((2 * v + head) * hd, hd), hd)
                kv_rows[:, col] = kv[own, (2 * n + v) * hd : (2 * n + v + 1) * hd]

    @pl.when(step >= DX_STEP)
    def _():
        acc = dot_nt(dq[0, own, :], wq_mine[...]) + dot_nt(dq[1, own, :], wq_other[...])
        dx_ref[...] = (acc + dot_nt(kv_rows[...], wkv[...])).astype(BF16)


def tail(core, o_mine, o_other, ys, q_mine, q_other, kvm, kvo, xts, wq, wkv):
    model, half, tile, wide = ys[0].shape[1], o_mine[0].shape[0], DUO, HALF
    wo = lambda i: jnp.minimum(i, WO_STEPS - 1)
    q = lambda i: jnp.clip(i - WO_STEPS, 0, 7)
    kv = lambda i: jnp.clip(i - DX_STEP + 4, 0, 3)
    dx = lambda i: jnp.maximum(i - DX_STEP, 0)
    hbm = [*o_mine, *o_other, *ys, *q_mine, *q_other, kvm, kvo]
    small = pl.BlockSpec((tile, 2, HD), lambda i, s: (kv(i), 0, 0))
    return pl.pallas_call(
        tail_kernel,
        out_shape=(
            jax.ShapeDtypeStruct((2 * half, model), F32),
            jax.ShapeDtypeStruct((model, 16, HD), F32),
            jax.ShapeDtypeStruct((model, 2, HD), F32),
            jax.ShapeDtypeStruct((model, 2, HD), F32),
            jax.ShapeDtypeStruct((DUO, model), BF16),
        ),
        grid_spec=pltpu.PrefetchScalarGridSpec(
            num_scalar_prefetch=1,
            grid=(DX_STEP + 4,),
            in_specs=[pl.BlockSpec(memory_space=pl.ANY) for _ in hbm]
            + [pl.BlockSpec((tile, x.shape[1]), lambda i, s: (q(i) % 4, 0)) for x in xts]
            + [
                pl.BlockSpec((tile, half), lambda i, s: (dx(i), s[0])),
                pl.BlockSpec((tile, half), lambda i, s: (dx(i), 1 - s[0])),
                pl.BlockSpec((tile, DUO), lambda i, s: (dx(i), 0)),
            ],
            out_specs=(
                pl.BlockSpec((tile, wide), lambda i, s: ((s[0] + wo(i) // 2) % 2 * 2 + wo(i) % 2, wo(i) // 4)),
                pl.BlockSpec((tile, 8, HD), lambda i, s: (q(i) % 4, (s[0] + q(i) // 4) % 2, 0)),
                small,
                small,
                pl.BlockSpec((DUO, tile), lambda i, s: (0, dx(i))),
            ),
            scratch_shapes=[
                pltpu.VMEM((2, half, SEQ), BF16),
                pltpu.VMEM((2, SEQ, wide), BF16),
                pltpu.VMEM((2, SEQ, half), BF16),
                pltpu.VMEM((SEQ, DUO), BF16),
                pltpu.VMEM((DUO, DUO), BF16),
                pltpu.SemaphoreType.DMA((4, 2)),
            ],
        ),
        compiler_params=params(1, 63),
        cost_estimate=cost(5e10, 8e7),
    )(core, *hbm, *xts, wq, wq, wkv)


def solution(mesh):
    row_spec = P(("dp", "cp"), None)
    rep_spec = P(None, None, None)
    part_spec = P("dp", None, None)
    core_swap = [(0, 1), (1, 0), (2, 3), (3, 2)]
    chip_swap = [(0, 2), (2, 0), (1, 3), (3, 1)]

    def device_layer(x, dy, w_query, w_key, w_value, w_out):
        _, model = x.shape
        num_heads, hd = w_query.shape[1:]
        kv_heads = w_key.shape[1]
        scale = hd ** -0.5
        rank = lax.axis_index("cp").astype(jnp.int32)
        c = rank & 1
        core = c.reshape(1)
        rank = rank.reshape(1)

        to_core = lambda v: lax.ppermute(v, "cp", core_swap)
        to_chip = lambda v: lax.ppermute(v, "cp", chip_swap)

        wk = w_key.reshape(model * kv_heads, hd)
        wv = w_value.reshape(model * kv_heads, hd)
        wo = w_out.reshape(num_heads * hd, model)
        x_p = to_core(x)
        dy_p = to_core(dy)

        kv, wkv, r_a, r_b = project_kv(core, x, dy, wk, wv)
        far_kv, kv_p = to_chip(kv), to_core(kv)
        w_s, _ = lax.optimization_barrier((w_query, kv))
        r_a, r_b = to_chip(r_a), to_chip(r_b)
        wq = flat_heads(w_s)
        kv_r, wq = lax.optimization_barrier((far_kv, wq))
        kv_rp = to_core(kv_r)
        pieces = (kv, kv_p, kv_r, kv_rp)

        o_c, dq_c, part, xt_c = attention(
            "near", rank, wq, wo, (x, x_p), (dy, dy_p), 0, pieces, None, scale)
        r_a, o_c, dq_c = lax.optimization_barrier((r_a, o_c, dq_c))
        r_pa, o_co, dq_co = to_core(r_a), to_core(o_c), to_core(dq_c)

        o_a, dq_a, part, xt_a = attention("a", rank, wq, wo, (r_a, r_pa), (r_a, r_pa), BLK, pieces, part, scale)
        r_b, o_a, dq_a = lax.optimization_barrier((r_b, o_a, dq_a))
        r_pb, o_ao, dq_ao = to_core(r_b), to_core(o_a), to_core(dq_a)

        o_b, dq_b, dkv, xt_b = attention("b", rank, wq, wo, (r_b, r_pb), (r_b, r_pb), BLK, pieces, part, scale)
        o_co, dkv = lax.optimization_barrier((o_co, dkv))
        dkv_o, o_bo, dq_bo = to_core(dkv), to_core(o_b), to_core(dq_b)
        y = out_rows(core, o_c, o_co, wo)

        ys = (dy, dy_p, r_a, r_pa, r_b, r_pb)
        gwo, gwq, gwk, gwv, dx = tail(
            core, (o_c, o_a, o_b), (o_co, o_ao, o_bo), ys,
            (dq_c, dq_a, dq_b), (dq_co, dq_ao, dq_bo), dkv, dkv_o, (xt_c, xt_a, xt_b), wq, wkv,
        )
        return y, dx, gwq, gwk, gwv, gwo.reshape(num_heads, hd, model)

    return jax.shard_map(
        device_layer,
        mesh=mesh,
        in_specs=(row_spec, row_spec, rep_spec, rep_spec, rep_spec, rep_spec),
        out_specs=(row_spec, row_spec, part_spec, part_spec, part_spec, part_spec),
        check_vma=False,
    )
```

```python
import functools
import math

import jax
import jax.numpy as jnp
import numpy as np
from jax import lax
from jax.experimental import pallas as pl
from jax.experimental.pallas import tpu as pltpu
from jax.sharding import PartitionSpec as P


BLK = 256
HD = 128
DUO = 512
HALF = 1024
SEQ = 2048
WO_STEPS = 8
DX_STEP = 16
LARGE = 2.0**60
LOW = -3.0e38
F32 = jnp.float32
BF16 = jnp.bfloat16


def dot(a, b):
    return jnp.dot(a, b, preferred_element_type=F32)


def dot_nt(a, b):
    return lax.dot_general(a, b, (((1,), (1,)), ((), ())), preferred_element_type=F32)


def params(n=1, mib=60):
    return pltpu.CompilerParams(
        dimension_semantics=("arbitrary",) * n, vmem_limit_bytes=mib * HALF * HALF
    )


def cost(flops, nbytes):
    return pl.CostEstimate(flops=int(flops), bytes_accessed=int(nbytes), transcendentals=0)


def heads_kernel(perm_ref, w_hbm, out_hbm, w_in, w_out, in_sem, out_sem):
    chunks, rows, num, hd = w_in.shape
    group = perm_ref.shape[0]
    loads = [
        pltpu.make_async_copy(w_hbm.at[c * rows : (c + 1) * rows], w_in.at[c], in_sem.at[c]) for c in range(chunks)
    ]
    stores = [
        pltpu.make_async_copy(w_out.at[c], out_hbm.at[c * rows : (c + 1) * rows, :], out_sem.at[c]) for c in range(chunks)
    ]
    for cp in loads:
        cp.start()

    def chunk(c, _):
        pltpu.make_async_copy(w_hbm.at[:rows], w_in.at[c], in_sem.at[c]).wait()
        flat = w_in.at[c].reshape(rows * num, hd)
        for g in range(0, rows // 16, 2):
            pair = [flat[(g + n) * group : (g + n + 1) * group, :] for n in range(2)]
            res = dot(perm_ref[...], jnp.concatenate(pair, axis=1)).astype(BF16)
            for n in range(2):
                for h in range(num):
                    w_out[c, (g + n) * 16 : (g + n + 1) * 16, h * hd : (h + 1) * hd] = res[
                        h * 16 : (h + 1) * 16, n * hd : (n + 1) * hd
                    ]
        at = pl.ds(pl.multiple_of(c * rows, rows), rows)
        pltpu.make_async_copy(w_out.at[c], out_hbm.at[at, :], out_sem.at[c]).start()
        return 0

    lax.fori_loop(0, chunks, chunk, 0)
    for cp in stores:
        cp.wait()


def gather_heads(num, rows):
    row = np.arange(num * rows)
    return jnp.asarray((row % rows * num + row // rows)[:, None] == row[None, :], BF16)


def flat_heads(w):
    model, num, hd = w.shape
    chunks = 8
    rows = model // chunks
    return pl.pallas_call(
        heads_kernel,
        out_shape=jax.ShapeDtypeStruct((model, num * hd), BF16),
        in_specs=[pl.BlockSpec(memory_space=pltpu.VMEM), pl.BlockSpec(memory_space=pl.ANY)],
        out_specs=pl.BlockSpec(memory_space=pl.ANY),
        scratch_shapes=[
            pltpu.VMEM((chunks, rows, num, hd), BF16),
            pltpu.VMEM((chunks, rows, num * hd), BF16),
            pltpu.SemaphoreType.DMA((chunks,)),
            pltpu.SemaphoreType.DMA((chunks,)),
        ],
        compiler_params=pltpu.CompilerParams(vmem_limit_bytes=params(1).vmem_limit_bytes),
        cost_estimate=cost(4e9, 4 * model * num * hd),
    )(gather_heads(num, 16), w)


def kv_kernel(sc, x_ref, dy_ref, wk_ref, wv_ref, perm_ref, out_ref, w_hbm, rows_a, rows_b, w_ref, sems):
    step, core = pl.program_id(0), sc[0]
    save_w = pltpu.make_async_copy(w_ref, w_hbm, sems.at[2])

    def cut(dst, n):
        return [
            pltpu.make_async_copy(src, dst.at[at : at + BLK, :], sems.at[n])
            for src, at in ((x_ref, 0), (dy_ref, BLK))
        ]

    for n, dst in enumerate((rows_a, rows_b)):

        @pl.when(step == (1 - core if n == 0 else core))
        def _():
            for cp in cut(dst, n):
                cp.start()

    @pl.when(pl.program_id(0) == 0)
    def _():
        for g in range(w_ref.shape[0] // HD):
            rows = slice(g * BLK, (g + 1) * BLK)
            pair = jnp.concatenate([wk_ref[rows, :], wv_ref[rows, :]], axis=1)
            res = dot(perm_ref[...], pair).astype(BF16)
            for h in range(2):
                for v in range(2):
                    col = (v * 2 + h) * HD
                    w_ref[g * HD : (g + 1) * HD, col : col + HD] = res[h * HD : (h + 1) * HD, v * HD : (v + 1) * HD]

        save_w.start()

    out_ref[...] = dot(x_ref[...], w_ref[...]).astype(BF16)

    @pl.when(step == 1)
    def _():
        save_w.wait()
        for n, dst in enumerate((rows_a, rows_b)):
            for cp in cut(dst, n):
                cp.wait()


def project_kv(core, x, dy, wk, wv):
    rows, depth = x.shape
    row = pl.BlockSpec((BLK, depth), lambda i, s: (i, 0))
    fixed = lambda shape: pl.BlockSpec(shape, lambda i, s: (0, 0))
    chunk = jax.ShapeDtypeStruct((rows, depth), BF16)
    return pl.pallas_call(
        kv_kernel,
        out_shape=(jax.ShapeDtypeStruct((rows, DUO), BF16), jax.ShapeDtypeStruct((depth, DUO), BF16), chunk, chunk),
        grid_spec=pltpu.PrefetchScalarGridSpec(
            num_scalar_prefetch=1,
            grid=(rows // BLK,),
            in_specs=[row, row, fixed(wk.shape), fixed(wv.shape), fixed((BLK, BLK))],
            out_specs=(pl.BlockSpec((BLK, DUO), lambda i, s: (i, 0)),) + (pl.BlockSpec(memory_space=pl.ANY),) * 3,
            scratch_shapes=[pltpu.VMEM((depth, DUO), BF16), pltpu.SemaphoreType.DMA((3,))],
        ),
        compiler_params=params(),
        cost_estimate=cost(2 * rows * depth * DUO, 8e6),
    )(core, x, dy, wk, wv, gather_heads(2, HD))


def ranks(rank):
    return rank, rank + 1 - rank % 2 * 2, (rank + 2) % 4, 3 - rank


def block_at(kind, rank, i):
    own, pair, far, far_pair = ranks(rank)
    if kind == "near":
        e = jnp.where(i < 2, own, pair)
        return jnp.where(i % 2 == 0, e, 7 - e)
    e = jnp.where(i == 0, far, far_pair)
    return jnp.where(e % 2 == (1 if kind == "a" else 0), e, 7 - e)


def slot_at(kind, rank, i):
    if kind == "near":
        return (rank + i // 2) % 2 * 2 + i % 2
    return (rank + i) % 2


def attn_kernel(kind, heads, scale, steps, base, sc, wq_hbm, wo_hbm, *refs):
    x_hbm, dy_hbm, kv_hbm, refs = refs[:2], refs[2:4], refs[4:8], refs[8:]
    first, final = kind == "near", kind == "b"
    if first:
        o_ref, dq_ref, dkv_ref, xt_ref = refs[:4]
        scratch = refs[4:]
    else:
        init_hbm, o_ref, dq_ref, dkv_ref, xt_ref = refs[:5]
        scratch = refs[5:]
    ks, vs, kt, vt, dk, dv, qt, dot_t, qst, dost, s_ref, p_ref, ds_ref, ot, dqt, l_ref, ref, wq, wo, xs, dys, w_sem, x_sem, dy_sem, g_sem = scratch
    step = pl.program_id(0)
    hd = HD
    c2 = scale * math.log2(math.e)

    rank = sc[0]
    pos = [p for e in ranks(rank) for p in (e, 7 - e)]
    core = pl.multiple_of(rank % 2 * heads * hd, heads * hd)
    load_kv = []
    for n, p in enumerate(pos):
        src = kv_hbm[n // 2].at[n % 2 * BLK : (n % 2 + 1) * BLK, :]
        at = pl.ds(pl.multiple_of(p * BLK, BLK), BLK)
        for v, dst in enumerate((ks, vs)):
            col = pl.ds(pl.multiple_of((2 * v + rank % 2) * hd, hd), hd)
            load_kv.append(pltpu.make_async_copy(src.at[:, col], dst.at[at, :], g_sem.at[0]))

    def grads(hbm, out):
        pairs = [(hbm.at[:, :hd], dk), (hbm.at[:, hd:], dv)]
        return [pltpu.make_async_copy(*(p[::-1] if out else p), g_sem.at[1]) for p in pairs]

    load_wq, load_wo = [], []
    for n in range(4):
        span = slice(n * DUO, (n + 1) * DUO)
        load_wq.append(pltpu.make_async_copy(wq_hbm.at[span, pl.ds(core, heads * hd)], wq.at[span, :], w_sem.at[0]))
        rows = heads * hd // 4
        dst = wo.at[n * rows : (n + 1) * rows, :]
        load_wo.append(pltpu.make_async_copy(wo_hbm.at[pl.ds(core + n * rows, rows), :], dst, w_sem.at[1]))

    def load_rows(n):
        piece, row = divmod(n, steps // 2)
        src = pl.ds(row * BLK, BLK)
        return (
            pltpu.make_async_copy(x_hbm[piece].at[src, :], xs.at[n % 2], x_sem.at[n % 2]),
            pltpu.make_async_copy(dy_hbm[piece].at[pl.ds(base + row * BLK, BLK), :], dys.at[n % 2], dy_sem.at[n % 2]),
        )

    @pl.when(step == 0)
    def _():
        load_x, _ = load_rows(0)
        for cp in load_kv:
            cp.start()
        load_x.start()
        for cp in load_wq:
            cp.start()

    @pl.when(step == 0)
    def _():
        if first:
            dk[...] = jnp.zeros_like(dk)
            dv[...] = jnp.zeros_like(dv)
        for cp in load_kv:
            cp.wait()
        for i in range(8):
            at = slice(i * BLK, (i + 1) * BLK)
            kt[:, at] = ks[at, :].T
            vt[:, at] = vs[at, :].T
        for cp in [load_rows(0)[1], *load_wo, *([] if first else grads(init_hbm, False))]:
            cp.start()

    @pl.when(step == 0)
    def _():
        for cp in load_wq:
            cp.wait()

    slot = step % 2
    pltpu.make_async_copy(x_hbm[0].at[0:BLK, :], xs.at[slot], x_sem.at[slot]).wait()
    q = dot(xs[slot], wq[...]).astype(BF16)
    xt_ref[...] = xs[slot].T
    for h in range(heads):
        qh = q[:, h * hd : (h + 1) * hd]
        qst[h * BLK : (h + 1) * BLK, :] = qh
        qt[:, h * BLK : (h + 1) * BLK] = qh.T

    @pl.when(step == 0)
    def _():
        for cp in load_wo:
            cp.wait()

    pltpu.make_async_copy(dy_hbm[0].at[0:BLK, :], dys.at[slot], dy_sem.at[slot]).wait()
    do = dot_nt(dys[slot], wo[...]).astype(BF16)

    for n in range(1, steps):

        @pl.when(step == n - 1)
        def _():
            for cp in load_rows(n):
                cp.start()

    for h in range(heads):
        dh = do[:, h * hd : (h + 1) * hd]
        dost[h * BLK : (h + 1) * BLK, :] = dh
        dot_t[:, h * BLK : (h + 1) * BLK] = dh.T

    b = block_at(kind, rank, step)

    def sweep(count, block):
        def pair(j, _):
            block(pl.multiple_of(j * 2 * BLK, 2 * BLK), 2 * BLK)
            return 0

        lax.fori_loop(0, count // 2, pair, 0)

        @pl.when(count % 2 == 1)
        def _():
            block(pl.multiple_of((count - 1) * BLK, BLK), BLK)

    def scores(start, rows, h):
        at = pl.ds(start, rows)
        return at, slice(h * BLK, (h + 1) * BLK), dot(ks[at, :], qt[:, h * BLK : (h + 1) * BLK]) * c2

    def rows_of(t):
        return t.reshape(t.shape[0] // 8, 8, BLK)

    key = lax.broadcasted_iota(jnp.int32, (BLK, BLK), 0)
    query = lax.broadcasted_iota(jnp.int32, (BLK, BLK), 1)
    for h in range(heads):
        at, span, t = scores(pl.multiple_of(b * BLK, BLK), BLK, h)
        t = jnp.where(key <= query, t, LOW)
        s_ref[at, span] = t
        base = jnp.max(t, axis=0, keepdims=True)
        ref[:, span] = base
        l_ref[:, span] = jnp.sum(jnp.exp2(rows_of(t - base)), axis=0)

    def open_block(start, rows):
        for h in range(heads):
            at, span, t = scores(start, rows, h)
            s_ref[at, span] = t
            l_ref[:, span] += jnp.sum(jnp.exp2(rows_of(t - ref[:, span])), axis=0)

    sweep(b, open_block)

    @pl.when(jnp.max(l_ref[...]) > LARGE)
    def _():
        def each(start, fn):
            for h in range(heads):
                span = slice(h * BLK, (h + 1) * BLK)
                fn(span, s_ref[pl.ds(start, BLK), span])

        def peak(span, t):
            ref[:, span] = jnp.maximum(ref[:, span], jnp.max(t, axis=0, keepdims=True))

        def total(span, t):
            l_ref[:, span] += jnp.sum(jnp.exp2(rows_of(t - ref[:, span])), axis=0)

        def over(fn):
            def body(j, _):
                each(pl.multiple_of(j * BLK, BLK), fn)
                return 0

            lax.fori_loop(0, b + 1, body, 0)

        over(peak)
        l_ref[...] = jnp.zeros_like(l_ref)
        over(total)

    lse = ref[...] + jnp.log2(jnp.sum(l_ref[...], axis=0, keepdims=True))

    ot[...] = jnp.zeros_like(ot)

    def value_block(start, rows):
        at = pl.ds(start, rows)
        for h in range(heads):
            span = slice(h * BLK, (h + 1) * BLK)
            p = jnp.exp2(s_ref[at, span] - lse[:, span]).astype(BF16)
            p_ref[at, span] = p
            ot[:, span] += dot(vt[:, at], p)

    sweep(b + 1, value_block)

    o_round = ot[...].astype(BF16)
    delta = jnp.sum(o_round.astype(F32) * dot_t[...].astype(F32), axis=0, keepdims=True)
    for h in range(heads):
        o_ref[h * hd : (h + 1) * hd, :] = o_round[:, h * BLK : (h + 1) * BLK]
    dqt[...] = jnp.zeros_like(dqt)

    def grad_block(start, rows):
        at = pl.ds(start, rows)
        dp = dot(vs[at, :], dot_t[...])
        dv[at, :] += dot(p_ref[at, :], dost[...])
        ds_ref[:rows, :] = (p_ref[at, :].astype(F32) * (dp - delta)).astype(BF16)
        dqt[...] += dot(kt[:, at], ds_ref[:rows, :])
        dk[at, :] += dot(ds_ref[:rows, :], qst[...])

    if not first:

        @pl.when(step == 0)
        def _():
            for cp in grads(init_hbm, False):
                cp.wait()

    if first:
        sweep(b + 1, grad_block)
    else:

        def one_block(j, _):
            grad_block(pl.multiple_of(j * BLK, BLK), BLK)
            return 0

        lax.fori_loop(0, b + 1, one_block, 0)

    for h in range(heads):
        dq_ref[:, h * hd : (h + 1) * hd] = (dqt[:, h * BLK : (h + 1) * BLK] * scale).astype(BF16).T

    @pl.when(step == steps - 1)
    def _():
        if not final:
            for cp in grads(dkv_ref, True):
                cp.start()
            for cp in grads(dkv_ref, True):
                cp.wait()
        else:
            for n, (p, e) in enumerate(zip(pos, [e for e in ranks(rank) for _ in "ab"])):
                at = pl.ds(pl.multiple_of(p * BLK, BLK), BLK)
                if n < 4:
                    row = e % 2 * 2 + n % 2
                else:
                    row = jnp.where((e + n) % 2 == 1, 4, 6) + e % 2
                out = pl.ds(pl.multiple_of(row * BLK, BLK), BLK)
                dkv_ref[out, :hd] = (dk[at, :] * scale).astype(BF16)
                dkv_ref[out, hd:] = dv[at, :].astype(BF16)


def attention(kind, rank, wq, wo, x_pieces, dy_pieces, base, kv_pieces, init, scale):
    final = kind == "b"
    rows, width, model = 2 * (x_pieces[0].shape[0] - base), wq.shape[1] // 2, wq.shape[0]
    hd = HD
    heads = width // hd
    wide = heads * BLK
    seq = SEQ
    slot = functools.partial(slot_at, kind)
    o_spec = pl.BlockSpec((width, BLK), lambda i, s: (0, slot(s[0], i)))
    out_spec = pl.BlockSpec((BLK, width), lambda i, s: (slot(s[0], i), 0))
    xt_spec = pl.BlockSpec((model, BLK), lambda i, s: (0, slot(s[0], i)))
    dkv_spec = pl.BlockSpec((seq, BLK), lambda i, s: (0, 0)) if final else pl.BlockSpec(memory_space=pl.ANY)
    ins = [wq, wo, *x_pieces, *dy_pieces, *kv_pieces] + ([] if init is None else [init])
    return pl.pallas_call(
        functools.partial(attn_kernel, kind, heads, scale, rows // BLK, base),
        out_shape=(
            jax.ShapeDtypeStruct((width, rows), BF16),
            jax.ShapeDtypeStruct((rows, width), BF16),
            jax.ShapeDtypeStruct((seq, BLK), BF16 if final else F32),
            jax.ShapeDtypeStruct((model, rows), BF16),
        ),
        grid_spec=pltpu.PrefetchScalarGridSpec(
            num_scalar_prefetch=1,
            grid=(rows // BLK,),
            in_specs=[pl.BlockSpec(memory_space=pl.ANY) for _ in ins],
            out_specs=(o_spec, out_spec, dkv_spec, xt_spec),
            scratch_shapes=[
                *[pltpu.VMEM((seq, hd), BF16) for _ in "kv"],
                *[pltpu.VMEM((hd, seq), BF16) for _ in "kv"],
                *[pltpu.VMEM((seq, hd), F32) for _ in "kv"],
                *[pltpu.VMEM((hd, wide), BF16) for _ in "qd"],
                *[pltpu.VMEM((wide, hd), BF16) for _ in "qd"],
                pltpu.VMEM((seq, wide), F32),
                pltpu.VMEM((seq, wide), BF16),
                pltpu.VMEM((2 * BLK, wide), BF16),
                *[pltpu.VMEM((hd, wide), F32) for _ in "od"],
                pltpu.VMEM((8, wide), F32),
                pltpu.VMEM((1, wide), F32),
                pltpu.VMEM((model, width), BF16),
                pltpu.VMEM((width, model), BF16),
                *[pltpu.VMEM((2, BLK, model), BF16) for _ in "xd"],
                *[pltpu.SemaphoreType.DMA((2,)) for _ in "wxdg"],
            ],
        ),
        compiler_params=params(1, 63),
        cost_estimate=cost(8e9 * (rows // BLK), 20e6),
    )(rank, *ins)


def y_kernel(sc, o_mine, o_other, w_mine, w_other, out_ref, os):
    half = o_mine.shape[0]

    @pl.when(pl.program_id(0) == 0)
    def _():
        os[:, :half] = o_mine[...].T
        os[:, half:] = o_other[...].T

    out_ref[...] = (dot(os[:, :half], w_mine[...]) + dot(os[:, half:], w_other[...])).astype(BF16)


def out_rows(core, o_mine, o_other, wo):
    rows, half, model, tile = DUO, o_mine.shape[0], wo.shape[1], DUO
    return pl.pallas_call(
        y_kernel,
        out_shape=jax.ShapeDtypeStruct((rows, model), BF16),
        grid_spec=pltpu.PrefetchScalarGridSpec(
            num_scalar_prefetch=1,
            grid=(model // tile,),
            in_specs=[
                pl.BlockSpec((half, rows), lambda i, s: (0, s[0])),
                pl.BlockSpec((half, rows), lambda i, s: (0, s[0])),
                pl.BlockSpec((half, tile), lambda i, s: (s[0], i)),
                pl.BlockSpec((half, tile), lambda i, s: (1 - s[0], i)),
            ],
            out_specs=pl.BlockSpec((rows, tile), lambda i, s: (0, i)),
            scratch_shapes=[pltpu.VMEM((rows, 2 * half), BF16)],
        ),
        compiler_params=params(),
        cost_estimate=cost(4 * rows * half * model, 12e6),
    )(core, o_mine, o_other, wo, wo)


PIECES = ((0, DUO), (1, DUO), (0, BLK), (1, BLK), (0, BLK), (1, BLK))
STARTS = (0, DUO, HALF, 1280, 1536, 1792)


def piece_copies(core, arrays, dst, sem, rows):
    copies = []
    for n, ((flip, size), start) in enumerate(zip(PIECES, STARTS)):
        at = pl.ds(pl.multiple_of((1 - core if flip else core) * size, size), size)
        copies.append(pltpu.make_async_copy(arrays[n // 2].at[rows, at], dst.at[rows, start : start + size], sem))
    return copies


def tail_kernel(sc, *refs):
    o_mine, o_other, ys, q_mine, q_other, kv_in = (refs[a:b] for a, b in ((0, 3), (3, 6), (6, 12), (12, 15), (15, 18), (18, 20)))
    xts, (wq_mine, wq_other, wkv), refs = refs[20:23], refs[23:26], refs[26:]
    gwo_ref, gwq_ref, gk_ref, gv_ref, dx_ref, o_all, y_all, dq, kv, kv_rows, sems = refs
    step, core, hd = pl.program_id(0), sc[0], HD
    tile, wide = gwo_ref.shape
    spans = [slice(0, HALF), slice(HALF, HALF + DUO), slice(HALF + DUO, SEQ)]
    o_copies = [
        [piece_copies(core, o, o_all.at[n], sems.at[n, t], slice(t * tile, (t + 1) * tile)) for t in range(2)]
        for n, o in enumerate((o_mine, o_other))
    ]
    y_copies = [
        [
            pltpu.make_async_copy(
                y.at[y.shape[0] - r if r == BLK else 0 :, n * wide : (n + 1) * wide], y_all.at[n, s : s + r, :], sems.at[2, n]
            )
            for y, s, (_, r) in zip(ys, STARTS, PIECES)
        ]
        for n in range(2)
    ]
    q_copies = [
        [pltpu.make_async_copy(a, dq.at[n, at, :], sems.at[3, 0]) for a, at in zip(part, spans)]
        for n, part in enumerate((q_mine, q_other))
    ]
    kv_copies = [pltpu.make_async_copy(a, kv.at[:, n * BLK : (n + 1) * BLK], sems.at[3, 0]) for n, a in enumerate(kv_in)]

    def start(at, copies):
        @pl.when(step == at)
        def _():
            for cp in copies:
                cp.start()

    def wait(at, copies):
        @pl.when(step == at)
        def _():
            for cp in copies:
                cp.wait()

    rest = q_copies[0] + q_copies[1] + kv_copies
    start(0, o_copies[0][0] + y_copies[0])
    wait(0, o_copies[0][0] + y_copies[0])
    start(0, o_copies[0][1] + o_copies[1][0] + o_copies[1][1])
    start(2, y_copies[1])
    start(3, rest)
    wait(1, o_copies[0][1])
    wait(2, o_copies[1][0] + o_copies[1][1])
    wait(4, y_copies[1])
    wait(WO_STEPS, rest)

    @pl.when(step < WO_STEPS)
    def _():
        rows = pl.ds(pl.multiple_of(step % 2 * tile, tile), tile)
        gwo_ref[...] = dot(o_all[step // 2 % 2, rows, :], y_all[step // 4])

    @pl.when((step >= WO_STEPS) & (step < DX_STEP))
    def _():
        part = (step - WO_STEPS) // 4
        acc = sum(dot(x[...], dq[part, at, :]) for x, at in zip(xts, spans))
        flat = gwq_ref.reshape(tile * 8, hd)
        for h in range(8):
            flat[pl.ds(h, tile, stride=8), :] = acc[:, h * hd : (h + 1) * hd]

    @pl.when((step >= DX_STEP - 4) & (step < DX_STEP))
    def _():
        k_flat, v_flat = gk_ref.reshape(tile * 2, hd), gv_ref.reshape(tile * 2, hd)
        both = sum(dot(x[...], kv[at, :]) for x, at in zip(xts, spans))
        for n, head in enumerate((core, 1 - core)):
            k_flat[pl.ds(head, tile, stride=2), :] = both[:, 2 * n * hd : (2 * n + 1) * hd]
            v_flat[pl.ds(head, tile, stride=2), :] = both[:, (2 * n + 1) * hd : (2 * n + 2) * hd]

    own = pl.ds(pl.multiple_of(core * DUO, DUO), DUO)

    @pl.when(step == DX_STEP)
    def _():
        for n, head in enumerate((core, 1 - core)):
            for v in range(2):
                col = pl.ds(pl.multiple_of((2 * v + head) * hd, hd), hd)
                kv_rows[:, col] = kv[own, (2 * n + v) * hd : (2 * n + v + 1) * hd]

    @pl.when(step >= DX_STEP)
    def _():
        acc = dot_nt(dq[0, own, :], wq_mine[...]) + dot_nt(dq[1, own, :], wq_other[...])
        dx_ref[...] = (acc + dot_nt(kv_rows[...], wkv[...])).astype(BF16)


def tail(core, o_mine, o_other, ys, q_mine, q_other, kvm, kvo, xts, wq, wkv):
    model, half, tile, wide = ys[0].shape[1], o_mine[0].shape[0], DUO, HALF
    wo = lambda i: jnp.minimum(i, WO_STEPS - 1)
    q = lambda i: jnp.clip(i - WO_STEPS, 0, 7)
    kv = lambda i: jnp.clip(i - DX_STEP + 4, 0, 3)
    dx = lambda i: jnp.maximum(i - DX_STEP, 0)
    hbm = [*o_mine, *o_other, *ys, *q_mine, *q_other, kvm, kvo]
    small = pl.BlockSpec((tile, 2, HD), lambda i, s: (kv(i), 0, 0))
    return pl.pallas_call(
        tail_kernel,
        out_shape=(
            jax.ShapeDtypeStruct((2 * half, model), F32),
            jax.ShapeDtypeStruct((model, 16, HD), F32),
            jax.ShapeDtypeStruct((model, 2, HD), F32),
            jax.ShapeDtypeStruct((model, 2, HD), F32),
            jax.ShapeDtypeStruct((DUO, model), BF16),
        ),
        grid_spec=pltpu.PrefetchScalarGridSpec(
            num_scalar_prefetch=1,
            grid=(DX_STEP + 4,),
            in_specs=[pl.BlockSpec(memory_space=pl.ANY) for _ in hbm]
            + [pl.BlockSpec((tile, x.shape[1]), lambda i, s: (q(i) % 4, 0)) for x in xts]
            + [
                pl.BlockSpec((tile, half), lambda i, s: (dx(i), s[0])),
                pl.BlockSpec((tile, half), lambda i, s: (dx(i), 1 - s[0])),
                pl.BlockSpec((tile, DUO), lambda i, s: (dx(i), 0)),
            ],
            out_specs=(
                pl.BlockSpec((tile, wide), lambda i, s: ((s[0] + wo(i) // 2) % 2 * 2 + wo(i) % 2, wo(i) // 4)),
                pl.BlockSpec((tile, 8, HD), lambda i, s: (q(i) % 4, (s[0] + q(i) // 4) % 2, 0)),
                small,
                small,
                pl.BlockSpec((DUO, tile), lambda i, s: (0, dx(i))),
            ),
            scratch_shapes=[
                pltpu.VMEM((2, half, SEQ), BF16),
                pltpu.VMEM((2, SEQ, wide), BF16),
                pltpu.VMEM((2, SEQ, half), BF16),
                pltpu.VMEM((SEQ, DUO), BF16),
                pltpu.VMEM((DUO, DUO), BF16),
                pltpu.SemaphoreType.DMA((4, 2)),
            ],
        ),
        compiler_params=params(1, 63),
        cost_estimate=cost(5e10, 8e7),
    )(core, *hbm, *xts, wq, wq, wkv)


def solution(mesh):
    row_spec = P(("dp", "cp"), None)
    rep_spec = P(None, None, None)
    part_spec = P("dp", None, None)
    core_swap = [(0, 1), (1, 0), (2, 3), (3, 2)]
    chip_swap = [(0, 2), (2, 0), (1, 3), (3, 1)]

    def device_layer(x, dy, w_query, w_key, w_value, w_out):
        _, model = x.shape
        num_heads, hd = w_query.shape[1:]
        kv_heads = w_key.shape[1]
        scale = hd ** -0.5
        rank = lax.axis_index("cp").astype(jnp.int32)
        c = rank & 1
        core = c.reshape(1)
        rank = rank.reshape(1)

        to_core = lambda v: lax.ppermute(v, "cp", core_swap)
        to_chip = lambda v: lax.ppermute(v, "cp", chip_swap)

        wk = w_key.reshape(model * kv_heads, hd)
        wv = w_value.reshape(model * kv_heads, hd)
        wo = w_out.reshape(num_heads * hd, model)
        x_p = to_core(x)
        dy_p = to_core(dy)

        kv, wkv, r_a, r_b = project_kv(core, x, dy, wk, wv)
        far_kv, kv_p = to_chip(kv), to_core(kv)
        w_s, _ = lax.optimization_barrier((w_query, kv))
        r_a, r_b = to_chip(r_a), to_chip(r_b)
        wq = flat_heads(w_s)
        kv_r, wq = lax.optimization_barrier((far_kv, wq))
        kv_rp = to_core(kv_r)
        pieces = (kv, kv_p, kv_r, kv_rp)

        o_c, dq_c, part, xt_c = attention(
            "near", rank, wq, wo, (x, x_p), (dy, dy_p), 0, pieces, None, scale)
        r_a, o_c, dq_c = lax.optimization_barrier((r_a, o_c, dq_c))
        r_pa, o_co, dq_co = to_core(r_a), to_core(o_c), to_core(dq_c)

        o_a, dq_a, part, xt_a = attention("a", rank, wq, wo, (r_a, r_pa), (r_a, r_pa), BLK, pieces, part, scale)
        r_b, o_a, dq_a = lax.optimization_barrier((r_b, o_a, dq_a))
        r_pb, o_ao, dq_ao = to_core(r_b), to_core(o_a), to_core(dq_a)

        o_b, dq_b, dkv, xt_b = attention("b", rank, wq, wo, (r_b, r_pb), (r_b, r_pb), BLK, pieces, part, scale)
        o_co, dkv = lax.optimization_barrier((o_co, dkv))
        dkv_o, o_bo, dq_bo = to_core(dkv), to_core(o_b), to_core(dq_b)
        y = out_rows(core, o_c, o_co, wo)

        ys = (dy, dy_p, r_a, r_pa, r_b, r_pb)
        gwo, gwq, gwk, gwv, dx = tail(
            core, (o_c, o_a, o_b), (o_co, o_ao, o_bo), ys,
            (dq_c, dq_a, dq_b), (dq_co, dq_ao, dq_bo), dkv, dkv_o, (xt_c, xt_a, xt_b), wq, wkv,
        )
        return y, dx, gwq, gwk, gwv, gwo.reshape(num_heads, hd, model)

    return jax.shard_map(
        device_layer,
        mesh=mesh,
        in_specs=(row_spec, row_spec, rep_spec, rep_spec, rep_spec, rep_spec),
        out_specs=(row_spec, row_spec, part_spec, part_spec, part_spec, part_spec),
        check_vma=False,
    )
```
